256 devices in a mesh: replica: 32 (over z_lo, y, core), model: 8 (over z_hi, x).
Axes of the slice: x: 4, y: 4, z: 8 (z_hi: 2, z_lo: 4; z = z_hi * 4 + z_lo), core: 2. Of those that a mesh axis runs over, the one named last changes fastest.
Arguments:
- layer_grads: bfloat16 [32, 2, 4096, 1024], P('replica', None, 'model'), may hold values from -6 to 6
- last_basis: float32 [2, 1024, 32], replicated, may hold values from -6 to 6
- layer_weights: float32 [2, 4096, 1024], P(None, 'model', 'replica'), may hold values from -0.1875 to 0.1875
- momentum: float32 [2, 4096, 1024], P(None, 'model', 'replica'), may hold values from -0.3125 to 0.3125
Outputs:
- new_weights: float32 [2, 4096, 1024], P(None, 'model', 'replica')
- new_basis: float32 [2, 1024, 32], replicated
- new_momentum: float32 [2, 4096, 1024], P(None, 'model', 'replica')
The draws below stay inside these ranges and needn't reach their ends.
All inputs are finite; a program needn't handle non-finite values.
Results may differ from the reference program's by a relative error of at most 0.0029.
Values sent between devices are 32-bit elements; how exact they have to be, the bound alone decides.
No kernel may reach another device: no remote copies, remote signals or barrier semaphores. Data moves between devices by JAX's collectives and lax.ppermute only.
A program may use at most 64 MiB of HBM per device.

```python
import jax
import jax.numpy as jnp
from jax import lax

WIDTH = 1024
INNER = 4096
RANK = 32
LAYERS = 2
REPLICAS = 32
N_MODEL = 8


def draw_layer_grads(key, part):
    keys = jax.random.split(key, 5)
    level = jnp.exp(jax.random.uniform(keys[4], (1, LAYERS, N_MODEL, 1, RANK), jnp.float32, -1.3, 1.3))
    left = jax.random.normal(keys[0], (1, LAYERS, N_MODEL, INNER // N_MODEL, RANK), jnp.float32) * level
    left = left.reshape(1, LAYERS, INNER, RANK)
    right = jax.random.normal(keys[1], (1, LAYERS, RANK, WIDTH), jnp.float32)
    strength = jax.random.normal(keys[2], (REPLICAS, LAYERS, 1, RANK), jnp.float32)
    noise = jax.random.normal(keys[3], (REPLICAS, LAYERS, INNER, WIDTH), jnp.float32)
    low = jnp.einsum('alir,lrw->aliw', left * strength, right[0])
    values = low * RANK ** (-0.5) + 0.5 * noise
    return jnp.clip(values, -6.0, 6.0).astype(jnp.bfloat16)


def block_scale(key, dims, shards, least, high):
    level = 1.0
    for dim, blocks in shards:
        draws = jax.random.uniform(jax.random.fold_in(jax.random.fold_in(key, 6), dim), (blocks,), jnp.float32, least / len(shards), high / len(shards))
        level = level * jnp.repeat(jnp.exp(draws), dims[dim] // blocks).reshape((-1,) + (1,) * (len(dims) - 1 - dim))
    return level


def gaussian(key, shape, width, reach, pieces=(), kind=jnp.bfloat16):
    values = width * jax.random.normal(key, shape, jnp.float32)
    if pieces:
        values = values * block_scale(key, shape, pieces, -0.22, 0.18)
    return jnp.clip(values, -reach, reach).astype(kind)


def setup_inputs(seed: int = 0) -> dict:
    seeds = jax.random.split(jax.random.key(seed), 5)
    layer_grads = draw_layer_grads(jax.random.fold_in(seeds[4], 71), 0)
    last_basis = gaussian(seeds[1], (LAYERS, WIDTH, RANK), 1.0, 6.0, (), jnp.float32)
    layer_weights = gaussian(seeds[2], (LAYERS, INNER, WIDTH), WIDTH ** -0.5, 0.1875, ((1, 8), (2, 32)), jnp.float32)
    momentum = gaussian(seeds[3], (LAYERS, INNER, WIDTH), 0.05, 0.3125, ((1, 8), (2, 32)), jnp.float32)
    return dict(layer_grads=layer_grads, last_basis=last_basis, layer_weights=layer_weights, momentum=momentum)


def reference(layer_grads, last_basis, layer_weights, momentum):
    small_basis = last_basis.astype(jnp.bfloat16)
    small_basis = lax.optimization_barrier(small_basis)
    left = jnp.einsum('aliw,lwr->lir', layer_grads.astype(jnp.float32), small_basis.astype(jnp.float32))
    gram = jnp.einsum('lir,lis->lrs', left, left, precision=lax.Precision.HIGHEST)
    gram = gram + 0.001 * lax.optimization_barrier(jnp.mean(jnp.diagonal(gram, axis1=1, axis2=2), axis=1))[:, None, None] * jnp.eye(RANK, dtype=jnp.float32)
    small_left = lax.optimization_barrier(left.astype(jnp.bfloat16))
    right = jnp.einsum('aliw,lir->lwr', layer_grads.astype(jnp.float32), small_left.astype(jnp.float32))
    root = jnp.linalg.cholesky(gram)
    half = lax.linalg.triangular_solve(root, jnp.swapaxes(right, 1, 2), left_side=True, lower=True)
    mixed = lax.linalg.triangular_solve(root, half, left_side=True, lower=True, transpose_a=True)
    change = jnp.einsum('lir,lrw->liw', left, mixed, precision=lax.Precision.HIGHEST) / REPLICAS
    new_momentum = 0.9 * momentum + change
    new_weights = layer_weights - 0.02 * new_momentum
    new_basis = right * lax.rsqrt(lax.optimization_barrier(jnp.mean(right * right, axis=(1, 2), keepdims=True)) + 1e-12)
    return (new_weights, new_basis, new_momentum)
```

```python
import functools

import jax
import jax.numpy as jnp
from jax import lax
from jax.experimental import pallas as pl
from jax.experimental.pallas import tpu as pltpu
from jax.sharding import Mesh
from jax.sharding import PartitionSpec as P

RANK = 32
LANES = 128
SIZES = {"zlo": 4, "y": 4, "core": 2, "zhi": 2, "x": 4}
REPLICA = ("zlo", "y", "core")
MODEL = ("zhi", "x")
PLANE = ("y", "core", "x")
COLUMN = ("zlo", "zhi")
REPLICAS, PEERS, STACK = 32, 32, 8
SHARES = 8
CHUNK = 18
EXACT = lax.Precision.HIGHEST
VMEM_LIMIT = 24 * 1024 * 1024


def kernel_call(body, outs, flops=1 << 20, moved=1 << 18):
    many = isinstance(outs, (list, tuple))
    count = len(outs) if many else 1
    spec = pl.BlockSpec(memory_space=pltpu.VMEM)
    return lambda *args: pl.pallas_call(
        body,
        out_shape=outs,
        in_specs=[spec] * len(args),
        out_specs=[spec] * count if many else spec,
        compiler_params=pltpu.CompilerParams(vmem_limit_bytes=VMEM_LIMIT),
        cost_estimate=pl.CostEstimate(flops=flops, bytes_accessed=moved, transcendentals=0),
    )(*args)


def f32(*shape):
    return jax.ShapeDtypeStruct(shape, jnp.float32)


def joined(ref, rows, columns):
    return jnp.concatenate(
        [
            jnp.concatenate([ref[t * columns + j] for j in range(columns)], axis=1)
            for t in range(rows)
        ],
        axis=0,
    )


def lane_of(shape):
    return lax.broadcasted_iota(jnp.int32, shape, 1)


def row_of(shape):
    return lax.broadcasted_iota(jnp.int32, shape, 0)


def right_body(left_ref, grads_ref, out_ref):
    left = joined(left_ref, 8, 4)
    share = lax.axis_index("y") * 2 + lax.axis_index("core")
    twice = jnp.concatenate([left, left], axis=0)
    gram = lax.dot_general(
        left, twice, (((1,), (1,)), ((), ())), precision=EXACT, preferred_element_type=jnp.float32
    )
    lane = lane_of((16, LANES))
    packed = jnp.where(
        lane < 32,
        gram[0:16],
        jnp.where(lane < 64, gram[32:48], jnp.where(lane < 96, gram[16:32], gram[48:64])),
    )
    mine = packed[0:2]
    for s in range(1, SHARES):
        mine = jnp.where(share == s, packed[2 * s : 2 * s + 2], mine)
    for l in range(2):
        right = jnp.dot(
            left[l * RANK : (l + 1) * RANK].astype(jnp.bfloat16),
            grads_ref[l],
            preferred_element_type=jnp.float32,
        )
        for t in range(4):
            for j in range(4):
                at = CHUNK * (16 * l + 4 * t + j)
                rows = right[8 * t : 8 * t + 8]
                out_ref[at : at + 8] = rows[:, 256 * j : 256 * j + 128]
                out_ref[at + 8 : at + 16] = rows[:, 256 * j + 128 : 256 * j + 256]
                out_ref[at + 16 : at + 18] = mine


def plane_body(in_ref, out_ref):
    total = in_ref[0:16]
    for s in range(1, PEERS):
        total = total + in_ref[CHUNK * s : CHUNK * s + 16]
    for z in range(STACK):
        out_ref[z, 0:16] = total
    for share in range(SHARES):
        part = None
        for x in range(4):
            at = CHUNK * (4 * share + x) + 16
            piece = in_ref[at : at + 2]
            part = piece if part is None else part + piece
        for z in range(STACK):
            out_ref[z, 16 + 2 * share : 18 + 2 * share] = part


def column_body(in_ref, out_ref, gram_ref):
    total = in_ref[0]
    for z in range(1, STACK):
        total = total + in_ref[z]
    for d in range(PEERS):
        out_ref[d] = total[0:16]
    gram_ref[...] = total[16:32] * 0.25


def factor_body(gram_ref, left_ref, inverse_ref, frame_ref):
    packed = gram_ref[...]
    shape = (RANK, LANES)
    lane, row = lane_of(shape), row_of(shape)
    gram = jnp.concatenate([packed, pltpu.roll(packed, 64, 1)], axis=0)
    first = (lane // RANK) % 2 == 0
    unit = (lane % RANK) == row
    diagonal = jnp.where(unit & (lane < 64), gram, 0.0)
    mean0 = jnp.sum(jnp.where(first, diagonal, 0.0)) * (1.0 / RANK)
    mean1 = jnp.sum(jnp.where(first, 0.0, diagonal)) * (1.0 / RANK)
    ridge = 0.001 * jnp.where(first, mean0, mean1)
    work = jnp.where(lane < 64, gram, 0.0) + jnp.where(unit, jnp.where(lane < 64, ridge, 1.0), 0.0)
    pivots = jnp.ones(shape, jnp.float32)
    for k in range(RANK):
        column = jnp.where(first, work[:, k : k + 1], work[:, RANK + k : RANK + k + 1])
        pivot = column[k : k + 1]
        pivots = jnp.where(row == k, column, pivots)
        if k + 1 < RANK:
            step = work[k : k + 1] / pivot
            work = work - jnp.where(row > k, column * step, 0.0)
    inverse = pltpu.roll(work / jnp.sqrt(pivots), 64, 1)
    inverse_ref[...] = inverse
    left = joined(left_ref, 8, 4)
    for l in range(2):
        frame_ref[l] = (
            jnp.dot(
                inverse[:, l * RANK : (l + 1) * RANK],
                left[l * RANK : (l + 1) * RANK],
                precision=EXACT,
                preferred_element_type=jnp.float32,
            )
            * (1.0 / REPLICAS)
        )


def final_body(right_ref, inverse_ref, frame_ref, weights_ref, momentum_ref, basis_ref, new_w_ref, new_m_ref):
    place = (lax.axis_index("zlo") * 4 + lax.axis_index("y")) * 2 + lax.axis_index("core")
    block = place // 4
    shift = (4 - place % 4) * 32
    for l in range(2):
        square = jnp.zeros((8, LANES), jnp.float32)
        for i in range(32):
            tile = right_ref[32 * l + i]
            square = square + tile * tile
        scale = lax.rsqrt(jnp.sum(square) * (1.0 / (RANK * 1024)) + 1e-12)
        for t in range(4):
            for j in range(8):
                basis_ref[l, 8 * t : 8 * t + 8, 128 * j : 128 * j + 128] = (
                    right_ref[32 * l + 8 * t + j] * scale
                )
        own = jnp.concatenate([right_ref[32 * l + 8 * t + block] for t in range(4)], axis=0)
        half = jnp.dot(
            inverse_ref[:, l * RANK : (l + 1) * RANK],
            own,
            precision=EXACT,
            preferred_element_type=jnp.float32,
        )
        half = pltpu.roll(half, shift, 1)[:, :RANK]
        change = lax.dot_general(
            half,
            frame_ref[l],
            (((0,), (0,)), ((), ())),
            precision=EXACT,
            preferred_element_type=jnp.float32,
        )
        new = 0.9 * momentum_ref[l] + change
        new_m_ref[l] = new
        new_w_ref[l] = weights_ref[l] - 0.02 * new


def shards(layer_grads, last_basis, layer_weights, momentum):
    grads = layer_grads[0]
    layers, rows, width = grads.shape
    basis = jnp.swapaxes(last_basis, 1, 2).astype(jnp.bfloat16)
    part_left = jnp.einsum("lrw,liw->lri", basis, grads, preferred_element_type=jnp.float32)
    tiles = part_left.reshape(8, 8, 4, LANES).transpose(0, 2, 1, 3).reshape(REPLICAS, 8, LANES)
    tile = jnp.sum(lax.all_to_all(tiles, REPLICA, 0, 0, tiled=True), axis=0)
    copies = jnp.broadcast_to(tile[None], tiles.shape)
    left = lax.all_to_all(copies, REPLICA, 0, 0, tiled=True)

    sent = kernel_call(right_body, f32(PEERS * CHUNK, LANES))(left, grads)
    sent = sent.reshape(PEERS * CHUNK // 2, 2, LANES)
    came = lax.all_to_all(sent, PLANE, 0, 0, tiled=True).reshape(PEERS * CHUNK, LANES)
    sent = kernel_call(plane_body, f32(STACK, 32, LANES))(came)
    came = lax.all_to_all(sent, COLUMN, 0, 0, tiled=True)
    sent, gram = kernel_call(column_body, [f32(PEERS, 16, LANES), f32(16, LANES)])(came)
    right = lax.all_to_all(sent, PLANE, 0, 0, tiled=True).reshape(64, 8, LANES)
    inverse, frame = kernel_call(
        factor_body, [f32(RANK, LANES), f32(layers, RANK, rows)], flops=1 << 28
    )(gram, left)
    new_basis, new_weights, new_momentum = kernel_call(
        final_body,
        [f32(layers, RANK, width), f32(layers, RANK, rows), f32(layers, RANK, rows)],
    )(right, inverse, frame, jnp.swapaxes(layer_weights, 1, 2), jnp.swapaxes(momentum, 1, 2))
    return tuple(jnp.swapaxes(a, 1, 2) for a in (new_weights, new_basis, new_momentum))


def solution(mesh):
    fine = Mesh(mesh.devices.reshape(tuple(SIZES.values())), tuple(SIZES))
    sharded = P(None, MODEL, REPLICA)
    return jax.shard_map(
        shards,
        mesh=fine,
        in_specs=(P(REPLICA, None, MODEL, None), P(), sharded, sharded),
        out_specs=(sharded, P(), sharded),
        check_vma=False,
    )
```

```python
import functools

import jax
import jax.numpy as jnp
from jax import lax
from jax.experimental import pallas as pl
from jax.experimental.pallas import tpu as pltpu
from jax.sharding import Mesh
from jax.sharding import PartitionSpec as P

RANK = 32
LANES = 128
SIZES = {"zlo": 4, "y": 4, "core": 2, "zhi": 2, "x": 4}
REPLICA = ("zlo", "y", "core")
MODEL = ("zhi", "x")
LINES = ("zlo", "y")
PLANE = ("y", "x")
COLUMN = ("zlo", "zhi")
REPLICAS, PEERS, STACK = 32, 16, 8
CHUNK = 20
EXACT = lax.Precision.HIGHEST
VMEM_LIMIT = 24 * 1024 * 1024


def kernel_call(body, outs, flops=1 << 20, moved=1 << 18):
    many = isinstance(outs, (list, tuple))
    count = len(outs) if many else 1
    spec = pl.BlockSpec(memory_space=pltpu.VMEM)
    return lambda *args: pl.pallas_call(
        body,
        out_shape=outs,
        in_specs=[spec] * len(args),
        out_specs=[spec] * count if many else spec,
        compiler_params=pltpu.CompilerParams(vmem_limit_bytes=VMEM_LIMIT),
        cost_estimate=pl.CostEstimate(flops=flops, bytes_accessed=moved, transcendentals=0),
    )(*args)


def f32(*shape):
    return jax.ShapeDtypeStruct(shape, jnp.float32)


def joined(ref, rows, columns):
    return jnp.concatenate(
        [
            jnp.concatenate([ref[t * columns + j] for j in range(columns)], axis=1)
            for t in range(rows)
        ],
        axis=0,
    )


def lane_of(shape):
    return lax.broadcasted_iota(jnp.int32, shape, 1)


def row_of(shape):
    return lax.broadcasted_iota(jnp.int32, shape, 0)


def core():
    return lax.axis_index("core")


def left_body(mine, basis_ref, grads_ref, out_ref):
    layer = core() if mine else 1 - core()
    left = lax.dot_general(
        basis_ref[layer].astype(jnp.bfloat16),
        grads_ref[layer],
        (((1,), (1,)), ((), ())),
        preferred_element_type=jnp.float32,
    )
    for t in range(4):
        for j in range(4):
            out_ref[4 * t + j] = left[8 * t : 8 * t + 8, LANES * j : LANES * j + LANES]


def right_body(mine, left_ref, grads_ref, out_ref):
    layer = core() if mine else 1 - core()
    right = jnp.dot(
        joined(left_ref, 4, 4).astype(jnp.bfloat16),
        grads_ref[layer],
        preferred_element_type=jnp.float32,
    )
    for t in range(4):
        for j in range(8):
            d, h = divmod(8 * t + j, 2)
            out_ref[d, 8 * h : 8 * h + 8] = right[8 * t : 8 * t + 8, LANES * j : LANES * j + LANES]


def by_layer(mine_ref, other_ref):
    mine, other = joined(mine_ref, 4, 4), joined(other_ref, 4, 4)
    first = core() == 0
    return jnp.where(first, mine, other), jnp.where(first, other, mine)


def gram_body(mine_ref, other_ref, share_ref):
    left = jnp.concatenate(by_layer(mine_ref, other_ref), axis=0)
    twice = jnp.concatenate([left, left], axis=0)
    gram = lax.dot_general(
        left, twice, (((1,), (1,)), ((), ())), precision=EXACT, preferred_element_type=jnp.float32
    )
    lane = lane_of((16, LANES))
    packed = jnp.where(
        lane < 32,
        gram[0:16],
        jnp.where(lane < 64, gram[32:48], jnp.where(lane < 96, gram[16:32], gram[48:64])),
    )
    share_ref[...] = picked([packed[4 * s : 4 * s + 4] for s in range(4)], lax.axis_index("y"))


def picked(values, index):
    out = values[0]
    for s in range(1, len(values)):
        out = jnp.where(index == s, values[s], out)
    return out


def pack_body(mine_ref, other_ref, share_ref, out_ref):
    share = share_ref[...]
    for d in range(PEERS):
        out_ref[CHUNK * d : CHUNK * d + 16] = mine_ref[d] + other_ref[d]
        out_ref[CHUNK * d + 16 : CHUNK * d + CHUNK] = share


def plane_body(in_ref, out_ref):
    total = in_ref[0:16]
    for s in range(1, PEERS):
        total = total + in_ref[CHUNK * s : CHUNK * s + 16]
    parts = []
    for y in range(4):
        part = None
        for x in range(4):
            at = CHUNK * (4 * y + x) + 16
            piece = in_ref[at : at + 4]
            part = piece if part is None else part + piece
        parts.append(part)
    share = picked(parts, lax.axis_index("zlo"))
    for z in range(STACK):
        out_ref[CHUNK * z : CHUNK * z + 16] = total
        out_ref[CHUNK * z + 16 : CHUNK * z + CHUNK] = share


def column_body(in_ref, out_ref, gram_ref):
    total = in_ref[0:16]
    for s in range(1, STACK):
        total = total + in_ref[CHUNK * s : CHUNK * s + 16]
    for d in range(PEERS):
        out_ref[d] = total
    for q in range(4):
        at = 2 * CHUNK * q + 16
        gram_ref[4 * q : 4 * q + 4] = in_ref[at : at + 4] + in_ref[at + CHUNK : at + CHUNK + 4]


def factor_body(gram_ref, mine_ref, other_ref, inverse_ref, frame_ref):
    packed = gram_ref[...]
    shape = (RANK, LANES)
    lane, row = lane_of(shape), row_of(shape)
    gram = jnp.concatenate([packed, pltpu.roll(packed, 64, 1)], axis=0)
    first = (lane // RANK) % 2 == 0
    unit = (lane % RANK) == row
    diagonal = jnp.where(unit & (lane < 64), gram, 0.0)
    mean0 = jnp.sum(jnp.where(first, diagonal, 0.0)) * (1.0 / RANK)
    mean1 = jnp.sum(jnp.where(first, 0.0, diagonal)) * (1.0 / RANK)
    ridge = 0.001 * jnp.where(first, mean0, mean1)
    work = jnp.where(lane < 64, gram, 0.0) + jnp.where(unit, jnp.where(lane < 64, ridge, 1.0), 0.0)
    pivots = jnp.ones(shape, jnp.float32)
    for k in range(RANK):
        column = jnp.where(first, work[:, k : k + 1], work[:, RANK + k : RANK + k + 1])
        pivot = column[k : k + 1]
        pivots = jnp.where(row == k, column, pivots)
        if k + 1 < RANK:
            step = work[k : k + 1] / pivot
            work = work - jnp.where(row > k, column * step, 0.0)
    inverse = pltpu.roll(work / jnp.sqrt(pivots), 64, 1)
    inverse_ref[...] = inverse
    left = by_layer(mine_ref, other_ref)
    for l in range(2):
        frame_ref[l] = (
            jnp.dot(
                inverse[:, l * RANK : (l + 1) * RANK],
                left[l],
                precision=EXACT,
                preferred_element_type=jnp.float32,
            )
            * (1.0 / REPLICAS)
        )


def settle(layer, right_ref, inverse_ref, frame_ref, weights_ref, momentum_ref):
    place = (lax.axis_index("zlo") * 4 + lax.axis_index("y")) * 2 + core()
    block = place // 4
    shift = (4 - place % 4) * 32
    square = jnp.zeros((8, LANES), jnp.float32)
    for i in range(32):
        tile = right_ref[i]
        square = square + tile * tile
    scale = lax.rsqrt(jnp.sum(square) * (1.0 / (RANK * 1024)) + 1e-12)
    own = jnp.concatenate([right_ref[8 * t + block] for t in range(4)], axis=0)
    inverse = inverse_ref[...]
    inverse = jnp.where(layer == 0, inverse[:, :RANK], inverse[:, RANK : 2 * RANK])
    half = jnp.dot(inverse, own, precision=EXACT, preferred_element_type=jnp.float32)
    half = pltpu.roll(half, shift, 1)[:, :RANK]
    change = lax.dot_general(
        half,
        frame_ref[layer],
        (((0,), (0,)), ((), ())),
        precision=EXACT,
        preferred_element_type=jnp.float32,
    )
    new = 0.9 * momentum_ref[layer] + change
    return scale, new, weights_ref[layer] - 0.02 * new


def scaled(right_ref, scale, basis_ref, layer):
    for t in range(4):
        for j in range(8):
            at = (slice(8 * t, 8 * t + 8), slice(LANES * j, LANES * j + LANES))
            at = at if layer is None else (layer, *at)
            basis_ref[at] = right_ref[8 * t + j] * scale


def early_body(right_ref, inverse_ref, frame_ref, weights_ref, momentum_ref, basis_ref, w_ref, m_ref):
    scale, new, weights = settle(core(), right_ref, inverse_ref, frame_ref, weights_ref, momentum_ref)
    scaled(right_ref, scale, basis_ref, None)
    m_ref[...] = new
    w_ref[...] = weights


def late_body(
    right_ref, inverse_ref, frame_ref, weights_ref, momentum_ref, b_ref, w_ref, m_ref,
    basis_ref, new_w_ref, new_m_ref,
):
    c = core()
    basis_ref[c] = b_ref[...]
    new_w_ref[c] = w_ref[...]
    new_m_ref[c] = m_ref[...]
    layer = 1 - c
    scale, new, weights = settle(layer, right_ref, inverse_ref, frame_ref, weights_ref, momentum_ref)
    scaled(right_ref, scale, basis_ref, layer)
    new_m_ref[layer] = new
    new_w_ref[layer] = weights


def swapped(value):
    return lax.ppermute(value, "core", [(0, 1), (1, 0)])


def all_to_all(value, axes):
    return lax.all_to_all(value, axes, 0, 0, tiled=True)


def shards(layer_grads, last_basis, layer_weights, momentum):
    grads = layer_grads[0]
    layers, rows, width = grads.shape
    basis = jnp.swapaxes(last_basis, 1, 2)
    weights, momentum = jnp.swapaxes(layer_weights, 1, 2), jnp.swapaxes(momentum, 1, 2)
    lefts, rights = f32(PEERS, 8, LANES), f32(PEERS, 16, LANES)

    away = swapped(kernel_call(functools.partial(left_body, False), lefts)(basis, grads))
    mine = kernel_call(functools.partial(left_body, True), lefts)(basis, grads)
    tile = jnp.sum(all_to_all(mine + away, LINES), axis=0)
    mine = all_to_all(jnp.broadcast_to(tile[None], lefts.shape), LINES)
    other = swapped(mine)
    kept = kernel_call(functools.partial(right_body, True), rights)(mine, grads)
    kept, other = lax.optimization_barrier((kept, other))
    away = swapped(kernel_call(functools.partial(right_body, False), rights)(other, grads))
    share = kernel_call(gram_body, f32(4, LANES))(mine, other)

    sent = kernel_call(pack_body, f32(PEERS * CHUNK, LANES))(kept, away, share)
    came = all_to_all(sent.reshape(PEERS * CHUNK // 4, 4, LANES), PLANE)
    sent = kernel_call(plane_body, f32(STACK * CHUNK, LANES))(came.reshape(-1, LANES))
    came = all_to_all(sent.reshape(STACK * CHUNK // 4, 4, LANES), COLUMN)
    sent, gram = kernel_call(column_body, [rights, f32(16, LANES)])(came.reshape(-1, LANES))
    right = all_to_all(sent, PLANE)
    inverse, frame = kernel_call(
        factor_body, [f32(RANK, LANES), f32(layers, RANK, rows)], flops=1 << 28
    )(gram, mine, other)
    right, inverse, frame = lax.optimization_barrier((right.reshape(32, 8, LANES), inverse, frame))
    late = swapped(right)
    solved = (inverse, frame, weights, momentum)
    early = kernel_call(
        early_body, [f32(RANK, width), f32(RANK, rows), f32(RANK, rows)]
    )(right, *solved)
    new_basis, new_weights, new_momentum = kernel_call(
        late_body,
        [f32(layers, RANK, width), f32(layers, RANK, rows), f32(layers, RANK, rows)],
    )(late, *solved, *early)
    return tuple(jnp.swapaxes(a, 1, 2) for a in (new_weights, new_basis, new_momentum))


def solution(mesh):
    fine = Mesh(mesh.devices.reshape(tuple(SIZES.values())), tuple(SIZES))
    sharded = P(None, MODEL, REPLICA)
    return jax.shard_map(
        shards,
        mesh=fine,
        in_specs=(P(REPLICA, None, MODEL, None), P(), sharded, sharded),
        out_specs=(sharded, P(), sharded),
        check_vma=False,
    )
```

```python
import functools

import jax
import jax.numpy as jnp
from jax import lax
from jax.experimental import pallas as pl
from jax.experimental.pallas import tpu as pltpu
from jax.sharding import Mesh
from jax.sharding import PartitionSpec as P

RANK = 32
LANES = 128
SIZES = {"zlo": 4, "y": 4, "core": 2, "zhi": 2, "x": 4}
REPLICA = ("zlo", "y", "core")
MODEL = ("zhi", "x")
PLANE = ("y", "x")
COLUMN = ("zlo", "zhi")
REPLICAS, PEERS, STACK = 32, 16, 8
CHUNK = 20
EXACT = lax.Precision.HIGHEST
VMEM_LIMIT = 24 * 1024 * 1024


def kernel_call(body, outs, flops=1 << 20, moved=1 << 18):
    many = isinstance(outs, (list, tuple))
    count = len(outs) if many else 1
    spec = pl.BlockSpec(memory_space=pltpu.VMEM)
    return lambda *args: pl.pallas_call(
        body,
        out_shape=outs,
        in_specs=[spec] * len(args),
        out_specs=[spec] * count if many else spec,
        compiler_params=pltpu.CompilerParams(vmem_limit_bytes=VMEM_LIMIT),
        cost_estimate=pl.CostEstimate(flops=flops, bytes_accessed=moved, transcendentals=0),
    )(*args)


def f32(*shape):
    return jax.ShapeDtypeStruct(shape, jnp.float32)


def joined(ref, rows, columns):
    return jnp.concatenate(
        [
            jnp.concatenate([ref[t * columns + j] for j in range(columns)], axis=1)
            for t in range(rows)
        ],
        axis=0,
    )


def lane_of(shape):
    return lax.broadcasted_iota(jnp.int32, shape, 1)


def row_of(shape):
    return lax.broadcasted_iota(jnp.int32, shape, 0)


def core():
    return lax.axis_index("core")


ROWS = 128


def left_of(basis, grads):
    return lax.dot_general(
        basis.astype(jnp.bfloat16),
        grads,
        (((1,), (1,)), ((), ())),
        preferred_element_type=jnp.float32,
    )


def first_body(basis_hbm, grads_hbm, out_ref, grads_ref, basis_ref, sems):
    c = core()
    whole = pltpu.make_async_copy(basis_hbm, basis_ref, sems.at[8])
    whole.start()
    copies = []
    for k in range(8):
        at = (1 - c if k < 4 else c, pl.ds(ROWS * (k % 4), ROWS))
        copies.append(pltpu.make_async_copy(grads_hbm.at[at], grads_ref.at[at], sems.at[k]))
        copies[-1].start()
    whole.wait()
    for j in range(4):
        copies[j].wait()
        left = left_of(basis_ref[1 - c], grads_ref[1 - c, ROWS * j : ROWS * (j + 1)])
        for t in range(4):
            out_ref[4 * t + j] = left[8 * t : 8 * t + 8]
    for k in range(4, 8):
        copies[k].wait()


def left_body(basis_ref, grads_ref, out_ref):
    left = left_of(basis_ref[core()], grads_ref[core()])
    for t in range(4):
        for j in range(4):
            out_ref[4 * t + j] = left[8 * t : 8 * t + 8, LANES * j : LANES * j + LANES]


def right_body(mine, left_ref, grads_ref, out_ref):
    layer = core() if mine else 1 - core()
    right = jnp.dot(
        joined(left_ref, 4, 4).astype(jnp.bfloat16),
        grads_ref[layer],
        preferred_element_type=jnp.float32,
    )
    for t in range(4):
        for j in range(8):
            d, h = divmod(8 * t + j, 2)
            out_ref[d, 8 * h : 8 * h + 8] = right[8 * t : 8 * t + 8, LANES * j : LANES * j + LANES]


def by_layer(mine_ref, other_ref):
    mine, other = joined(mine_ref, 4, 4), joined(other_ref, 4, 4)
    first = core() == 0
    return jnp.where(first, mine, other), jnp.where(first, other, mine)


def gram_body(mine_ref, other_ref, share_ref):
    left = jnp.concatenate(by_layer(mine_ref, other_ref), axis=0)
    twice = jnp.concatenate([left, left], axis=0)
    gram = lax.dot_general(
        left, twice, (((1,), (1,)), ((), ())), precision=EXACT, preferred_element_type=jnp.float32
    )
    lane = lane_of((16, LANES))
    packed = jnp.where(
        lane < 32,
        gram[0:16],
        jnp.where(lane < 64, gram[32:48], jnp.where(lane < 96, gram[16:32], gram[48:64])),
    )
    share_ref[...] = picked([packed[4 * s : 4 * s + 4] for s in range(4)], lax.axis_index("y"))


def picked(values, index):
    out = values[0]
    for s in range(1, len(values)):
        out = jnp.where(index == s, values[s], out)
    return out


def pack_body(mine_ref, other_ref, share_ref, out_ref):
    share = share_ref[...]
    for d in range(PEERS):
        out_ref[CHUNK * d : CHUNK * d + 16] = mine_ref[d] + other_ref[d]
        out_ref[CHUNK * d + 16 : CHUNK * d + CHUNK] = share


def plane_body(in_ref, out_ref):
    total = in_ref[0:16]
    for s in range(1, PEERS):
        total = total + in_ref[CHUNK * s : CHUNK * s + 16]
    parts = []
    for y in range(4):
        part = None
        for x in range(4):
            at = CHUNK * (4 * y + x) + 16
            piece = in_ref[at : at + 4]
            part = piece if part is None else part + piece
        parts.append(part)
    share = picked(parts, lax.axis_index("zlo"))
    for z in range(STACK):
        out_ref[CHUNK * z : CHUNK * z + 16] = total
        out_ref[CHUNK * z + 16 : CHUNK * z + CHUNK] = share


def column_body(in_ref, out_ref, gram_ref):
    total = in_ref[0:16]
    for s in range(1, STACK):
        total = total + in_ref[CHUNK * s : CHUNK * s + 16]
    for d in range(PEERS):
        out_ref[d] = total
    for q in range(4):
        at = 2 * CHUNK * q + 16
        gram_ref[4 * q : 4 * q + 4] = in_ref[at : at + 4] + in_ref[at + CHUNK : at + CHUNK + 4]


def factor_body(gram_ref, mine_ref, other_ref, inverse_ref, frame_ref):
    packed = gram_ref[...]
    shape = (RANK, LANES)
    lane, row = lane_of(shape), row_of(shape)
    gram = jnp.concatenate([packed, pltpu.roll(packed, 64, 1)], axis=0)
    first = (lane // RANK) % 2 == 0
    unit = (lane % RANK) == row
    diagonal = jnp.where(unit & (lane < 64), gram, 0.0)
    mean0 = jnp.sum(jnp.where(first, diagonal, 0.0)) * (1.0 / RANK)
    mean1 = jnp.sum(jnp.where(first, 0.0, diagonal)) * (1.0 / RANK)
    ridge = 0.001 * jnp.where(first, mean0, mean1)
    work = jnp.where(lane < 64, gram, 0.0) + jnp.where(unit, jnp.where(lane < 64, ridge, 1.0), 0.0)
    pivots = jnp.ones(shape, jnp.float32)
    for k in range(RANK):
        column = jnp.where(first, work[:, k : k + 1], work[:, RANK + k : RANK + k + 1])
        pivot = column[k : k + 1]
        pivots = jnp.where(row == k, column, pivots)
        if k + 1 < RANK:
            step = work[k : k + 1] / pivot
            work = work - jnp.where(row > k, column * step, 0.0)
    inverse = pltpu.roll(work / jnp.sqrt(pivots), 64, 1)
    inverse_ref[...] = inverse
    left = by_layer(mine_ref, other_ref)
    for l in range(2):
        frame_ref[l] = (
            jnp.dot(
                inverse[:, l * RANK : (l + 1) * RANK],
                left[l],
                precision=EXACT,
                preferred_element_type=jnp.float32,
            )
            * (1.0 / REPLICAS)
        )


def settle(layer, right_ref, inverse_ref, frame_ref, weights_ref, momentum_ref):
    place = (lax.axis_index("zlo") * 4 + lax.axis_index("y")) * 2 + core()
    block = place // 4
    shift = (4 - place % 4) * 32
    square = jnp.zeros((8, LANES), jnp.float32)
    for i in range(32):
        tile = right_ref[i]
        square = square + tile * tile
    scale = lax.rsqrt(jnp.sum(square) * (1.0 / (RANK * 1024)) + 1e-12)
    own = jnp.concatenate([right_ref[8 * t + block] for t in range(4)], axis=0)
    inverse = inverse_ref[...]
    inverse = jnp.where(layer == 0, inverse[:, :RANK], inverse[:, RANK : 2 * RANK])
    half = jnp.dot(inverse, own, precision=EXACT, preferred_element_type=jnp.float32)
    half = pltpu.roll(half, shift, 1)[:, :RANK]
    change = lax.dot_general(
        half,
        frame_ref[layer],
        (((0,), (0,)), ((), ())),
        precision=EXACT,
        preferred_element_type=jnp.float32,
    )
    new = 0.9 * momentum_ref[layer] + change
    return scale, new, weights_ref[layer] - 0.02 * new


def scaled(right_ref, scale, basis_ref, layer):
    for t in range(4):
        for j in range(8):
            at = (slice(8 * t, 8 * t + 8), slice(LANES * j, LANES * j + LANES))
            at = at if layer is None else (layer, *at)
            basis_ref[at] = right_ref[8 * t + j] * scale


def early_body(right_ref, inverse_ref, frame_ref, weights_ref, momentum_ref, basis_ref, w_ref, m_ref):
    scale, new, weights = settle(core(), right_ref, inverse_ref, frame_ref, weights_ref, momentum_ref)
    scaled(right_ref, scale, basis_ref, None)
    m_ref[...] = new
    w_ref[...] = weights


def late_body(
    right_ref, inverse_ref, frame_ref, weights_ref, momentum_ref, b_ref, w_ref, m_ref,
    basis_ref, new_w_ref, new_m_ref,
):
    c = core()
    basis_ref[c] = b_ref[...]
    new_w_ref[c] = w_ref[...]
    new_m_ref[c] = m_ref[...]
    layer = 1 - c
    scale, new, weights = settle(layer, right_ref, inverse_ref, frame_ref, weights_ref, momentum_ref)
    scaled(right_ref, scale, basis_ref, layer)
    new_m_ref[layer] = new
    new_w_ref[layer] = weights


def swapped(value):
    return lax.ppermute(value, "core", [(0, 1), (1, 0)])


def all_to_all(value, axes):
    return lax.all_to_all(value, axes, 0, 0, tiled=True)


def shards(layer_grads, last_basis, layer_weights, momentum):
    grads = layer_grads[0]
    layers, rows, width = grads.shape
    basis = jnp.swapaxes(last_basis, 1, 2)
    weights, momentum = jnp.swapaxes(layer_weights, 1, 2), jnp.swapaxes(momentum, 1, 2)
    lefts, rights = f32(PEERS, 8, LANES), f32(PEERS, 16, LANES)

    anywhere = pl.BlockSpec(memory_space=pltpu.HBM)
    local = pl.BlockSpec(memory_space=pltpu.VMEM)
    away, grads, basis = pl.pallas_call(
        first_body,
        out_shape=[lefts, jax.ShapeDtypeStruct(grads.shape, grads.dtype), f32(*basis.shape)],
        in_specs=[anywhere] * 2,
        out_specs=[local] * 3,
        scratch_shapes=[pltpu.SemaphoreType.DMA((9,))],
        compiler_params=pltpu.CompilerParams(vmem_limit_bytes=VMEM_LIMIT),
        cost_estimate=pl.CostEstimate(flops=1 << 20, bytes_accessed=1 << 18, transcendentals=0),
    )(*(pltpu.with_memory_space_constraint(a, pltpu.HBM) for a in (basis, grads)))
    away = swapped(away)
    mine = kernel_call(left_body, lefts)(basis, grads) + away
    for axis, bit in (("y", 1), ("y", 3), ("zlo", 1), ("zlo", 2)):
        mine = mine + lax.ppermute(mine, axis, [(i, i ^ bit) for i in range(SIZES[axis])])
    other = swapped(mine)
    kept = kernel_call(functools.partial(right_body, True), rights)(mine, grads)
    kept, other = lax.optimization_barrier((kept, other))
    away = swapped(kernel_call(functools.partial(right_body, False), rights)(other, grads))
    share = kernel_call(gram_body, f32(4, LANES))(mine, other)

    sent = kernel_call(pack_body, f32(PEERS * CHUNK, LANES))(kept, away, share)
    came = all_to_all(sent.reshape(PEERS * CHUNK // 4, 4, LANES), PLANE)
    sent = kernel_call(plane_body, f32(STACK * CHUNK, LANES))(came.reshape(-1, LANES))
    came = all_to_all(sent.reshape(STACK * CHUNK // 4, 4, LANES), COLUMN)
    sent, gram = kernel_call(column_body, [rights, f32(16, LANES)])(came.reshape(-1, LANES))
    right = all_to_all(sent, PLANE)
    inverse, frame = kernel_call(
        factor_body, [f32(RANK, LANES), f32(layers, RANK, rows)], flops=1 << 28
    )(gram, mine, other)
    right, inverse, frame = lax.optimization_barrier((right.reshape(32, 8, LANES), inverse, frame))
    late = swapped(right)
    solved = (inverse, frame, weights, momentum)
    early = kernel_call(
        early_body, [f32(RANK, width), f32(RANK, rows), f32(RANK, rows)]
    )(right, *solved)
    new_basis, new_weights, new_momentum = kernel_call(
        late_body,
        [f32(layers, RANK, width), f32(layers, RANK, rows), f32(layers, RANK, rows)],
    )(late, *solved, *early)
    return tuple(jnp.swapaxes(a, 1, 2) for a in (new_weights, new_basis, new_momentum))


def solution(mesh):
    fine = Mesh(mesh.devices.reshape(tuple(SIZES.values())), tuple(SIZES))
    sharded = P(None, MODEL, REPLICA)
    return jax.shard_map(
        shards,
        mesh=fine,
        in_specs=(P(REPLICA, None, MODEL, None), P(), sharded, sharded),
        out_specs=(sharded, P(), sharded),
        check_vma=False,
    )
```

```python
import functools

import jax
import jax.numpy as jnp
from jax import lax
from jax.experimental import pallas as pl
from jax.experimental.pallas import tpu as pltpu
from jax.sharding import Mesh
from jax.sharding import PartitionSpec as P

RANK = 32
LANES = 128
SIZES = {"zlo": 4, "y": 4, "core": 2, "zhi": 2, "x": 4}
REPLICA = ("zlo", "y", "core")
MODEL = ("zhi", "x")
PLANE = ("y", "x")
COLUMN = ("zlo", "zhi")
REPLICAS, PEERS, STACK = 32, 16, 8
CHUNK = 20
EXACT = lax.Precision.HIGHEST
VMEM_LIMIT = 24 * 1024 * 1024


def kernel_call(body, outs, flops=1 << 20, moved=1 << 18):
    many = isinstance(outs, (list, tuple))
    count = len(outs) if many else 1
    spec = pl.BlockSpec(memory_space=pltpu.VMEM)
    return lambda *args: pl.pallas_call(
        body,
        out_shape=outs,
        in_specs=[spec] * len(args),
        out_specs=[spec] * count if many else spec,
        compiler_params=pltpu.CompilerParams(vmem_limit_bytes=VMEM_LIMIT),
        cost_estimate=pl.CostEstimate(flops=flops, bytes_accessed=moved, transcendentals=0),
    )(*args)


def f32(*shape):
    return jax.ShapeDtypeStruct(shape, jnp.float32)


def joined(ref, rows, columns):
    return jnp.concatenate(
        [
            jnp.concatenate([ref[t * columns + j] for j in range(columns)], axis=1)
            for t in range(rows)
        ],
        axis=0,
    )


def lane_of(shape):
    return lax.broadcasted_iota(jnp.int32, shape, 1)


def row_of(shape):
    return lax.broadcasted_iota(jnp.int32, shape, 0)


def core():
    return lax.axis_index("core")


ROWS = 128


def left_of(basis, grads):
    return lax.dot_general(
        basis.astype(jnp.bfloat16),
        grads,
        (((1,), (1,)), ((), ())),
        preferred_element_type=jnp.float32,
    )


def left_body(mine, basis_hbm, grads_hbm, out_ref, grads_ref, basis_ref, sems):
    layer = core() if mine else 1 - core()
    pieces = [pltpu.make_async_copy(basis_hbm.at[layer], basis_ref, sems.at[4])]
    for j in range(4):
        rows = pl.ds(ROWS * j, ROWS)
        pieces.append(
            pltpu.make_async_copy(grads_hbm.at[layer, rows], grads_ref.at[rows], sems.at[j])
        )
    for piece in pieces:
        piece.start()
    pieces[0].wait()
    basis = basis_ref[...]
    for j in range(4):
        pieces[1 + j].wait()
        left = left_of(basis, grads_ref[ROWS * j : ROWS * (j + 1)])
        for t in range(4):
            out_ref[4 * t + j] = left[8 * t : 8 * t + 8]


def right_body(left_ref, grads_ref, out_ref):
    right = jnp.dot(
        joined(left_ref, 4, 4).astype(jnp.bfloat16),
        grads_ref[...],
        preferred_element_type=jnp.float32,
    )
    for t in range(4):
        for j in range(8):
            d, h = divmod(8 * t + j, 2)
            out_ref[d, 8 * h : 8 * h + 8] = right[8 * t : 8 * t + 8, LANES * j : LANES * j + LANES]


def by_layer(mine_ref, other_ref):
    mine, other = joined(mine_ref, 4, 4), joined(other_ref, 4, 4)
    first = core() == 0
    return jnp.where(first, mine, other), jnp.where(first, other, mine)


def gram_body(mine_ref, other_ref, share_ref):
    left = jnp.concatenate(by_layer(mine_ref, other_ref), axis=0)
    twice = jnp.concatenate([left, left], axis=0)
    gram = lax.dot_general(
        left, twice, (((1,), (1,)), ((), ())), precision=EXACT, preferred_element_type=jnp.float32
    )
    lane = lane_of((16, LANES))
    packed = jnp.where(
        lane < 32,
        gram[0:16],
        jnp.where(lane < 64, gram[32:48], jnp.where(lane < 96, gram[16:32], gram[48:64])),
    )
    share_ref[...] = picked([packed[4 * s : 4 * s + 4] for s in range(4)], lax.axis_index("y"))


def picked(values, index):
    out = values[0]
    for s in range(1, len(values)):
        out = jnp.where(index == s, values[s], out)
    return out


def pack_body(mine_ref, other_ref, share_ref, out_ref):
    share = share_ref[...]
    for d in range(PEERS):
        out_ref[CHUNK * d : CHUNK * d + 16] = mine_ref[d] + other_ref[d]
        out_ref[CHUNK * d + 16 : CHUNK * d + CHUNK] = share


def plane_body(in_ref, out_ref):
    total = in_ref[0:16]
    for s in range(1, PEERS):
        total = total + in_ref[CHUNK * s : CHUNK * s + 16]
    parts = []
    for y in range(4):
        part = None
        for x in range(4):
            at = CHUNK * (4 * y + x) + 16
            piece = in_ref[at : at + 4]
            part = piece if part is None else part + piece
        parts.append(part)
    share = picked(parts, lax.axis_index("zlo"))
    for z in range(STACK):
        out_ref[CHUNK * z : CHUNK * z + 16] = total
        out_ref[CHUNK * z + 16 : CHUNK * z + CHUNK] = share


def column_body(in_ref, out_ref, gram_ref):
    total = in_ref[0:16]
    for s in range(1, STACK):
        total = total + in_ref[CHUNK * s : CHUNK * s + 16]
    for d in range(PEERS):
        out_ref[d] = total
    for q in range(4):
        at = 2 * CHUNK * q + 16
        gram_ref[4 * q : 4 * q + 4] = in_ref[at : at + 4] + in_ref[at + CHUNK : at + CHUNK + 4]


def factor_body(gram_ref, mine_ref, other_ref, inverse_ref, frame_ref):
    packed = gram_ref[...]
    shape = (RANK, LANES)
    lane, row = lane_of(shape), row_of(shape)
    gram = jnp.concatenate([packed, pltpu.roll(packed, 64, 1)], axis=0)
    first = (lane // RANK) % 2 == 0
    unit = (lane % RANK) == row
    diagonal = jnp.where(unit & (lane < 64), gram, 0.0)
    mean0 = jnp.sum(jnp.where(first, diagonal, 0.0)) * (1.0 / RANK)
    mean1 = jnp.sum(jnp.where(first, 0.0, diagonal)) * (1.0 / RANK)
    ridge = 0.001 * jnp.where(first, mean0, mean1)
    work = jnp.where(lane < 64, gram, 0.0) + jnp.where(unit, jnp.where(lane < 64, ridge, 1.0), 0.0)
    pivots = jnp.ones(shape, jnp.float32)
    for k in range(RANK):
        column = jnp.where(first, work[:, k : k + 1], work[:, RANK + k : RANK + k + 1])
        pivot = column[k : k + 1]
        pivots = jnp.where(row == k, column, pivots)
        if k + 1 < RANK:
            step = work[k : k + 1] / pivot
            work = work - jnp.where(row > k, column * step, 0.0)
    inverse = pltpu.roll(work / jnp.sqrt(pivots), 64, 1)
    inverse_ref[...] = inverse
    left = by_layer(mine_ref, other_ref)
    for l in range(2):
        frame_ref[l] = (
            jnp.dot(
                inverse[:, l * RANK : (l + 1) * RANK],
                left[l],
                precision=EXACT,
                preferred_element_type=jnp.float32,
            )
            * (1.0 / REPLICAS)
        )


def finish_body(mine, right_ref, inverse_ref, frame_ref, weights_ref, momentum_ref, *refs):
    basis_hbm, w_hbm, m_hbm, basis_ref, w_ref, m_ref, sems = refs[-7:]
    layer = core() if mine else 1 - core()
    place = (lax.axis_index("zlo") * 4 + lax.axis_index("y")) * 2 + core()
    block = place // 4
    shift = (4 - place % 4) * 32
    copies = []

    def send(source, target):
        copies.append(pltpu.make_async_copy(source, target, sems.at[len(copies)]))
        copies[-1].start()

    own = jnp.concatenate([right_ref[8 * t + block] for t in range(4)], axis=0)
    inverse = inverse_ref[...]
    inverse = jnp.where(layer == 0, inverse[:, :RANK], inverse[:, RANK : 2 * RANK])
    half = jnp.dot(inverse, own, precision=EXACT, preferred_element_type=jnp.float32)
    half = pltpu.roll(half, shift, 1)[:, :RANK]
    squares = [jnp.zeros((8, LANES), jnp.float32)] * 4
    for i in range(32):
        tile = right_ref[i]
        squares[i % 4] = squares[i % 4] + tile * tile
    square = (squares[0] + squares[1]) + (squares[2] + squares[3])
    scale = lax.rsqrt(jnp.sum(square) * (1.0 / (RANK * 1024)) + 1e-12)
    for t in range(4):
        rows = slice(8 * t, 8 * t + 8)
        for j in range(8):
            basis_ref[rows, LANES * j : LANES * j + LANES] = right_ref[8 * t + j] * scale
        send(basis_ref.at[rows], basis_hbm.at[layer, rows])
    change = lax.dot_general(
        half,
        frame_ref[layer],
        (((0,), (0,)), ((), ())),
        precision=EXACT,
        preferred_element_type=jnp.float32,
    )
    new = 0.9 * momentum_ref[layer] + change
    m_ref[...] = new
    send(m_ref, m_hbm.at[layer])
    w_ref[...] = weights_ref[layer] - 0.02 * new
    send(w_ref, w_hbm.at[layer])
    for copy in copies:
        copy.wait()


def finish(right, solved, partial, width, rows):
    local, far = pl.BlockSpec(memory_space=pltpu.VMEM), pl.BlockSpec(memory_space=pltpu.HBM)
    first = not partial
    return pl.pallas_call(
        functools.partial(finish_body, first),
        out_shape=[f32(2, RANK, width), f32(2, RANK, rows), f32(2, RANK, rows)],
        in_specs=[local] * 5 + [far] * len(partial),
        out_specs=[far] * 3,
        scratch_shapes=[
            pltpu.VMEM((RANK, width), jnp.float32),
            pltpu.VMEM((RANK, rows), jnp.float32),
            pltpu.VMEM((RANK, rows), jnp.float32),
            pltpu.SemaphoreType.DMA((6,)),
        ],
        input_output_aliases={} if first else {5: 0, 6: 1, 7: 2},
        compiler_params=pltpu.CompilerParams(vmem_limit_bytes=VMEM_LIMIT),
        cost_estimate=pl.CostEstimate(flops=1 << 20, bytes_accessed=1 << 18, transcendentals=0),
    )(right, *solved, *partial)


def part_left(mine, basis, grads):
    far, local = pl.BlockSpec(memory_space=pltpu.HBM), pl.BlockSpec(memory_space=pltpu.VMEM)
    return pl.pallas_call(
        functools.partial(left_body, mine),
        out_shape=[f32(PEERS, 8, LANES), jax.ShapeDtypeStruct(grads.shape[1:], grads.dtype)],
        in_specs=[far] * 2,
        out_specs=[local] * 2,
        scratch_shapes=[pltpu.VMEM(basis.shape[1:], jnp.float32), pltpu.SemaphoreType.DMA((5,))],
        compiler_params=pltpu.CompilerParams(vmem_limit_bytes=VMEM_LIMIT),
        cost_estimate=pl.CostEstimate(flops=1 << 20, bytes_accessed=1 << 18, transcendentals=0),
    )(basis, grads)


DOUBLING = ((4, 8, 1, 3), (1, 3, 4, 8))


def doubled(value, step):
    flips = []
    for i in range(REPLICAS):
        place, c = divmod(i, 2)
        bit = DOUBLING[c][step]
        flips.append((i, (place ^ bit) * 2 + c))
    return value + lax.ppermute(value, REPLICA, flips)


def swapped(value):
    return lax.ppermute(value, "core", [(0, 1), (1, 0)])


def all_to_all(value, axes):
    return lax.all_to_all(value, axes, 0, 0, tiled=True)


def shards(layer_grads, last_basis, layer_weights, momentum):
    grads = layer_grads[0]
    layers, rows, width = grads.shape
    basis = jnp.swapaxes(last_basis, 1, 2)
    weights, momentum = jnp.swapaxes(layer_weights, 1, 2), jnp.swapaxes(momentum, 1, 2)
    lefts, rights = f32(PEERS, 8, LANES), f32(PEERS, 16, LANES)

    far = [pltpu.with_memory_space_constraint(a, pltpu.HBM) for a in (basis, grads)]
    away, other_grads = part_left(False, *far)
    away = swapped(away)
    mine, own_grads = part_left(True, *far)
    mine = mine + away
    for step in range(4):
        mine = doubled(mine, step)
    other = swapped(mine)
    kept = kernel_call(right_body, rights)(mine, own_grads)
    kept, other = lax.optimization_barrier((kept, other))
    away = swapped(kernel_call(right_body, rights)(other, other_grads))
    share = kernel_call(gram_body, f32(4, LANES))(mine, other)

    sent = kernel_call(pack_body, f32(PEERS * CHUNK, LANES))(kept, away, share)
    came = all_to_all(sent.reshape(PEERS * CHUNK // 4, 4, LANES), PLANE)
    sent = kernel_call(plane_body, f32(STACK * CHUNK, LANES))(came.reshape(-1, LANES))
    came = all_to_all(sent.reshape(STACK * CHUNK // 4, 4, LANES), COLUMN)
    sent, gram = kernel_call(column_body, [rights, f32(16, LANES)])(came.reshape(-1, LANES))
    right = all_to_all(sent, PLANE)
    inverse, frame = kernel_call(
        factor_body, [f32(RANK, LANES), f32(layers, RANK, rows)], flops=1 << 28
    )(gram, mine, other)
    right, inverse, frame = lax.optimization_barrier((right.reshape(32, 8, LANES), inverse, frame))
    late = swapped(right)
    solved = (inverse, frame, weights, momentum)
    early = finish(right, solved, (), width, rows)
    new_basis, new_weights, new_momentum = finish(late, solved, early, width, rows)
    return tuple(jnp.swapaxes(a, 1, 2) for a in (new_weights, new_basis, new_momentum))


def solution(mesh):
    fine = Mesh(mesh.devices.reshape(tuple(SIZES.values())), tuple(SIZES))
    sharded = P(None, MODEL, REPLICA)
    return jax.shard_map(
        shards,
        mesh=fine,
        in_specs=(P(REPLICA, None, MODEL, None), P(), sharded, sharded),
        out_specs=(sharded, P(), sharded),
        check_vma=False,
    )
```

```python
import functools

import jax
import jax.numpy as jnp
from jax import lax
from jax.experimental import pallas as pl
from jax.experimental.pallas import tpu as pltpu
from jax.sharding import Mesh
from jax.sharding import PartitionSpec as P

RANK = 32
LANES = 128
SIZES = {"zlo": 4, "y": 4, "core": 2, "zhi": 2, "x": 4}
REPLICA = ("zlo", "y", "core")
MODEL = ("zhi", "x")
PLANE = ("y", "x")
COLUMN = ("zlo", "zhi")
REPLICAS, PEERS, STACK = 32, 16, 8
CHUNK = 20
BLOCK = 16
EXACT = lax.Precision.HIGHEST
VMEM_LIMIT = 24 * 1024 * 1024


def kernel_call(body, outs, flops=1 << 20, moved=1 << 18):
    many = isinstance(outs, (list, tuple))
    count = len(outs) if many else 1
    spec = pl.BlockSpec(memory_space=pltpu.VMEM)
    return lambda *args: pl.pallas_call(
        body,
        out_shape=outs,
        in_specs=[spec] * len(args),
        out_specs=[spec] * count if many else spec,
        compiler_params=pltpu.CompilerParams(vmem_limit_bytes=VMEM_LIMIT),
        cost_estimate=pl.CostEstimate(flops=flops, bytes_accessed=moved, transcendentals=0),
    )(*args)


def f32(*shape):
    return jax.ShapeDtypeStruct(shape, jnp.float32)


def joined(ref, rows, columns):
    return jnp.concatenate(
        [
            jnp.concatenate([ref[t * columns + j] for j in range(columns)], axis=1)
            for t in range(rows)
        ],
        axis=0,
    )


def lane_of(shape):
    return lax.broadcasted_iota(jnp.int32, shape, 1)


def row_of(shape):
    return lax.broadcasted_iota(jnp.int32, shape, 0)


def core():
    return lax.axis_index("core")


ROWS = 128


def left_of(basis, grads):
    return lax.dot_general(
        basis.astype(jnp.bfloat16),
        grads,
        (((1,), (1,)), ((), ())),
        preferred_element_type=jnp.float32,
    )


def first_body(basis_hbm, grads_hbm, out_ref, grads_ref, basis_ref, sems):
    c = core()
    whole = pltpu.make_async_copy(basis_hbm, basis_ref, sems.at[8])
    whole.start()
    copies = []
    for k in range(8):
        at = (1 - c if k < 4 else c, pl.ds(ROWS * (k % 4), ROWS))
        copies.append(pltpu.make_async_copy(grads_hbm.at[at], grads_ref.at[at], sems.at[k]))
        copies[-1].start()
    whole.wait()
    for j in range(4):
        copies[j].wait()
        left = left_of(basis_ref[1 - c], grads_ref[1 - c, ROWS * j : ROWS * (j + 1)])
        for t in range(4):
            out_ref[4 * t + j] = left[8 * t : 8 * t + 8]
    for k in range(4, 8):
        copies[k].wait()


def left_body(basis_ref, grads_ref, out_ref):
    left = left_of(basis_ref[core()], grads_ref[core()])
    for t in range(4):
        for j in range(4):
            out_ref[4 * t + j] = left[8 * t : 8 * t + 8, LANES * j : LANES * j + LANES]


def right_body(mine, left_ref, grads_ref, out_ref):
    layer = core() if mine else 1 - core()
    right = jnp.dot(
        joined(left_ref, 4, 4).astype(jnp.bfloat16),
        grads_ref[layer],
        preferred_element_type=jnp.float32,
    )
    for t in range(4):
        for j in range(8):
            d, h = divmod(8 * t + j, 2)
            out_ref[d, 8 * h : 8 * h + 8] = right[8 * t : 8 * t + 8, LANES * j : LANES * j + LANES]


def by_layer(mine_ref, other_ref):
    mine, other = joined(mine_ref, 4, 4), joined(other_ref, 4, 4)
    first = core() == 0
    return jnp.where(first, mine, other), jnp.where(first, other, mine)


def gram_body(mine_ref, other_ref, share_ref):
    left = jnp.concatenate(by_layer(mine_ref, other_ref), axis=0)
    twice = jnp.concatenate([left, left], axis=0)
    gram = lax.dot_general(
        left, twice, (((1,), (1,)), ((), ())), precision=EXACT, preferred_element_type=jnp.float32
    )
    lane = lane_of((16, LANES))
    packed = jnp.where(
        lane < 32,
        gram[0:16],
        jnp.where(lane < 64, gram[32:48], jnp.where(lane < 96, gram[16:32], gram[48:64])),
    )
    share_ref[...] = picked([packed[4 * s : 4 * s + 4] for s in range(4)], lax.axis_index("y"))


def picked(values, index):
    out = values[0]
    for s in range(1, len(values)):
        out = jnp.where(index == s, values[s], out)
    return out


def pack_body(mine_ref, other_ref, share_ref, out_ref):
    share = share_ref[...]
    for d in range(PEERS):
        out_ref[CHUNK * d : CHUNK * d + 16] = mine_ref[d] + other_ref[d]
        out_ref[CHUNK * d + 16 : CHUNK * d + CHUNK] = share


def plane_body(in_ref, out_ref):
    total = in_ref[0:16]
    for s in range(1, PEERS):
        total = total + in_ref[CHUNK * s : CHUNK * s + 16]
    parts = []
    for y in range(4):
        part = None
        for x in range(4):
            at = CHUNK * (4 * y + x) + 16
            piece = in_ref[at : at + 4]
            part = piece if part is None else part + piece
        parts.append(part)
    share = picked(parts, lax.axis_index("zlo"))
    for z in range(STACK):
        out_ref[CHUNK * z : CHUNK * z + 16] = total
        out_ref[CHUNK * z + 16 : CHUNK * z + CHUNK] = share


def column_body(in_ref, out_ref, gram_ref):
    total = in_ref[0:16]
    for s in range(1, STACK):
        total = total + in_ref[CHUNK * s : CHUNK * s + 16]
    for d in range(PEERS):
        out_ref[d] = total
    for q in range(4):
        at = 2 * CHUNK * q + 16
        gram_ref[4 * q : 4 * q + 4] = in_ref[at : at + 4] + in_ref[at + CHUNK : at + CHUNK + 4]


def factor_body(gram_ref, mine_ref, other_ref, inverse_ref, frame_ref):
    packed = gram_ref[...]
    turned = pltpu.roll(packed, 64, 1)
    grams = [packed[0:8], packed[8:16], turned[0:8], turned[8:16]]
    shape = (8, LANES)
    lane, row = lane_of(shape), row_of(shape)
    first = (lane // RANK) % 2 == 0
    front = lane < 64
    units = [(lane % RANK) == row + 8 * r for r in range(4)]
    diagonal = jnp.zeros(shape, jnp.float32)
    for r in range(4):
        diagonal = diagonal + jnp.where(units[r] & front, grams[r], 0.0)
    mean0 = jnp.sum(jnp.where(first, diagonal, 0.0)) * (1.0 / RANK)
    mean1 = jnp.sum(jnp.where(first, 0.0, diagonal)) * (1.0 / RANK)
    ridge = jnp.where(front, 0.001 * jnp.where(first, mean0, mean1), 1.0)
    work = [jnp.where(front, grams[r], 0.0) + jnp.where(units[r], ridge, 0.0) for r in range(4)]
    for b in range(0, RANK, BLOCK):
        columns = [
            {
                r: jnp.where(first, work[r][:, k : k + 1], work[r][:, RANK + k : RANK + k + 1])
                for r in range(b // 8, 4)
            }
            for k in range(b, b + BLOCK)
        ]
        for i in range(BLOCK):
            at, s = divmod(b + i, 8)
            pivot = columns[i][at][s : s + 1]
            inverse = 1.0 / pivot
            chosen = work[at][s : s + 1]
            ahead = {j: columns[j][at][s : s + 1] for j in range(i + 1, BLOCK)}
            for r in range(at, 4):
                factor = columns[i][r] * inverse
                if r == at:
                    factor = jnp.where(row > s, factor, 0.0)
                work[r] = work[r] - factor * chosen
                for j in ahead:
                    columns[j][r] = columns[j][r] - factor * ahead[j]
            work[at] = jnp.where(row == s, work[at] * lax.rsqrt(pivot), work[at])
    inverse = pltpu.roll(jnp.concatenate(work, axis=0), 64, 1)
    inverse_ref[...] = inverse
    left = by_layer(mine_ref, other_ref)
    for l in range(2):
        frame_ref[l] = (
            jnp.dot(
                inverse[:, l * RANK : (l + 1) * RANK],
                left[l],
                precision=EXACT,
                preferred_element_type=jnp.float32,
            )
            * (1.0 / REPLICAS)
        )


def settle(layer, right_ref, inverse_ref, frame_ref, weights_ref, momentum_ref):
    place = (lax.axis_index("zlo") * 4 + lax.axis_index("y")) * 2 + core()
    block = place // 4
    shift = (4 - place % 4) * 32
    square = jnp.zeros((8, LANES), jnp.float32)
    for i in range(32):
        tile = right_ref[i]
        square = square + tile * tile
    scale = lax.rsqrt(jnp.sum(square) * (1.0 / (RANK * 1024)) + 1e-12)
    own = jnp.concatenate([right_ref[8 * t + block] for t in range(4)], axis=0)
    inverse = inverse_ref[...]
    inverse = jnp.where(layer == 0, inverse[:, :RANK], inverse[:, RANK : 2 * RANK])
    half = jnp.dot(inverse, own, precision=EXACT, preferred_element_type=jnp.float32)
    half = pltpu.roll(half, shift, 1)[:, :RANK]
    change = lax.dot_general(
        half,
        frame_ref[layer],
        (((0,), (0,)), ((), ())),
        precision=EXACT,
        preferred_element_type=jnp.float32,
    )
    new = 0.9 * momentum_ref[layer] + change
    return scale, new, weights_ref[layer] - 0.02 * new


def scaled(right_ref, scale, basis_ref, layer):
    for t in range(4):
        for j in range(8):
            at = (slice(8 * t, 8 * t + 8), slice(LANES * j, LANES * j + LANES))
            at = at if layer is None else (layer, *at)
            basis_ref[at] = right_ref[8 * t + j] * scale


def early_body(right_ref, inverse_ref, frame_ref, weights_ref, momentum_ref, basis_ref, w_ref, m_ref):
    scale, new, weights = settle(core(), right_ref, inverse_ref, frame_ref, weights_ref, momentum_ref)
    scaled(right_ref, scale, basis_ref, None)
    m_ref[...] = new
    w_ref[...] = weights


def late_body(
    right_ref, inverse_ref, frame_ref, weights_ref, momentum_ref, b_ref, w_ref, m_ref,
    basis_ref, new_w_ref, new_m_ref,
):
    c = core()
    basis_ref[c] = b_ref[...]
    new_w_ref[c] = w_ref[...]
    new_m_ref[c] = m_ref[...]
    layer = 1 - c
    scale, new, weights = settle(layer, right_ref, inverse_ref, frame_ref, weights_ref, momentum_ref)
    scaled(right_ref, scale, basis_ref, layer)
    new_m_ref[layer] = new
    new_w_ref[layer] = weights


def swapped(value):
    return lax.ppermute(value, "core", [(0, 1), (1, 0)])


def all_to_all(value, axes):
    return lax.all_to_all(value, axes, 0, 0, tiled=True)


def shards(layer_grads, last_basis, layer_weights, momentum):
    grads = layer_grads[0]
    layers, rows, width = grads.shape
    basis = jnp.swapaxes(last_basis, 1, 2)
    weights, momentum = jnp.swapaxes(layer_weights, 1, 2), jnp.swapaxes(momentum, 1, 2)
    lefts, rights = f32(PEERS, 8, LANES), f32(PEERS, 16, LANES)

    anywhere = pl.BlockSpec(memory_space=pltpu.HBM)
    local = pl.BlockSpec(memory_space=pltpu.VMEM)
    away, grads, basis = pl.pallas_call(
        first_body,
        out_shape=[lefts, jax.ShapeDtypeStruct(grads.shape, grads.dtype), f32(*basis.shape)],
        in_specs=[anywhere] * 2,
        out_specs=[local] * 3,
        scratch_shapes=[pltpu.SemaphoreType.DMA((9,))],
        compiler_params=pltpu.CompilerParams(vmem_limit_bytes=VMEM_LIMIT),
        cost_estimate=pl.CostEstimate(flops=1 << 20, bytes_accessed=1 << 18, transcendentals=0),
    )(*(pltpu.with_memory_space_constraint(a, pltpu.HBM) for a in (basis, grads)))
    away = swapped(away)
    mine = kernel_call(left_body, lefts)(basis, grads) + away
    for axis, bit in (("y", 1), ("y", 3), ("zlo", 1), ("zlo", 2)):
        mine = mine + lax.ppermute(mine, axis, [(i, i ^ bit) for i in range(SIZES[axis])])
    other = swapped(mine)
    kept = kernel_call(functools.partial(right_body, True), rights)(mine, grads)
    kept, other = lax.optimization_barrier((kept, other))
    away = swapped(kernel_call(functools.partial(right_body, False), rights)(other, grads))
    share = kernel_call(gram_body, f32(4, LANES))(mine, other)

    sent = kernel_call(pack_body, f32(PEERS * CHUNK, LANES))(kept, away, share)
    came = all_to_all(sent.reshape(PEERS * CHUNK // 4, 4, LANES), PLANE)
    sent = kernel_call(plane_body, f32(STACK * CHUNK, LANES))(came.reshape(-1, LANES))
    came = all_to_all(sent.reshape(STACK * CHUNK // 4, 4, LANES), COLUMN)
    sent, gram = kernel_call(column_body, [rights, f32(16, LANES)])(came.reshape(-1, LANES))
    right = all_to_all(sent, PLANE)
    right, gram = lax.optimization_barrier((right.reshape(32, 8, LANES), gram))
    late = swapped(right)
    inverse, frame = kernel_call(factor_body, [f32(RANK, LANES), f32(layers, RANK, rows)])(
        gram, mine, other
    )
    solved = (inverse, frame, weights, momentum)
    early = kernel_call(
        early_body, [f32(RANK, width), f32(RANK, rows), f32(RANK, rows)]
    )(right, *solved)
    new_basis, new_weights, new_momentum = kernel_call(
        late_body,
        [f32(layers, RANK, width), f32(layers, RANK, rows), f32(layers, RANK, rows)],
    )(late, *solved, *early)
    return tuple(jnp.swapaxes(a, 1, 2) for a in (new_weights, new_basis, new_momentum))


def solution(mesh):
    fine = Mesh(mesh.devices.reshape(tuple(SIZES.values())), tuple(SIZES))
    sharded = P(None, MODEL, REPLICA)
    return jax.shard_map(
        shards,
        mesh=fine,
        in_specs=(P(REPLICA, None, MODEL, None), P(), sharded, sharded),
        out_specs=(sharded, P(), sharded),
        check_vma=False,
    )
```

```python
import functools

import jax
import jax.numpy as jnp
from jax import lax
from jax.experimental import pallas as pl
from jax.experimental.pallas import tpu as pltpu
from jax.sharding import Mesh
from jax.sharding import PartitionSpec as P

RANK = 32
LANES = 128
SIZES = {"zlo": 4, "y": 4, "core": 2, "zhi": 2, "x": 4}
REPLICA = ("zlo", "y", "core")
MODEL = ("zhi", "x")
PLANE = ("y", "x")
COLUMN = ("zlo", "zhi")
REPLICAS, PEERS, STACK = 32, 16, 8
CHUNK = 20
BLOCK = 16
EXACT = lax.Precision.HIGHEST
VMEM_LIMIT = 24 * 1024 * 1024


def kernel_call(body, outs, flops=1 << 20, moved=1 << 18):
    many = isinstance(outs, (list, tuple))
    count = len(outs) if many else 1
    spec = pl.BlockSpec(memory_space=pltpu.VMEM)
    return lambda *args: pl.pallas_call(
        body,
        out_shape=outs,
        in_specs=[spec] * len(args),
        out_specs=[spec] * count if many else spec,
        compiler_params=pltpu.CompilerParams(vmem_limit_bytes=VMEM_LIMIT),
        cost_estimate=pl.CostEstimate(flops=flops, bytes_accessed=moved, transcendentals=0),
    )(*args)


def f32(*shape):
    return jax.ShapeDtypeStruct(shape, jnp.float32)


def joined(ref, rows, columns):
    return jnp.concatenate(
        [
            jnp.concatenate([ref[t * columns + j] for j in range(columns)], axis=1)
            for t in range(rows)
        ],
        axis=0,
    )


def lane_of(shape):
    return lax.broadcasted_iota(jnp.int32, shape, 1)


def row_of(shape):
    return lax.broadcasted_iota(jnp.int32, shape, 0)


def core():
    return lax.axis_index("core")


def held():
    return (core() + lax.axis_index("y") + lax.axis_index("zlo")) % 2


WIDE = 256


def left_of(basis, grads):
    return lax.dot_general(
        basis.astype(jnp.bfloat16),
        grads,
        (((1,), (1,)), ((), ())),
        preferred_element_type=jnp.float32,
    )


def put_left(left, out_ref):
    for t in range(4):
        for j in range(4):
            out_ref[4 * t + j] = left[8 * t : 8 * t + 8, LANES * j : LANES * j + LANES]


def first_body(basis_hbm, grads_hbm, out_ref, grads_ref, basis_ref, sems):
    h = held()
    whole = pltpu.make_async_copy(basis_hbm, basis_ref, sems.at[8])
    whole.start()
    copies = []
    for k in range(8):
        at = (1 - h if k < 4 else h, slice(None), pl.ds(WIDE * (k % 4), WIDE))
        copies.append(pltpu.make_async_copy(grads_hbm.at[at], grads_ref.at[at], sems.at[k]))
        copies[-1].start()
    whole.wait()
    left = jnp.zeros((RANK, grads_ref.shape[1]), jnp.float32)
    for j in range(4):
        copies[j].wait()
        columns = slice(WIDE * j, WIDE * (j + 1))
        left = left + left_of(basis_ref[1 - h, :, columns], grads_ref[1 - h, :, columns])
    put_left(left, out_ref)
    for k in range(4, 8):
        copies[k].wait()


def left_body(basis_ref, grads_ref, out_ref):
    h = held()
    put_left(left_of(basis_ref[h], grads_ref[h]), out_ref)


def right_body(kept, mine_ref, other_ref, grads_ref, out_ref):
    layer = core() if kept else 1 - core()
    left = jnp.where(layer == held(), joined(mine_ref, 4, 4), joined(other_ref, 4, 4))
    right = jnp.dot(
        left.astype(jnp.bfloat16),
        grads_ref[layer],
        preferred_element_type=jnp.float32,
    )
    for t in range(4):
        for j in range(8):
            d, h = divmod(8 * t + j, 2)
            out_ref[d, 8 * h : 8 * h + 8] = right[8 * t : 8 * t + 8, LANES * j : LANES * j + LANES]


def by_layer(mine_ref, other_ref):
    mine, other = joined(mine_ref, 4, 4), joined(other_ref, 4, 4)
    first = held() == 0
    return jnp.where(first, mine, other), jnp.where(first, other, mine)


def gram_body(mine_ref, other_ref, share_ref):
    left = jnp.concatenate(by_layer(mine_ref, other_ref), axis=0)
    twice = jnp.concatenate([left, left], axis=0)
    gram = lax.dot_general(
        left, twice, (((1,), (1,)), ((), ())), precision=EXACT, preferred_element_type=jnp.float32
    )
    lane = lane_of((16, LANES))
    packed = jnp.where(
        lane < 32,
        gram[0:16],
        jnp.where(lane < 64, gram[32:48], jnp.where(lane < 96, gram[16:32], gram[48:64])),
    )
    share_ref[...] = picked([packed[4 * s : 4 * s + 4] for s in range(4)], lax.axis_index("y"))


def picked(values, index):
    out = values[0]
    for s in range(1, len(values)):
        out = jnp.where(index == s, values[s], out)
    return out


def pack_body(mine_ref, other_ref, share_ref, out_ref):
    share = share_ref[...]
    for d in range(PEERS):
        out_ref[CHUNK * d : CHUNK * d + 16] = mine_ref[d] + other_ref[d]
        out_ref[CHUNK * d + 16 : CHUNK * d + CHUNK] = share


def plane_body(in_ref, out_ref):
    total = in_ref[0:16]
    for s in range(1, PEERS):
        total = total + in_ref[CHUNK * s : CHUNK * s + 16]
    parts = []
    for y in range(4):
        part = None
        for x in range(4):
            at = CHUNK * (4 * y + x) + 16
            piece = in_ref[at : at + 4]
            part = piece if part is None else part + piece
        parts.append(part)
    share = picked(parts, lax.axis_index("zlo"))
    for z in range(STACK):
        out_ref[CHUNK * z : CHUNK * z + 16] = total
        out_ref[CHUNK * z + 16 : CHUNK * z + CHUNK] = share


def column_body(in_ref, out_ref, gram_ref):
    total = in_ref[0:16]
    for s in range(1, STACK):
        total = total + in_ref[CHUNK * s : CHUNK * s + 16]
    for d in range(PEERS):
        out_ref[d] = total
    for q in range(4):
        at = 2 * CHUNK * q + 16
        gram_ref[4 * q : 4 * q + 4] = in_ref[at : at + 4] + in_ref[at + CHUNK : at + CHUNK + 4]


def factor_body(gram_ref, mine_ref, other_ref, inverse_ref, frame_ref):
    packed = gram_ref[...]
    turned = pltpu.roll(packed, 64, 1)
    grams = [packed[0:8], packed[8:16], turned[0:8], turned[8:16]]
    shape = (8, LANES)
    lane, row = lane_of(shape), row_of(shape)
    first = (lane // RANK) % 2 == 0
    front = lane < 64
    units = [(lane % RANK) == row + 8 * r for r in range(4)]
    diagonal = jnp.zeros(shape, jnp.float32)
    for r in range(4):
        diagonal = diagonal + jnp.where(units[r] & front, grams[r], 0.0)
    mean0 = jnp.sum(jnp.where(first, diagonal, 0.0)) * (1.0 / RANK)
    mean1 = jnp.sum(jnp.where(first, 0.0, diagonal)) * (1.0 / RANK)
    ridge = jnp.where(front, 0.001 * jnp.where(first, mean0, mean1), 1.0)
    work = [jnp.where(front, grams[r], 0.0) + jnp.where(units[r], ridge, 0.0) for r in range(4)]
    for b in range(0, RANK, BLOCK):
        columns = [
            {
                r: jnp.where(first, work[r][:, k : k + 1], work[r][:, RANK + k : RANK + k + 1])
                for r in range(b // 8, 4)
            }
            for k in range(b, b + BLOCK)
        ]
        for i in range(BLOCK):
            at, s = divmod(b + i, 8)
            pivot = columns[i][at][s : s + 1]
            inverse = 1.0 / pivot
            chosen = work[at][s : s + 1]
            ahead = {j: columns[j][at][s : s + 1] for j in range(i + 1, BLOCK)}
            for r in range(at, 4):
                factor = columns[i][r] * inverse
                if r == at:
                    factor = jnp.where(row > s, factor, 0.0)
                work[r] = work[r] - factor * chosen
                for j in ahead:
                    columns[j][r] = columns[j][r] - factor * ahead[j]
            work[at] = jnp.where(row == s, work[at] * lax.rsqrt(pivot), work[at])
    inverse = pltpu.roll(jnp.concatenate(work, axis=0), 64, 1)
    inverse_ref[...] = inverse
    left = by_layer(mine_ref, other_ref)
    for l in range(2):
        frame_ref[l] = (
            jnp.dot(
                inverse[:, l * RANK : (l + 1) * RANK],
                left[l],
                precision=EXACT,
                preferred_element_type=jnp.float32,
            )
            * (1.0 / REPLICAS)
        )


def settle(layer, right_ref, inverse_ref, frame_ref, weights_ref, momentum_ref):
    place = (lax.axis_index("zlo") * 4 + lax.axis_index("y")) * 2 + core()
    block = place // 4
    shift = (4 - place % 4) * 32
    square = jnp.zeros((8, LANES), jnp.float32)
    for i in range(32):
        tile = right_ref[i]
        square = square + tile * tile
    scale = lax.rsqrt(jnp.sum(square) * (1.0 / (RANK * 1024)) + 1e-12)
    own = jnp.concatenate([right_ref[8 * t + block] for t in range(4)], axis=0)
    inverse = inverse_ref[...]
    inverse = jnp.where(layer == 0, inverse[:, :RANK], inverse[:, RANK : 2 * RANK])
    half = jnp.dot(inverse, own, precision=EXACT, preferred_element_type=jnp.float32)
    half = pltpu.roll(half, shift, 1)[:, :RANK]
    change = lax.dot_general(
        half,
        frame_ref[layer],
        (((0,), (0,)), ((), ())),
        precision=EXACT,
        preferred_element_type=jnp.float32,
    )
    new = 0.9 * momentum_ref[layer] + change
    return scale, new, weights_ref[layer] - 0.02 * new


def scaled(right_ref, scale, basis_ref, layer):
    for t in range(4):
        for j in range(8):
            at = (slice(8 * t, 8 * t + 8), slice(LANES * j, LANES * j + LANES))
            at = at if layer is None else (layer, *at)
            basis_ref[at] = right_ref[8 * t + j] * scale


def early_body(right_ref, inverse_ref, frame_ref, weights_ref, momentum_ref, basis_ref, w_ref, m_ref):
    scale, new, weights = settle(core(), right_ref, inverse_ref, frame_ref, weights_ref, momentum_ref)
    scaled(right_ref, scale, basis_ref, None)
    m_ref[...] = new
    w_ref[...] = weights


def late_body(
    right_ref, inverse_ref, frame_ref, weights_ref, momentum_ref, b_ref, w_ref, m_ref,
    basis_ref, new_w_ref, new_m_ref,
):
    c = core()
    basis_ref[c] = b_ref[...]
    new_w_ref[c] = w_ref[...]
    new_m_ref[c] = m_ref[...]
    layer = 1 - c
    scale, new, weights = settle(layer, right_ref, inverse_ref, frame_ref, weights_ref, momentum_ref)
    scaled(right_ref, scale, basis_ref, layer)
    new_m_ref[layer] = new
    new_w_ref[layer] = weights


DOUBLING = ((1, 1), (3, 1), (4, 1), (8, 0))


def swapped(value):
    return lax.ppermute(value, "core", [(0, 1), (1, 0)])


def all_to_all(value, axes):
    return lax.all_to_all(value, axes, 0, 0, tiled=True)


def shards(layer_grads, last_basis, layer_weights, momentum):
    grads = layer_grads[0]
    layers, rows, width = grads.shape
    basis = jnp.swapaxes(last_basis, 1, 2)
    weights, momentum = jnp.swapaxes(layer_weights, 1, 2), jnp.swapaxes(momentum, 1, 2)
    lefts, rights = f32(PEERS, 8, LANES), f32(PEERS, 16, LANES)

    anywhere = pl.BlockSpec(memory_space=pltpu.HBM)
    local = pl.BlockSpec(memory_space=pltpu.VMEM)
    away, grads, basis = pl.pallas_call(
        first_body,
        out_shape=[lefts, jax.ShapeDtypeStruct(grads.shape, grads.dtype), f32(*basis.shape)],
        in_specs=[anywhere] * 2,
        out_specs=[local] * 3,
        scratch_shapes=[pltpu.SemaphoreType.DMA((9,))],
        compiler_params=pltpu.CompilerParams(vmem_limit_bytes=VMEM_LIMIT),
        cost_estimate=pl.CostEstimate(flops=1 << 20, bytes_accessed=1 << 18, transcendentals=0),
    )(*(pltpu.with_memory_space_constraint(a, pltpu.HBM) for a in (basis, grads)))
    away = swapped(away)
    mine = kernel_call(left_body, lefts)(basis, grads) + away
    for flip, cross in DOUBLING:
        pairs = [(2 * p + c, 2 * (p ^ flip) + (c ^ cross)) for p in range(16) for c in range(2)]
        mine = mine + lax.ppermute(mine, REPLICA, pairs)
    other = swapped(mine)
    away = swapped(kernel_call(functools.partial(right_body, False), rights)(mine, other, grads))
    kept = kernel_call(functools.partial(right_body, True), rights)(mine, other, grads)
    share = kernel_call(gram_body, f32(4, LANES))(mine, other)

    sent = kernel_call(pack_body, f32(PEERS * CHUNK, LANES))(kept, away, share)
    came = all_to_all(sent.reshape(PEERS * CHUNK // 4, 4, LANES), PLANE)
    sent = kernel_call(plane_body, f32(STACK * CHUNK, LANES))(came.reshape(-1, LANES))
    came = all_to_all(sent.reshape(STACK * CHUNK // 4, 4, LANES), COLUMN)
    sent, gram = kernel_call(column_body, [rights, f32(16, LANES)])(came.reshape(-1, LANES))
    right = all_to_all(sent, PLANE)
    right, gram = lax.optimization_barrier((right.reshape(32, 8, LANES), gram))
    late = swapped(right)
    inverse, frame = kernel_call(factor_body, [f32(RANK, LANES), f32(layers, RANK, rows)])(
        gram, mine, other
    )
    solved = (inverse, frame, weights, momentum)
    early = kernel_call(
        early_body, [f32(RANK, width), f32(RANK, rows), f32(RANK, rows)]
    )(right, *solved)
    new_basis, new_weights, new_momentum = kernel_call(
        late_body,
        [f32(layers, RANK, width), f32(layers, RANK, rows), f32(layers, RANK, rows)],
    )(late, *solved, *early)
    return tuple(jnp.swapaxes(a, 1, 2) for a in (new_weights, new_basis, new_momentum))


def solution(mesh):
    fine = Mesh(mesh.devices.reshape(tuple(SIZES.values())), tuple(SIZES))
    sharded = P(None, MODEL, REPLICA)
    return jax.shard_map(
        shards,
        mesh=fine,
        in_specs=(P(REPLICA, None, MODEL, None), P(), sharded, sharded),
        out_specs=(sharded, P(), sharded),
        check_vma=False,
    )
```

```python
import functools
import itertools

import jax
import jax.numpy as jnp
from jax import lax
from jax.experimental import pallas as pl
from jax.experimental.pallas import tpu as pltpu
from jax.sharding import Mesh
from jax.sharding import PartitionSpec as P

RANK = 32
LANES = 128
SIZES = {"zlo": 4, "y": 4, "core": 2, "zhi": 2, "x": 4}
REPLICA = ("zlo", "y", "core")
MODEL = ("zhi", "x")
PLANE = ("y", "core", "x")
COLUMN = ("zlo", "core", "zhi")
REPLICAS, PEERS, STACK = 32, 16, 8
CHUNK = 20
BLOCK = 16
EXACT = lax.Precision.HIGHEST
VMEM_LIMIT = 24 * 1024 * 1024


def kernel_call(body, outs, flops=1 << 20, moved=1 << 18):
    many = isinstance(outs, (list, tuple))
    count = len(outs) if many else 1
    spec = pl.BlockSpec(memory_space=pltpu.VMEM)
    return lambda *args: pl.pallas_call(
        body,
        out_shape=outs,
        in_specs=[spec] * len(args),
        out_specs=[spec] * count if many else spec,
        compiler_params=pltpu.CompilerParams(vmem_limit_bytes=VMEM_LIMIT),
        cost_estimate=pl.CostEstimate(flops=flops, bytes_accessed=moved, transcendentals=0),
    )(*args)


def f32(*shape):
    return jax.ShapeDtypeStruct(shape, jnp.float32)


def joined(ref, rows, columns):
    return jnp.concatenate(
        [
            jnp.concatenate([ref[t * columns + j] for j in range(columns)], axis=1)
            for t in range(rows)
        ],
        axis=0,
    )


def lane_of(shape):
    return lax.broadcasted_iota(jnp.int32, shape, 1)


def row_of(shape):
    return lax.broadcasted_iota(jnp.int32, shape, 0)


def core():
    return lax.axis_index("core")


def held():
    return (core() + lax.axis_index("y") + lax.axis_index("zlo")) % 2


def owned():
    return (core() + lax.axis_index("y") // 2 + lax.axis_index("zhi")) % 2


WIDE = 256


def left_of(basis, grads):
    return lax.dot_general(
        basis.astype(jnp.bfloat16),
        grads,
        (((1,), (1,)), ((), ())),
        preferred_element_type=jnp.float32,
    )


def put_left(left, out_ref):
    for t in range(4):
        for j in range(4):
            out_ref[4 * t + j] = left[8 * t : 8 * t + 8, LANES * j : LANES * j + LANES]


def first_body(basis_hbm, grads_hbm, out_ref, grads_ref, basis_ref, sems):
    h = held()
    whole = pltpu.make_async_copy(basis_hbm, basis_ref, sems.at[8])
    whole.start()
    copies = []
    for k in range(8):
        at = (1 - h if k < 4 else h, slice(None), pl.ds(WIDE * (k % 4), WIDE))
        copies.append(pltpu.make_async_copy(grads_hbm.at[at], grads_ref.at[at], sems.at[k]))
        copies[-1].start()
    whole.wait()
    left = jnp.zeros((RANK, grads_ref.shape[1]), jnp.float32)
    for j in range(4):
        copies[j].wait()
        columns = slice(WIDE * j, WIDE * (j + 1))
        left = left + left_of(basis_ref[1 - h, :, columns], grads_ref[1 - h, :, columns])
    put_left(left, out_ref)
    for k in range(4, 8):
        copies[k].wait()


def left_body(basis_ref, grads_ref, out_ref):
    h = held()
    put_left(left_of(basis_ref[h], grads_ref[h]), out_ref)


def right_body(kept, mine_ref, other_ref, grads_ref, out_ref):
    layer = owned() if kept else 1 - owned()
    left = jnp.where(layer == held(), joined(mine_ref, 4, 4), joined(other_ref, 4, 4))
    right = jnp.dot(
        left.astype(jnp.bfloat16),
        grads_ref[layer],
        preferred_element_type=jnp.float32,
    )
    for t in range(4):
        for j in range(8):
            d, h = divmod(8 * t + j, 2)
            out_ref[d, 8 * h : 8 * h + 8] = right[8 * t : 8 * t + 8, LANES * j : LANES * j + LANES]


def by_layer(mine_ref, other_ref):
    mine, other = joined(mine_ref, 4, 4), joined(other_ref, 4, 4)
    first = held() == 0
    return jnp.where(first, mine, other), jnp.where(first, other, mine)


def gram_body(mine_ref, other_ref, share_ref):
    left = jnp.concatenate(by_layer(mine_ref, other_ref), axis=0)
    twice = jnp.concatenate([left, left], axis=0)
    gram = lax.dot_general(
        left, twice, (((1,), (1,)), ((), ())), precision=EXACT, preferred_element_type=jnp.float32
    )
    lane = lane_of((16, LANES))
    packed = jnp.where(
        lane < 32,
        gram[0:16],
        jnp.where(lane < 64, gram[32:48], jnp.where(lane < 96, gram[16:32], gram[48:64])),
    )
    share_ref[...] = picked([packed[4 * s : 4 * s + 4] for s in range(4)], lax.axis_index("y"))


def picked(values, index):
    out = values[0]
    for s in range(1, len(values)):
        out = jnp.where(index == s, values[s], out)
    return out


def pack_body(mine_ref, other_ref, share_ref, out_ref):
    share = share_ref[...]
    for d in range(PEERS):
        out_ref[CHUNK * d : CHUNK * d + 16] = mine_ref[d] + other_ref[d]
        out_ref[CHUNK * d + 16 : CHUNK * d + CHUNK] = share


def plane_body(in_ref, out_ref):
    total = in_ref[0:16]
    for s in range(1, PEERS):
        total = total + in_ref[CHUNK * s : CHUNK * s + 16]
    parts = []
    for y in range(4):
        part = None
        for x in range(4):
            at = CHUNK * (4 * y + x) + 16
            piece = in_ref[at : at + 4]
            part = piece if part is None else part + piece
        parts.append(part)
    share = picked(parts, lax.axis_index("zlo"))
    for z in range(STACK):
        out_ref[CHUNK * z : CHUNK * z + 16] = total
        out_ref[CHUNK * z + 16 : CHUNK * z + CHUNK] = share


def column_body(in_ref, out_ref, gram_ref):
    total = in_ref[0:16]
    for s in range(1, STACK):
        total = total + in_ref[CHUNK * s : CHUNK * s + 16]
    for d in range(PEERS):
        out_ref[d] = total
    for q in range(4):
        at = 2 * CHUNK * q + 16
        gram_ref[4 * q : 4 * q + 4] = in_ref[at : at + 4] + in_ref[at + CHUNK : at + CHUNK + 4]


def factor_body(gram_ref, mine_ref, other_ref, inverse_ref, frame_ref):
    packed = gram_ref[...]
    turned = pltpu.roll(packed, 64, 1)
    grams = [packed[0:8], packed[8:16], turned[0:8], turned[8:16]]
    shape = (8, LANES)
    lane, row = lane_of(shape), row_of(shape)
    first = (lane // RANK) % 2 == 0
    front = lane < 64
    units = [(lane % RANK) == row + 8 * r for r in range(4)]
    diagonal = jnp.zeros(shape, jnp.float32)
    for r in range(4):
        diagonal = diagonal + jnp.where(units[r] & front, grams[r], 0.0)
    mean0 = jnp.sum(jnp.where(first, diagonal, 0.0)) * (1.0 / RANK)
    mean1 = jnp.sum(jnp.where(first, 0.0, diagonal)) * (1.0 / RANK)
    ridge = jnp.where(front, 0.001 * jnp.where(first, mean0, mean1), 1.0)
    work = [jnp.where(front, grams[r], 0.0) + jnp.where(units[r], ridge, 0.0) for r in range(4)]
    for b in range(0, RANK, BLOCK):
        columns = [
            {
                r: jnp.where(first, work[r][:, k : k + 1], work[r][:, RANK + k : RANK + k + 1])
                for r in range(b // 8, 4)
            }
            for k in range(b, b + BLOCK)
        ]
        for i in range(BLOCK):
            at, s = divmod(b + i, 8)
            pivot = columns[i][at][s : s + 1]
            inverse = 1.0 / pivot
            chosen = work[at][s : s + 1]
            ahead = {j: columns[j][at][s : s + 1] for j in range(i + 1, BLOCK)}
            for r in range(at, 4):
                factor = columns[i][r] * inverse
                if r == at:
                    factor = jnp.where(row > s, factor, 0.0)
                work[r] = work[r] - factor * chosen
                for j in ahead:
                    columns[j][r] = columns[j][r] - factor * ahead[j]
            work[at] = jnp.where(row == s, work[at] * lax.rsqrt(pivot), work[at])
    inverse = pltpu.roll(jnp.concatenate(work, axis=0), 64, 1)
    inverse_ref[...] = inverse
    left = by_layer(mine_ref, other_ref)
    for l in range(2):
        frame_ref[l] = (
            jnp.dot(
                inverse[:, l * RANK : (l + 1) * RANK],
                left[l],
                precision=EXACT,
                preferred_element_type=jnp.float32,
            )
            * (1.0 / REPLICAS)
        )


def settle(layer, right_ref, inverse_ref, frame_ref, weights_ref, momentum_ref):
    place = (lax.axis_index("zlo") * 4 + lax.axis_index("y")) * 2 + core()
    block = place // 4
    shift = (4 - place % 4) * 32
    square = jnp.zeros((8, LANES), jnp.float32)
    for i in range(32):
        tile = right_ref[i]
        square = square + tile * tile
    scale = lax.rsqrt(jnp.sum(square) * (1.0 / (RANK * 1024)) + 1e-12)
    own = jnp.concatenate([right_ref[8 * t + block] for t in range(4)], axis=0)
    inverse = inverse_ref[...]
    inverse = jnp.where(layer == 0, inverse[:, :RANK], inverse[:, RANK : 2 * RANK])
    half = jnp.dot(inverse, own, precision=EXACT, preferred_element_type=jnp.float32)
    half = pltpu.roll(half, shift, 1)[:, :RANK]
    change = lax.dot_general(
        half,
        frame_ref[layer],
        (((0,), (0,)), ((), ())),
        precision=EXACT,
        preferred_element_type=jnp.float32,
    )
    new = 0.9 * momentum_ref[layer] + change
    return scale, new, weights_ref[layer] - 0.02 * new


def scaled(right_ref, scale, basis_ref, layer):
    for t in range(4):
        for j in range(8):
            at = (slice(8 * t, 8 * t + 8), slice(LANES * j, LANES * j + LANES))
            at = at if layer is None else (layer, *at)
            basis_ref[at] = right_ref[8 * t + j] * scale


def early_body(right_ref, inverse_ref, frame_ref, weights_ref, momentum_ref, basis_ref, w_ref, m_ref):
    scale, new, weights = settle(owned(), right_ref, inverse_ref, frame_ref, weights_ref, momentum_ref)
    scaled(right_ref, scale, basis_ref, None)
    m_ref[...] = new
    w_ref[...] = weights


def late_body(
    right_ref, inverse_ref, frame_ref, weights_ref, momentum_ref, b_ref, w_ref, m_ref,
    basis_ref, new_w_ref, new_m_ref,
):
    c = owned()
    basis_ref[c] = b_ref[...]
    new_w_ref[c] = w_ref[...]
    new_m_ref[c] = m_ref[...]
    layer = 1 - c
    scale, new, weights = settle(layer, right_ref, inverse_ref, frame_ref, weights_ref, momentum_ref)
    scaled(right_ref, scale, basis_ref, layer)
    new_m_ref[layer] = new
    new_w_ref[layer] = weights


DOUBLING = ((1, 1), (3, 1), (4, 1), (8, 0))


def swapped(value):
    return lax.ppermute(value, "core", [(0, 1), (1, 0)])


def all_to_all(value, axes):
    groups = ([], [])
    for i, place in enumerate(itertools.product(*(range(SIZES[a]) for a in axes))):
        at = dict(zip(axes, place))
        groups[(at["core"] + at.get("y", 0) // 2 + at.get("zhi", 0)) % 2].append(i)
    return lax.all_to_all(value, axes, 0, 0, axis_index_groups=groups, tiled=True)


def shards(layer_grads, last_basis, layer_weights, momentum):
    grads = layer_grads[0]
    layers, rows, width = grads.shape
    basis = jnp.swapaxes(last_basis, 1, 2)
    weights, momentum = jnp.swapaxes(layer_weights, 1, 2), jnp.swapaxes(momentum, 1, 2)
    lefts, rights = f32(PEERS, 8, LANES), f32(PEERS, 16, LANES)

    anywhere = pl.BlockSpec(memory_space=pltpu.HBM)
    local = pl.BlockSpec(memory_space=pltpu.VMEM)
    away, grads, basis = pl.pallas_call(
        first_body,
        out_shape=[lefts, jax.ShapeDtypeStruct(grads.shape, grads.dtype), f32(*basis.shape)],
        in_specs=[anywhere] * 2,
        out_specs=[local] * 3,
        scratch_shapes=[pltpu.SemaphoreType.DMA((9,))],
        compiler_params=pltpu.CompilerParams(vmem_limit_bytes=VMEM_LIMIT),
        cost_estimate=pl.CostEstimate(flops=1 << 20, bytes_accessed=1 << 18, transcendentals=0),
    )(*(pltpu.with_memory_space_constraint(a, pltpu.HBM) for a in (basis, grads)))
    away = swapped(away)
    mine = kernel_call(left_body, lefts)(basis, grads) + away
    for flip, cross in DOUBLING:
        pairs = [(2 * p + c, 2 * (p ^ flip) + (c ^ cross)) for p in range(16) for c in range(2)]
        mine = mine + lax.ppermute(mine, REPLICA, pairs)
    other = swapped(mine)
    away = swapped(kernel_call(functools.partial(right_body, False), rights)(mine, other, grads))
    kept = kernel_call(functools.partial(right_body, True), rights)(mine, other, grads)
    share = kernel_call(gram_body, f32(4, LANES))(mine, other)

    sent = kernel_call(pack_body, f32(PEERS * CHUNK, LANES))(kept, away, share)
    came = all_to_all(sent.reshape(PEERS * CHUNK // 4, 4, LANES), PLANE)
    sent = kernel_call(plane_body, f32(STACK * CHUNK, LANES))(came.reshape(-1, LANES))
    came = all_to_all(sent.reshape(STACK * CHUNK // 4, 4, LANES), COLUMN)
    sent, gram = kernel_call(column_body, [rights, f32(16, LANES)])(came.reshape(-1, LANES))
    right = all_to_all(sent, PLANE)
    right, gram = lax.optimization_barrier((right.reshape(32, 8, LANES), gram))
    late = swapped(right)
    inverse, frame = kernel_call(factor_body, [f32(RANK, LANES), f32(layers, RANK, rows)])(
        gram, mine, other
    )
    solved = (inverse, frame, weights, momentum)
    early = kernel_call(
        early_body, [f32(RANK, width), f32(RANK, rows), f32(RANK, rows)]
    )(right, *solved)
    new_basis, new_weights, new_momentum = kernel_call(
        late_body,
        [f32(layers, RANK, width), f32(layers, RANK, rows), f32(layers, RANK, rows)],
    )(late, *solved, *early)
    return tuple(jnp.swapaxes(a, 1, 2) for a in (new_weights, new_basis, new_momentum))


def solution(mesh):
    fine = Mesh(mesh.devices.reshape(tuple(SIZES.values())), tuple(SIZES))
    sharded = P(None, MODEL, REPLICA)
    return jax.shard_map(
        shards,
        mesh=fine,
        in_specs=(P(REPLICA, None, MODEL, None), P(), sharded, sharded),
        out_specs=(sharded, P(), sharded),
        check_vma=False,
    )
```

```python
import functools
import itertools

import jax
import jax.numpy as jnp
from jax import lax
from jax.experimental import pallas as pl
from jax.experimental.pallas import tpu as pltpu
from jax.sharding import Mesh
from jax.sharding import PartitionSpec as P

RANK = 32
LANES = 128
SIZES = {"zlo": 4, "y": 4, "core": 2, "zhi": 2, "x": 4}
REPLICA = ("zlo", "y", "core")
MODEL = ("zhi", "x")
PLANE = ("y", "core", "x")
COLUMN = ("zlo", "core", "zhi")
REPLICAS, PEERS, STACK = 32, 16, 8
CHUNK = 20
BLOCK = 16
EXACT = lax.Precision.HIGHEST
VMEM_LIMIT = 24 * 1024 * 1024


def kernel_call(body, outs, flops=1 << 20, moved=1 << 18):
    many = isinstance(outs, (list, tuple))
    count = len(outs) if many else 1
    spec = pl.BlockSpec(memory_space=pltpu.VMEM)
    return lambda *args: pl.pallas_call(
        body,
        out_shape=outs,
        in_specs=[spec] * len(args),
        out_specs=[spec] * count if many else spec,
        compiler_params=pltpu.CompilerParams(vmem_limit_bytes=VMEM_LIMIT),
        cost_estimate=pl.CostEstimate(flops=flops, bytes_accessed=moved, transcendentals=0),
    )(*args)


def f32(*shape):
    return jax.ShapeDtypeStruct(shape, jnp.float32)


def joined(ref, rows, columns):
    return jnp.concatenate(
        [
            jnp.concatenate([ref[t * columns + j] for j in range(columns)], axis=1)
            for t in range(rows)
        ],
        axis=0,
    )


def lane_of(shape):
    return lax.broadcasted_iota(jnp.int32, shape, 1)


def row_of(shape):
    return lax.broadcasted_iota(jnp.int32, shape, 0)


def core():
    return lax.axis_index("core")


def colour(y, zlo, zhi, c):
    return (c + y // 2 + zlo + zhi) % 2


def held():
    return colour(lax.axis_index("y"), lax.axis_index("zlo"), lax.axis_index("zhi"), core())


def owned():
    return 1 - held()


WIDE = 256


def left_of(basis, grads):
    return lax.dot_general(
        basis.astype(jnp.bfloat16),
        grads,
        (((1,), (1,)), ((), ())),
        preferred_element_type=jnp.float32,
    )


def put_left(left, out_ref):
    for t in range(4):
        for j in range(4):
            out_ref[4 * t + j] = left[8 * t : 8 * t + 8, LANES * j : LANES * j + LANES]


def first_body(basis_hbm, grads_hbm, out_ref, grads_ref, basis_ref, sems):
    h = held()
    whole = pltpu.make_async_copy(basis_hbm, basis_ref, sems.at[8])
    whole.start()
    copies = []
    for k in range(8):
        at = (1 - h if k < 4 else h, slice(None), pl.ds(WIDE * (k % 4), WIDE))
        copies.append(pltpu.make_async_copy(grads_hbm.at[at], grads_ref.at[at], sems.at[k]))
        copies[-1].start()
    whole.wait()
    left = jnp.zeros((RANK, grads_ref.shape[1]), jnp.float32)
    for j in range(4):
        copies[j].wait()
        columns = slice(WIDE * j, WIDE * (j + 1))
        left = left + left_of(basis_ref[1 - h, :, columns], grads_ref[1 - h, :, columns])
    put_left(left, out_ref)
    for k in range(4, 8):
        copies[k].wait()


def left_body(basis_ref, grads_ref, out_ref):
    h = held()
    put_left(left_of(basis_ref[h], grads_ref[h]), out_ref)


def right_body(kept, left_ref, grads_ref, out_ref):
    right = jnp.dot(
        joined(left_ref, 4, 4).astype(jnp.bfloat16),
        grads_ref[owned() if kept else held()],
        preferred_element_type=jnp.float32,
    )
    for t in range(4):
        for j in range(8):
            d, h = divmod(8 * t + j, 2)
            out_ref[d, 8 * h : 8 * h + 8] = right[8 * t : 8 * t + 8, LANES * j : LANES * j + LANES]


def by_layer(mine_ref, other_ref):
    mine, other = joined(mine_ref, 4, 4), joined(other_ref, 4, 4)
    first = held() == 0
    return jnp.where(first, mine, other), jnp.where(first, other, mine)


def gram_body(mine_ref, other_ref, share_ref):
    left = jnp.concatenate(by_layer(mine_ref, other_ref), axis=0)
    twice = jnp.concatenate([left, left], axis=0)
    gram = lax.dot_general(
        left, twice, (((1,), (1,)), ((), ())), precision=EXACT, preferred_element_type=jnp.float32
    )
    lane = lane_of((16, LANES))
    packed = jnp.where(
        lane < 32,
        gram[0:16],
        jnp.where(lane < 64, gram[32:48], jnp.where(lane < 96, gram[16:32], gram[48:64])),
    )
    share_ref[...] = picked([packed[4 * s : 4 * s + 4] for s in range(4)], lax.axis_index("y"))


def picked(values, index):
    out = values[0]
    for s in range(1, len(values)):
        out = jnp.where(index == s, values[s], out)
    return out


def pack_body(mine_ref, other_ref, share_ref, out_ref):
    share = share_ref[...]
    for d in range(PEERS):
        out_ref[CHUNK * d : CHUNK * d + 16] = mine_ref[d] + other_ref[d]
        out_ref[CHUNK * d + 16 : CHUNK * d + CHUNK] = share


def plane_body(in_ref, out_ref):
    total = in_ref[0:16]
    for s in range(1, PEERS):
        total = total + in_ref[CHUNK * s : CHUNK * s + 16]
    parts = []
    for y in range(4):
        part = None
        for x in range(4):
            at = CHUNK * (4 * y + x) + 16
            piece = in_ref[at : at + 4]
            part = piece if part is None else part + piece
        parts.append(part)
    share = picked(parts, lax.axis_index("zlo"))
    for z in range(STACK):
        out_ref[CHUNK * z : CHUNK * z + 16] = total
        out_ref[CHUNK * z + 16 : CHUNK * z + CHUNK] = share


def column_body(in_ref, out_ref, gram_ref):
    total = in_ref[0:16]
    for s in range(1, STACK):
        total = total + in_ref[CHUNK * s : CHUNK * s + 16]
    for d in range(PEERS):
        out_ref[d] = total
    for q in range(4):
        at = 2 * CHUNK * q + 16
        gram_ref[4 * q : 4 * q + 4] = in_ref[at : at + 4] + in_ref[at + CHUNK : at + CHUNK + 4]


def factor_body(gram_ref, mine_ref, other_ref, inverse_ref, frame_ref):
    packed = gram_ref[...]
    turned = pltpu.roll(packed, 64, 1)
    grams = [packed[0:8], packed[8:16], turned[0:8], turned[8:16]]
    shape = (8, LANES)
    lane, row = lane_of(shape), row_of(shape)
    first = (lane // RANK) % 2 == 0
    front = lane < 64
    units = [(lane % RANK) == row + 8 * r for r in range(4)]
    diagonal = jnp.zeros(shape, jnp.float32)
    for r in range(4):
        diagonal = diagonal + jnp.where(units[r] & front, grams[r], 0.0)
    mean0 = jnp.sum(jnp.where(first, diagonal, 0.0)) * (1.0 / RANK)
    mean1 = jnp.sum(jnp.where(first, 0.0, diagonal)) * (1.0 / RANK)
    ridge = jnp.where(front, 0.001 * jnp.where(first, mean0, mean1), 1.0)
    work = [jnp.where(front, grams[r], 0.0) + jnp.where(units[r], ridge, 0.0) for r in range(4)]
    for b in range(0, RANK, BLOCK):
        columns = [
            {
                r: jnp.where(first, work[r][:, k : k + 1], work[r][:, RANK + k : RANK + k + 1])
                for r in range(b // 8, 4)
            }
            for k in range(b, b + BLOCK)
        ]
        for i in range(BLOCK):
            at, s = divmod(b + i, 8)
            pivot = columns[i][at][s : s + 1]
            inverse = 1.0 / pivot
            chosen = work[at][s : s + 1]
            ahead = {j: columns[j][at][s : s + 1] for j in range(i + 1, BLOCK)}
            for r in range(at, 4):
                factor = columns[i][r] * inverse
                if r == at:
                    factor = jnp.where(row > s, factor, 0.0)
                work[r] = work[r] - factor * chosen
                for j in ahead:
                    columns[j][r] = columns[j][r] - factor * ahead[j]
            work[at] = jnp.where(row == s, work[at] * lax.rsqrt(pivot), work[at])
    inverse = pltpu.roll(jnp.concatenate(work, axis=0), 64, 1)
    inverse_ref[...] = inverse
    left = by_layer(mine_ref, other_ref)
    for l in range(2):
        frame_ref[l] = (
            jnp.dot(
                inverse[:, l * RANK : (l + 1) * RANK],
                left[l],
                precision=EXACT,
                preferred_element_type=jnp.float32,
            )
            * (1.0 / REPLICAS)
        )


def settle(layer, right_ref, inverse_ref, frame_ref, weights_ref, momentum_ref):
    place = (lax.axis_index("zlo") * 4 + lax.axis_index("y")) * 2 + core()
    block = place // 4
    shift = (4 - place % 4) * 32
    square = jnp.zeros((8, LANES), jnp.float32)
    for i in range(32):
        tile = right_ref[i]
        square = square + tile * tile
    scale = lax.rsqrt(jnp.sum(square) * (1.0 / (RANK * 1024)) + 1e-12)
    own = jnp.concatenate([right_ref[8 * t + block] for t in range(4)], axis=0)
    inverse = inverse_ref[...]
    inverse = jnp.where(layer == 0, inverse[:, :RANK], inverse[:, RANK : 2 * RANK])
    half = jnp.dot(inverse, own, precision=EXACT, preferred_element_type=jnp.float32)
    half = pltpu.roll(half, shift, 1)[:, :RANK]
    change = lax.dot_general(
        half,
        frame_ref[layer],
        (((0,), (0,)), ((), ())),
        precision=EXACT,
        preferred_element_type=jnp.float32,
    )
    new = 0.9 * momentum_ref[layer] + change
    return scale, new, weights_ref[layer] - 0.02 * new


def scaled(right_ref, scale, basis_ref, layer):
    for t in range(4):
        for j in range(8):
            at = (slice(8 * t, 8 * t + 8), slice(LANES * j, LANES * j + LANES))
            at = at if layer is None else (layer, *at)
            basis_ref[at] = right_ref[8 * t + j] * scale


def early_body(right_ref, inverse_ref, frame_ref, weights_ref, momentum_ref, basis_ref, w_ref, m_ref):
    scale, new, weights = settle(owned(), right_ref, inverse_ref, frame_ref, weights_ref, momentum_ref)
    scaled(right_ref, scale, basis_ref, None)
    m_ref[...] = new
    w_ref[...] = weights


def late_body(
    right_ref, inverse_ref, frame_ref, weights_ref, momentum_ref, b_ref, w_ref, m_ref,
    basis_ref, new_w_ref, new_m_ref,
):
    c = owned()
    basis_ref[c] = b_ref[...]
    new_w_ref[c] = w_ref[...]
    new_m_ref[c] = m_ref[...]
    layer = 1 - c
    scale, new, weights = settle(layer, right_ref, inverse_ref, frame_ref, weights_ref, momentum_ref)
    scaled(right_ref, scale, basis_ref, layer)
    new_m_ref[layer] = new
    new_w_ref[layer] = weights


DOUBLING = ((1, 0), (3, 1), (4, 1), (8, 0))


def swapped(value):
    return lax.ppermute(value, "core", [(0, 1), (1, 0)])


def all_to_all(value, axes):
    groups = ([], [])
    for i, place in enumerate(itertools.product(*(range(SIZES[a]) for a in axes))):
        at = dict(zip(axes, place))
        groups[colour(at.get("y", 0), at.get("zlo", 0), at.get("zhi", 0), at["core"])].append(i)
    return lax.all_to_all(value, axes, 0, 0, axis_index_groups=groups, tiled=True)


def shards(layer_grads, last_basis, layer_weights, momentum):
    grads = layer_grads[0]
    layers, rows, width = grads.shape
    basis = jnp.swapaxes(last_basis, 1, 2)
    weights, momentum = jnp.swapaxes(layer_weights, 1, 2), jnp.swapaxes(momentum, 1, 2)
    lefts, rights = f32(PEERS, 8, LANES), f32(PEERS, 16, LANES)

    anywhere = pl.BlockSpec(memory_space=pltpu.HBM)
    local = pl.BlockSpec(memory_space=pltpu.VMEM)
    away, grads, basis = pl.pallas_call(
        first_body,
        out_shape=[lefts, jax.ShapeDtypeStruct(grads.shape, grads.dtype), f32(*basis.shape)],
        in_specs=[anywhere] * 2,
        out_specs=[local] * 3,
        scratch_shapes=[pltpu.SemaphoreType.DMA((9,))],
        compiler_params=pltpu.CompilerParams(vmem_limit_bytes=VMEM_LIMIT),
        cost_estimate=pl.CostEstimate(flops=1 << 20, bytes_accessed=1 << 18, transcendentals=0),
    )(*(pltpu.with_memory_space_constraint(a, pltpu.HBM) for a in (basis, grads)))
    away = swapped(away)
    mine = kernel_call(left_body, lefts)(basis, grads) + away
    for flip, cross in DOUBLING:
        pairs = [(2 * p + c, 2 * (p ^ flip) + (c ^ cross)) for p in range(16) for c in range(2)]
        mine = mine + lax.ppermute(mine, REPLICA, pairs)
    other = swapped(mine)
    away = swapped(kernel_call(functools.partial(right_body, False), rights)(mine, grads))
    kept = kernel_call(functools.partial(right_body, True), rights)(other, grads)
    share = kernel_call(gram_body, f32(4, LANES))(mine, other)

    sent = kernel_call(pack_body, f32(PEERS * CHUNK, LANES))(kept, away, share)
    came = all_to_all(sent.reshape(PEERS * CHUNK // 4, 4, LANES), PLANE)
    sent = kernel_call(plane_body, f32(STACK * CHUNK, LANES))(came.reshape(-1, LANES))
    came = all_to_all(sent.reshape(STACK * CHUNK // 4, 4, LANES), COLUMN)
    sent, gram = kernel_call(column_body, [rights, f32(16, LANES)])(came.reshape(-1, LANES))
    right = all_to_all(sent, PLANE)
    right, gram = lax.optimization_barrier((right.reshape(32, 8, LANES), gram))
    late = swapped(right)
    inverse, frame = kernel_call(factor_body, [f32(RANK, LANES), f32(layers, RANK, rows)])(
        gram, mine, other
    )
    solved = (inverse, frame, weights, momentum)
    early = kernel_call(
        early_body, [f32(RANK, width), f32(RANK, rows), f32(RANK, rows)]
    )(right, *solved)
    new_basis, new_weights, new_momentum = kernel_call(
        late_body,
        [f32(layers, RANK, width), f32(layers, RANK, rows), f32(layers, RANK, rows)],
    )(late, *solved, *early)
    return tuple(jnp.swapaxes(a, 1, 2) for a in (new_weights, new_basis, new_momentum))


def solution(mesh):
    fine = Mesh(mesh.devices.reshape(tuple(SIZES.values())), tuple(SIZES))
    sharded = P(None, MODEL, REPLICA)
    return jax.shard_map(
        shards,
        mesh=fine,
        in_specs=(P(REPLICA, None, MODEL, None), P(), sharded, sharded),
        out_specs=(sharded, P(), sharded),
        check_vma=False,
    )
```

```python
import itertools

import jax
import jax.numpy as jnp
from jax import lax
from jax.experimental import pallas as pl
from jax.experimental.pallas import tpu as pltpu
from jax.sharding import Mesh
from jax.sharding import PartitionSpec as P


RANK = 32
LANES = 128
SIZES = {"zlo": 4, "y": 4, "core": 2, "zhi": 2, "x": 4}
REPLICA = ("zlo", "y", "core")
MODEL = ("zhi", "x")
PLANE = ("y", "core", "x")
COLUMN = ("zlo", "core", "zhi")
REPLICAS, PEERS, STACK = 32, 16, 8
CHUNK = 20
BLOCK = 16
EXACT = lax.Precision.HIGHEST
VMEM_LIMIT = 24 * 1024 * 1024


def kernel_call(body, outs, flops=1 << 20, moved=1 << 18):
    many = isinstance(outs, (list, tuple))
    count = len(outs) if many else 1
    spec = pl.BlockSpec(memory_space=pltpu.VMEM)
    return lambda *args: pl.pallas_call(
        body,
        out_shape=outs,
        in_specs=[spec] * len(args),
        out_specs=[spec] * count if many else spec,
        compiler_params=pltpu.CompilerParams(vmem_limit_bytes=VMEM_LIMIT),
        cost_estimate=pl.CostEstimate(flops=flops, bytes_accessed=moved, transcendentals=0),
    )(*args)


def f32(*shape):
    return jax.ShapeDtypeStruct(shape, jnp.float32)


def joined(ref, rows, columns):
    return jnp.concatenate(
        [
            jnp.concatenate([ref[t * columns + j] for j in range(columns)], axis=1)
            for t in range(rows)
        ],
        axis=0,
    )


def lane_of(shape):
    return lax.broadcasted_iota(jnp.int32, shape, 1)


def row_of(shape):
    return lax.broadcasted_iota(jnp.int32, shape, 0)


def core():
    return lax.axis_index("core")


def colour(y, zlo, zhi, c):
    return (c + y // 2 + zlo + zhi) % 2


def held():
    return colour(lax.axis_index("y"), lax.axis_index("zlo"), lax.axis_index("zhi"), core())


def owned():
    return 1 - held()


WIDE = 256


def left_of(basis, grads):
    return lax.dot_general(
        basis.astype(jnp.bfloat16),
        grads,
        (((1,), (1,)), ((), ())),
        preferred_element_type=jnp.float32,
    )


def put_left(left, out_ref):
    for t in range(4):
        for j in range(4):
            out_ref[4 * t + j] = left[8 * t : 8 * t + 8, LANES * j : LANES * j + LANES]


def first_body(basis_hbm, grads_hbm, out_ref, grads_ref, basis_ref, sems):
    h = held()
    whole = pltpu.make_async_copy(basis_hbm, basis_ref, sems.at[8])
    whole.start()
    copies = []
    for k in range(8):
        at = (1 - h if k < 4 else h, slice(None), pl.ds(WIDE * (k % 4), WIDE))
        copies.append(pltpu.make_async_copy(grads_hbm.at[at], grads_ref.at[at], sems.at[k]))
        copies[-1].start()
    whole.wait()
    left = jnp.zeros((RANK, grads_ref.shape[1]), jnp.float32)
    for j in range(4):
        copies[j].wait()
        columns = slice(WIDE * j, WIDE * (j + 1))
        left = left + left_of(basis_ref[1 - h, :, columns], grads_ref[1 - h, :, columns])
    put_left(left, out_ref)
    for k in range(4, 8):
        copies[k].wait()


def left_body(basis_ref, grads_ref, out_ref):
    h = held()
    put_left(left_of(basis_ref[h], grads_ref[h]), out_ref)


def put_right(left, grads, out_ref):
    right = jnp.dot(left.astype(jnp.bfloat16), grads, preferred_element_type=jnp.float32)
    for t in range(4):
        for j in range(8):
            d, h = divmod(8 * t + j, 2)
            out_ref[d, 8 * h : 8 * h + 8] = right[8 * t : 8 * t + 8, LANES * j : LANES * j + LANES]


def packed_gram(left):
    gram = lax.dot_general(
        left,
        jnp.concatenate([left] * 4, axis=0),
        (((1,), (1,)), ((), ())),
        precision=EXACT,
        preferred_element_type=jnp.float32,
    )
    return jnp.where(lane_of((16, LANES)) < 64, gram[:16], gram[16:])


def sent_body(left_ref, grads_ref, out_ref, gram_ref):
    left = joined(left_ref, 4, 4)
    put_right(left, grads_ref[held()], out_ref)
    gram_ref[...] = packed_gram(left)


def kept_body(left_ref, grads_ref, gram_ref, out_ref, share_ref):
    layer = owned()
    left = joined(left_ref, 4, 4)
    put_right(left, grads_ref[layer], out_ref)
    group = lane_of((16, LANES)) // RANK % 2
    packed = jnp.where(group == layer, packed_gram(left), gram_ref[...])
    share_ref[...] = picked([packed[4 * s : 4 * s + 4] for s in range(4)], lax.axis_index("y"))


def by_layer(mine_ref, other_ref):
    mine, other = joined(mine_ref, 4, 4), joined(other_ref, 4, 4)
    first = held() == 0
    return jnp.where(first, mine, other), jnp.where(first, other, mine)


def picked(values, index):
    out = values[0]
    for s in range(1, len(values)):
        out = jnp.where(index == s, values[s], out)
    return out


def pack_body(mine_ref, other_ref, share_ref, out_ref):
    share = share_ref[...]
    for d in range(PEERS):
        out_ref[CHUNK * d : CHUNK * d + 16] = mine_ref[d] + other_ref[d]
        out_ref[CHUNK * d + 16 : CHUNK * d + CHUNK] = share


def plane_body(in_ref, out_ref):
    total = in_ref[0:16]
    for s in range(1, PEERS):
        total = total + in_ref[CHUNK * s : CHUNK * s + 16]
    parts = []
    for y in range(4):
        part = None
        for x in range(4):
            at = CHUNK * (4 * y + x) + 16
            piece = in_ref[at : at + 4]
            part = piece if part is None else part + piece
        parts.append(part)
    share = picked(parts, lax.axis_index("zlo"))
    for z in range(STACK):
        out_ref[CHUNK * z : CHUNK * z + 16] = total
        out_ref[CHUNK * z + 16 : CHUNK * z + CHUNK] = share


def column_body(in_ref, out_ref, gram_ref):
    total = in_ref[0:16]
    for s in range(1, STACK):
        total = total + in_ref[CHUNK * s : CHUNK * s + 16]
    for d in range(PEERS):
        out_ref[d] = total
    for q in range(4):
        at = 2 * CHUNK * q + 16
        gram_ref[4 * q : 4 * q + 4] = in_ref[at : at + 4] + in_ref[at + CHUNK : at + CHUNK + 4]


def factor_body(gram_ref, mine_ref, other_ref, inverse_ref, frame_ref):
    packed = gram_ref[...]
    turned = pltpu.roll(packed, 64, 1)
    grams = [packed[0:8], packed[8:16], turned[0:8], turned[8:16]]
    shape = (8, LANES)
    lane, row = lane_of(shape), row_of(shape)
    first = (lane // RANK) % 2 == 0
    front = lane < 64
    units = [(lane % RANK) == row + 8 * r for r in range(4)]
    diagonal = jnp.zeros(shape, jnp.float32)
    for r in range(4):
        diagonal = diagonal + jnp.where(units[r] & front, grams[r], 0.0)
    mean0 = jnp.sum(jnp.where(first, diagonal, 0.0)) * (1.0 / RANK)
    mean1 = jnp.sum(jnp.where(first, 0.0, diagonal)) * (1.0 / RANK)
    ridge = jnp.where(front, 0.001 * jnp.where(first, mean0, mean1), 1.0)
    work = [jnp.where(front, grams[r], 0.0) + jnp.where(units[r], ridge, 0.0) for r in range(4)]
    for b in range(0, RANK, BLOCK):
        columns = [
            {
                r: jnp.where(first, work[r][:, k : k + 1], work[r][:, RANK + k : RANK + k + 1])
                for r in range(b // 8, 4)
            }
            for k in range(b, b + BLOCK)
        ]
        for i in range(BLOCK):
            at, s = divmod(b + i, 8)
            pivot = columns[i][at][s : s + 1]
            inverse = 1.0 / pivot
            chosen = work[at][s : s + 1]
            ahead = {j: columns[j][at][s : s + 1] for j in range(i + 1, BLOCK)}
            for r in range(at, 4):
                factor = columns[i][r] * inverse
                if r == at:
                    factor = jnp.where(row > s, factor, 0.0)
                work[r] = work[r] - factor * chosen
                for j in ahead:
                    columns[j][r] = columns[j][r] - factor * ahead[j]
            work[at] = jnp.where(row == s, work[at] * lax.rsqrt(pivot), work[at])
    inverse = pltpu.roll(jnp.concatenate(work, axis=0), 64, 1)
    inverse_ref[...] = inverse
    left = by_layer(mine_ref, other_ref)
    for l in range(2):
        frame_ref[l] = (
            jnp.dot(
                inverse[:, l * RANK : (l + 1) * RANK],
                left[l],
                precision=EXACT,
                preferred_element_type=jnp.float32,
            )
            * (1.0 / REPLICAS)
        )


def settle(layer, right_ref, inverse_ref, frame_ref, weights_ref, momentum_ref):
    place = (lax.axis_index("zlo") * 4 + lax.axis_index("y")) * 2 + core()
    block = place // 4
    shift = (4 - place % 4) * 32
    square = jnp.zeros((8, LANES), jnp.float32)
    for i in range(32):
        tile = right_ref[i]
        square = square + tile * tile
    scale = lax.rsqrt(jnp.sum(square) * (1.0 / (RANK * 1024)) + 1e-12)
    own = jnp.concatenate([right_ref[8 * t + block] for t in range(4)], axis=0)
    inverse = inverse_ref[...]
    inverse = jnp.where(layer == 0, inverse[:, :RANK], inverse[:, RANK : 2 * RANK])
    half = jnp.dot(inverse, own, precision=EXACT, preferred_element_type=jnp.float32)
    half = pltpu.roll(half, shift, 1)[:, :RANK]
    change = lax.dot_general(
        half,
        frame_ref[layer],
        (((0,), (0,)), ((), ())),
        precision=EXACT,
        preferred_element_type=jnp.float32,
    )
    new = 0.9 * momentum_ref[layer] + change
    return scale, new, weights_ref[layer] - 0.02 * new


def scaled(right_ref, scale, basis_ref, layer):
    for t in range(4):
        for j in range(8):
            at = (slice(8 * t, 8 * t + 8), slice(LANES * j, LANES * j + LANES))
            at = at if layer is None else (layer, *at)
            basis_ref[at] = right_ref[8 * t + j] * scale


def early_body(right_ref, inverse_ref, frame_ref, weights_ref, momentum_ref, basis_ref, w_ref, m_ref):
    scale, new, weights = settle(owned(), right_ref, inverse_ref, frame_ref, weights_ref, momentum_ref)
    scaled(right_ref, scale, basis_ref, None)
    m_ref[...] = new
    w_ref[...] = weights


def late_body(
    right_ref, inverse_ref, frame_ref, weights_ref, momentum_ref, b_ref, w_ref, m_ref,
    basis_ref, new_w_ref, new_m_ref,
):
    c = owned()
    basis_ref[c] = b_ref[...]
    new_w_ref[c] = w_ref[...]
    new_m_ref[c] = m_ref[...]
    layer = 1 - c
    scale, new, weights = settle(layer, right_ref, inverse_ref, frame_ref, weights_ref, momentum_ref)
    scaled(right_ref, scale, basis_ref, layer)
    new_m_ref[layer] = new
    new_w_ref[layer] = weights


DOUBLING = ((1, 0), (3, 1), (4, 1), (8, 0))


def swapped(value):
    return lax.ppermute(value, "core", [(0, 1), (1, 0)])


def all_to_all(value, axes):
    groups = ([], [])
    for i, place in enumerate(itertools.product(*(range(SIZES[a]) for a in axes))):
        at = dict(zip(axes, place))
        groups[colour(at.get("y", 0), at.get("zlo", 0), at.get("zhi", 0), at["core"])].append(i)
    return lax.all_to_all(value, axes, 0, 0, axis_index_groups=groups, tiled=True)


def shards(layer_grads, last_basis, layer_weights, momentum):
    grads = layer_grads[0]
    layers, rows, width = grads.shape
    basis = jnp.swapaxes(last_basis, 1, 2)
    weights, momentum = jnp.swapaxes(layer_weights, 1, 2), jnp.swapaxes(momentum, 1, 2)
    lefts, rights = f32(PEERS, 8, LANES), f32(PEERS, 16, LANES)

    anywhere = pl.BlockSpec(memory_space=pltpu.HBM)
    local = pl.BlockSpec(memory_space=pltpu.VMEM)
    away, grads, basis = pl.pallas_call(
        first_body,
        out_shape=[lefts, jax.ShapeDtypeStruct(grads.shape, grads.dtype), f32(*basis.shape)],
        in_specs=[anywhere] * 2,
        out_specs=[local] * 3,
        scratch_shapes=[pltpu.SemaphoreType.DMA((9,))],
        compiler_params=pltpu.CompilerParams(vmem_limit_bytes=VMEM_LIMIT),
        cost_estimate=pl.CostEstimate(flops=1 << 20, bytes_accessed=1 << 18, transcendentals=0),
    )(*(pltpu.with_memory_space_constraint(a, pltpu.HBM) for a in (basis, grads)))
    away = swapped(away)
    mine = kernel_call(left_body, lefts)(basis, grads) + away
    for flip, cross in DOUBLING:
        pairs = [(2 * p + c, 2 * (p ^ flip) + (c ^ cross)) for p in range(16) for c in range(2)]
        mine = mine + lax.ppermute(mine, REPLICA, pairs)
    other = swapped(mine)
    away, gram = kernel_call(sent_body, [rights, f32(16, LANES)])(mine, grads)
    away = swapped(away)
    kept, share = kernel_call(kept_body, [rights, f32(4, LANES)])(other, grads, gram)

    sent = kernel_call(pack_body, f32(PEERS * CHUNK, LANES))(kept, away, share)
    came = all_to_all(sent.reshape(PEERS * CHUNK // 4, 4, LANES), PLANE)
    sent = kernel_call(plane_body, f32(STACK * CHUNK, LANES))(came.reshape(-1, LANES))
    came = all_to_all(sent.reshape(STACK * CHUNK // 4, 4, LANES), COLUMN)
    sent, gram = kernel_call(column_body, [rights, f32(16, LANES)])(came.reshape(-1, LANES))
    right = all_to_all(sent, PLANE)
    right, gram = lax.optimization_barrier((right.reshape(32, 8, LANES), gram))
    late = swapped(right)
    inverse, frame = kernel_call(factor_body, [f32(RANK, LANES), f32(layers, RANK, rows)])(
        gram, mine, other
    )
    solved = (inverse, frame, weights, momentum)
    early = kernel_call(
        early_body, [f32(RANK, width), f32(RANK, rows), f32(RANK, rows)]
    )(right, *solved)
    new_basis, new_weights, new_momentum = kernel_call(
        late_body,
        [f32(layers, RANK, width), f32(layers, RANK, rows), f32(layers, RANK, rows)],
    )(late, *solved, *early)
    return tuple(jnp.swapaxes(a, 1, 2) for a in (new_weights, new_basis, new_momentum))


def solution(mesh):
    fine = Mesh(mesh.devices.reshape(tuple(SIZES.values())), tuple(SIZES))
    sharded = P(None, MODEL, REPLICA)
    return jax.shard_map(
        shards,
        mesh=fine,
        in_specs=(P(REPLICA, None, MODEL, None), P(), sharded, sharded),
        out_specs=(sharded, P(), sharded),
        check_vma=False,
    )
```

```python
import itertools

import jax
import jax.numpy as jnp
from jax import lax
from jax.experimental import pallas as pl
from jax.experimental.pallas import tpu as pltpu
from jax.sharding import Mesh
from jax.sharding import PartitionSpec as P


RANK = 32
LANES = 128
SIZES = {"zlo": 4, "y": 4, "core": 2, "zhi": 2, "x": 4}
REPLICA = ("zlo", "y", "core")
MODEL = ("zhi", "x")
PLANE = ("y", "core", "x")
COLUMN = ("zlo", "core", "zhi")
REPLICAS, PEERS, STACK = 32, 16, 8
CHUNK = 20
BLOCK = 16
EXACT = lax.Precision.HIGHEST
VMEM_LIMIT = 24 * 1024 * 1024


def kernel_call(body, outs, flops=1 << 20, moved=1 << 18):
    many = isinstance(outs, (list, tuple))
    count = len(outs) if many else 1
    spec = pl.BlockSpec(memory_space=pltpu.VMEM)
    return lambda *args: pl.pallas_call(
        body,
        out_shape=outs,
        in_specs=[spec] * len(args),
        out_specs=[spec] * count if many else spec,
        compiler_params=pltpu.CompilerParams(vmem_limit_bytes=VMEM_LIMIT),
        cost_estimate=pl.CostEstimate(flops=flops, bytes_accessed=moved, transcendentals=0),
    )(*args)


def f32(*shape):
    return jax.ShapeDtypeStruct(shape, jnp.float32)


def joined(ref, rows, columns):
    return jnp.concatenate(
        [
            jnp.concatenate([ref[t * columns + j] for j in range(columns)], axis=1)
            for t in range(rows)
        ],
        axis=0,
    )


def lane_of(shape):
    return lax.broadcasted_iota(jnp.int32, shape, 1)


def row_of(shape):
    return lax.broadcasted_iota(jnp.int32, shape, 0)


def core():
    return lax.axis_index("core")


def colour(y, zlo, zhi, c):
    return (c + y // 2 + zlo + zhi) % 2


def held():
    return colour(lax.axis_index("y"), lax.axis_index("zlo"), lax.axis_index("zhi"), core())


def owned():
    return 1 - held()


WIDE = 256


def left_of(basis, grads):
    return lax.dot_general(
        basis.astype(jnp.bfloat16),
        grads,
        (((1,), (1,)), ((), ())),
        preferred_element_type=jnp.float32,
    )


def put_left(left, out_ref):
    for t in range(4):
        for j in range(4):
            out_ref[4 * t + j] = left[8 * t : 8 * t + 8, LANES * j : LANES * j + LANES]


def first_body(basis_hbm, grads_hbm, out_ref, grads_ref, basis_ref, sems):
    h = held()
    whole = pltpu.make_async_copy(basis_hbm, basis_ref, sems.at[8])
    whole.start()
    copies = []
    for k in range(8):
        at = (1 - h if k < 4 else h, slice(None), pl.ds(WIDE * (k % 4), WIDE))
        copies.append(pltpu.make_async_copy(grads_hbm.at[at], grads_ref.at[at], sems.at[k]))
        copies[-1].start()
    whole.wait()
    left = jnp.zeros((RANK, grads_ref.shape[1]), jnp.float32)
    for j in range(4):
        copies[j].wait()
        columns = slice(WIDE * j, WIDE * (j + 1))
        left = left + left_of(basis_ref[1 - h, :, columns], grads_ref[1 - h, :, columns])
    put_left(left, out_ref)
    for k in range(4, 8):
        copies[k].wait()


def left_body(basis_ref, grads_ref, out_ref):
    h = held()
    put_left(left_of(basis_ref[h], grads_ref[h]), out_ref)


def put_right(left, grads, out_ref):
    right = jnp.dot(left.astype(jnp.bfloat16), grads, preferred_element_type=jnp.float32)
    for t in range(4):
        for j in range(8):
            d, h = divmod(8 * t + j, 2)
            out_ref[d, 8 * h : 8 * h + 8] = right[8 * t : 8 * t + 8, LANES * j : LANES * j + LANES]


def packed_gram(left):
    gram = lax.dot_general(
        left,
        jnp.concatenate([left] * 4, axis=0),
        (((1,), (1,)), ((), ())),
        precision=EXACT,
        preferred_element_type=jnp.float32,
    )
    return jnp.where(lane_of((16, LANES)) < 64, gram[:16], gram[16:])


def sent_body(left_ref, grads_ref, out_ref, gram_ref):
    left = joined(left_ref, 4, 4)
    put_right(left, grads_ref[held()], out_ref)
    gram_ref[...] = packed_gram(left)


def kept_body(left_ref, grads_ref, gram_ref, out_ref, share_ref):
    layer = owned()
    left = joined(left_ref, 4, 4)
    put_right(left, grads_ref[layer], out_ref)
    group = lane_of((16, LANES)) // RANK % 2
    packed = jnp.where(group == layer, packed_gram(left), gram_ref[...])
    share_ref[...] = picked([packed[4 * s : 4 * s + 4] for s in range(4)], lax.axis_index("y"))


def picked(values, index):
    out = values[0]
    for s in range(1, len(values)):
        out = jnp.where(index == s, values[s], out)
    return out


def pack_body(mine_ref, other_ref, share_ref, out_ref):
    share = share_ref[...]
    for d in range(PEERS):
        out_ref[CHUNK * d : CHUNK * d + 16] = mine_ref[d] + other_ref[d]
        out_ref[CHUNK * d + 16 : CHUNK * d + CHUNK] = share


def plane_body(in_ref, out_ref):
    total = in_ref[0:16]
    for s in range(1, PEERS):
        total = total + in_ref[CHUNK * s : CHUNK * s + 16]
    parts = []
    for y in range(4):
        part = None
        for x in range(4):
            at = CHUNK * (4 * y + x) + 16
            piece = in_ref[at : at + 4]
            part = piece if part is None else part + piece
        parts.append(part)
    share = picked(parts, lax.axis_index("zlo"))
    for z in range(STACK):
        out_ref[CHUNK * z : CHUNK * z + 16] = total
        out_ref[CHUNK * z + 16 : CHUNK * z + CHUNK] = share


def column_body(in_ref, out_ref, gram_ref):
    total = in_ref[0:16]
    for s in range(1, STACK):
        total = total + in_ref[CHUNK * s : CHUNK * s + 16]
    for d in range(PEERS):
        out_ref[d] = total
    for q in range(4):
        at = 2 * CHUNK * q + 16
        gram_ref[4 * q : 4 * q + 4] = in_ref[at : at + 4] + in_ref[at + CHUNK : at + CHUNK + 4]


def inverse_factors(packed):
    turned = pltpu.roll(packed, 64, 1)
    grams = [packed[0:8], packed[8:16], turned[0:8], turned[8:16]]
    shape = (8, LANES)
    lane, row = lane_of(shape), row_of(shape)
    first = (lane // RANK) % 2 == 0
    front = lane < 64
    units = [(lane % RANK) == row + 8 * r for r in range(4)]
    diagonal = jnp.zeros(shape, jnp.float32)
    for r in range(4):
        diagonal = diagonal + jnp.where(units[r] & front, grams[r], 0.0)
    mean0 = jnp.sum(jnp.where(first, diagonal, 0.0)) * (1.0 / RANK)
    mean1 = jnp.sum(jnp.where(first, 0.0, diagonal)) * (1.0 / RANK)
    ridge = jnp.where(front, 0.001 * jnp.where(first, mean0, mean1), 1.0)
    work = [jnp.where(front, grams[r], 0.0) + jnp.where(units[r], ridge, 0.0) for r in range(4)]
    for b in range(0, RANK, BLOCK):
        columns = [
            {
                r: jnp.where(first, work[r][:, k : k + 1], work[r][:, RANK + k : RANK + k + 1])
                for r in range(b // 8, 4)
            }
            for k in range(b, b + BLOCK)
        ]
        for i in range(BLOCK):
            at, s = divmod(b + i, 8)
            pivot = columns[i][at][s : s + 1]
            inverse = 1.0 / pivot
            chosen = work[at][s : s + 1]
            ahead = {j: columns[j][at][s : s + 1] for j in range(i + 1, BLOCK)}
            for r in range(at, 4):
                factor = columns[i][r] * inverse
                if r == at:
                    factor = jnp.where(row > s, factor, 0.0)
                work[r] = work[r] - factor * chosen
                for j in ahead:
                    columns[j][r] = columns[j][r] - factor * ahead[j]
            work[at] = jnp.where(row == s, work[at] * lax.rsqrt(pivot), work[at])
    return pltpu.roll(jnp.concatenate(work, axis=0), 64, 1)


def settled(layer, right_ref, inverse, left_ref, weights_ref, momentum_ref):
    place = (lax.axis_index("zlo") * 4 + lax.axis_index("y")) * 2 + core()
    block = place // 4
    shift = (4 - place % 4) * 32
    own = jnp.concatenate([right_ref[8 * t + block] for t in range(4)], axis=0)
    own = pltpu.roll(own, shift, 1)[:, :RANK]
    inverse = jnp.where(layer == 0, inverse[:, :RANK], inverse[:, RANK : 2 * RANK])
    half = jnp.dot(inverse, own, precision=EXACT, preferred_element_type=jnp.float32)
    columns = (((0,), (0,)), ((), ()))
    mixed = lax.dot_general(
        inverse, half, columns, precision=EXACT, preferred_element_type=jnp.float32
    )
    change = lax.dot_general(
        mixed,
        joined(left_ref, 4, 4),
        columns,
        precision=EXACT,
        preferred_element_type=jnp.float32,
    )
    new = 0.9 * momentum_ref[layer] + change * (1.0 / REPLICAS)
    return new, weights_ref[layer] - 0.02 * new


def scale_of(right_ref):
    squares = [jnp.zeros((8, LANES), jnp.float32)] * 4
    for i in range(32):
        tile = right_ref[i]
        squares[i % 4] = squares[i % 4] + tile * tile
    square = (squares[0] + squares[1]) + (squares[2] + squares[3])
    return lax.rsqrt(jnp.sum(square) * (1.0 / (RANK * 1024)) + 1e-12)


def put_scaled(right_ref, scale, t, basis_ref):
    for j in range(8):
        at = (slice(8 * t, 8 * t + 8), slice(LANES * j, LANES * j + LANES))
        basis_ref[at] = right_ref[8 * t + j] * scale


def early_body(
    gram_ref, right_ref, left_ref, weights_ref, momentum_ref, inverse_ref, basis_ref, w_ref, m_ref
):
    inverse = inverse_factors(gram_ref[...])
    inverse_ref[...] = inverse
    scale = scale_of(right_ref)
    for t in range(4):
        put_scaled(right_ref, scale, t, basis_ref)
    m_ref[...], w_ref[...] = settled(
        owned(), right_ref, inverse, left_ref, weights_ref, momentum_ref
    )


def late_body(
    right_ref, left_ref, weights_ref, momentum_ref, inverse_ref, b_ref, w_ref, m_ref,
    basis_hbm, w_hbm, m_hbm, basis_ref, new_w_ref, new_m_ref, sems,
):
    layer = held()
    copies = []

    def send(source, target):
        copies.append(pltpu.make_async_copy(source, target, sems.at[len(copies)]))
        copies[-1].start()

    send(b_ref, basis_hbm.at[1 - layer])
    send(w_ref, w_hbm.at[1 - layer])
    send(m_ref, m_hbm.at[1 - layer])
    new, weights = settled(
        layer, right_ref, inverse_ref[...], left_ref, weights_ref, momentum_ref
    )
    scale = scale_of(right_ref)
    for t in range(4):
        put_scaled(right_ref, scale, t, basis_ref)
        rows = slice(8 * t, 8 * t + 8)
        send(basis_ref.at[rows], basis_hbm.at[layer, rows])
    new_m_ref[...] = new
    send(new_m_ref, m_hbm.at[layer])
    new_w_ref[...] = weights
    send(new_w_ref, w_hbm.at[layer])
    for copy in copies:
        copy.wait()


def last(right, left, weights, momentum, early):
    local, far = pl.BlockSpec(memory_space=pltpu.VMEM), pl.BlockSpec(memory_space=pltpu.HBM)
    shapes = [early[1].shape, early[2].shape, early[3].shape]
    return pl.pallas_call(
        late_body,
        out_shape=[f32(2, *shape) for shape in shapes],
        in_specs=[local] * 8,
        out_specs=[far] * 3,
        scratch_shapes=[
            *(pltpu.VMEM(shape, jnp.float32) for shape in shapes),
            pltpu.SemaphoreType.DMA((9,)),
        ],
        compiler_params=pltpu.CompilerParams(vmem_limit_bytes=VMEM_LIMIT),
        cost_estimate=pl.CostEstimate(flops=1 << 20, bytes_accessed=1 << 18, transcendentals=0),
    )(right, left, weights, momentum, *early)


DOUBLING = ((1, 0), (3, 1), (4, 1), (8, 0))


def swapped(value):
    return lax.ppermute(value, "core", [(0, 1), (1, 0)])


def all_to_all(value, axes):
    groups = ([], [])
    for i, place in enumerate(itertools.product(*(range(SIZES[a]) for a in axes))):
        at = dict(zip(axes, place))
        groups[colour(at.get("y", 0), at.get("zlo", 0), at.get("zhi", 0), at["core"])].append(i)
    return lax.all_to_all(value, axes, 0, 0, axis_index_groups=groups, tiled=True)


def shards(layer_grads, last_basis, layer_weights, momentum):
    grads = layer_grads[0]
    _, rows, width = grads.shape
    basis = jnp.swapaxes(last_basis, 1, 2)
    weights, momentum = jnp.swapaxes(layer_weights, 1, 2), jnp.swapaxes(momentum, 1, 2)
    lefts, rights = f32(PEERS, 8, LANES), f32(PEERS, 16, LANES)

    anywhere = pl.BlockSpec(memory_space=pltpu.HBM)
    local = pl.BlockSpec(memory_space=pltpu.VMEM)
    away, grads, basis = pl.pallas_call(
        first_body,
        out_shape=[lefts, jax.ShapeDtypeStruct(grads.shape, grads.dtype), f32(*basis.shape)],
        in_specs=[anywhere] * 2,
        out_specs=[local] * 3,
        scratch_shapes=[pltpu.SemaphoreType.DMA((9,))],
        compiler_params=pltpu.CompilerParams(vmem_limit_bytes=VMEM_LIMIT),
        cost_estimate=pl.CostEstimate(flops=1 << 20, bytes_accessed=1 << 18, transcendentals=0),
    )(*(pltpu.with_memory_space_constraint(a, pltpu.HBM) for a in (basis, grads)))
    away = swapped(away)
    mine = kernel_call(left_body, lefts)(basis, grads) + away
    for flip, cross in DOUBLING:
        pairs = [(2 * p + c, 2 * (p ^ flip) + (c ^ cross)) for p in range(16) for c in range(2)]
        mine = mine + lax.ppermute(mine, REPLICA, pairs)
    other = swapped(mine)
    away, gram = kernel_call(sent_body, [rights, f32(16, LANES)])(mine, grads)
    away = swapped(away)
    kept, share = kernel_call(kept_body, [rights, f32(4, LANES)])(other, grads, gram)

    sent = kernel_call(pack_body, f32(PEERS * CHUNK, LANES))(kept, away, share)
    came = all_to_all(sent.reshape(PEERS * CHUNK // 4, 4, LANES), PLANE)
    sent = kernel_call(plane_body, f32(STACK * CHUNK, LANES))(came.reshape(-1, LANES))
    came = all_to_all(sent.reshape(STACK * CHUNK // 4, 4, LANES), COLUMN)
    sent, gram = kernel_call(column_body, [rights, f32(16, LANES)])(came.reshape(-1, LANES))
    right = all_to_all(sent, PLANE)
    right, gram = lax.optimization_barrier((right.reshape(32, 8, LANES), gram))
    late = swapped(right)
    early = kernel_call(
        early_body, [f32(RANK, LANES), f32(RANK, width), f32(RANK, rows), f32(RANK, rows)]
    )(gram, right, other, weights, momentum)
    new_basis, new_weights, new_momentum = last(late, mine, weights, momentum, early)
    return tuple(jnp.swapaxes(a, 1, 2) for a in (new_weights, new_basis, new_momentum))


def solution(mesh):
    fine = Mesh(mesh.devices.reshape(tuple(SIZES.values())), tuple(SIZES))
    sharded = P(None, MODEL, REPLICA)
    return jax.shard_map(
        shards,
        mesh=fine,
        in_specs=(P(REPLICA, None, MODEL, None), P(), sharded, sharded),
        out_specs=(sharded, P(), sharded),
        check_vma=False,
    )
```

```python
import itertools

import jax
import jax.numpy as jnp
from jax import lax
from jax.experimental import pallas as pl
from jax.experimental.pallas import tpu as pltpu
from jax.sharding import Mesh
from jax.sharding import PartitionSpec as P


RANK = 32
LANES = 128
SIZES = {"zlo": 4, "y": 4, "core": 2, "zhi": 2, "x": 4}
REPLICA = ("zlo", "y", "core")
MODEL = ("zhi", "x")
PLANE = ("y", "core", "x")
COLUMN = ("zlo", "core", "zhi")
REPLICAS, PEERS, STACK = 32, 16, 8
CHUNK = 20
BLOCK = 16
EXACT = lax.Precision.HIGHEST
VMEM_LIMIT = 24 * 1024 * 1024


def kernel_call(body, outs, flops=1 << 20, moved=1 << 18):
    many = isinstance(outs, (list, tuple))
    count = len(outs) if many else 1
    spec = pl.BlockSpec(memory_space=pltpu.VMEM)
    return lambda *args: pl.pallas_call(
        body,
        out_shape=outs,
        in_specs=[spec] * len(args),
        out_specs=[spec] * count if many else spec,
        compiler_params=pltpu.CompilerParams(vmem_limit_bytes=VMEM_LIMIT),
        cost_estimate=pl.CostEstimate(flops=flops, bytes_accessed=moved, transcendentals=0),
    )(*args)


def f32(*shape):
    return jax.ShapeDtypeStruct(shape, jnp.float32)


def joined(ref, rows, columns):
    return jnp.concatenate(
        [
            jnp.concatenate([ref[t * columns + j] for j in range(columns)], axis=1)
            for t in range(rows)
        ],
        axis=0,
    )


def lane_of(shape):
    return lax.broadcasted_iota(jnp.int32, shape, 1)


def row_of(shape):
    return lax.broadcasted_iota(jnp.int32, shape, 0)


def core():
    return lax.axis_index("core")


def colour(y, zlo, zhi, c):
    return (c + y // 2 + zlo + zhi) % 2


def held():
    return colour(lax.axis_index("y"), lax.axis_index("zlo"), lax.axis_index("zhi"), core())


def owned():
    return 1 - held()


WIDE = 256


def left_of(basis, grads):
    return lax.dot_general(
        basis.astype(jnp.bfloat16),
        grads,
        (((1,), (1,)), ((), ())),
        preferred_element_type=jnp.float32,
    )


def put_left(left, out_ref):
    for t in range(4):
        for j in range(4):
            out_ref[4 * t + j] = left[8 * t : 8 * t + 8, LANES * j : LANES * j + LANES]


def first_body(basis_hbm, grads_hbm, out_ref, grads_ref, basis_ref, sems):
    h = held()
    whole = pltpu.make_async_copy(basis_hbm, basis_ref, sems.at[8])
    whole.start()
    copies = []
    for k in range(8):
        at = (1 - h if k < 4 else h, slice(None), pl.ds(WIDE * (k % 4), WIDE))
        copies.append(pltpu.make_async_copy(grads_hbm.at[at], grads_ref.at[at], sems.at[k]))
        copies[-1].start()
    whole.wait()
    left = jnp.zeros((RANK, grads_ref.shape[1]), jnp.float32)
    for j in range(4):
        copies[j].wait()
        columns = slice(WIDE * j, WIDE * (j + 1))
        left = left + left_of(basis_ref[1 - h, :, columns], grads_ref[1 - h, :, columns])
    put_left(left, out_ref)
    for k in range(4, 8):
        copies[k].wait()


def left_body(basis_ref, grads_ref, out_ref):
    h = held()
    put_left(left_of(basis_ref[h], grads_ref[h]), out_ref)


def put_right(left, grads, out_ref):
    right = jnp.dot(left.astype(jnp.bfloat16), grads, preferred_element_type=jnp.float32)
    for t in range(4):
        for j in range(8):
            d, h = divmod(8 * t + j, 2)
            out_ref[d, 8 * h : 8 * h + 8] = right[8 * t : 8 * t + 8, LANES * j : LANES * j + LANES]


def packed_gram(left):
    gram = lax.dot_general(
        left,
        jnp.concatenate([left] * 4, axis=0),
        (((1,), (1,)), ((), ())),
        precision=EXACT,
        preferred_element_type=jnp.float32,
    )
    return jnp.where(lane_of((16, LANES)) < 64, gram[:16], gram[16:])


def sent_body(left_ref, grads_ref, out_ref):
    put_right(joined(left_ref, 4, 4), grads_ref[held()], out_ref)


def kept_body(mine_ref, other_ref, grads_ref, out_ref, share_ref):
    layer = owned()
    left = joined(other_ref, 4, 4)
    put_right(left, grads_ref[layer], out_ref)
    group = lane_of((16, LANES)) // RANK % 2
    packed = jnp.where(group == layer, packed_gram(left), packed_gram(joined(mine_ref, 4, 4)))
    share_ref[...] = picked([packed[4 * s : 4 * s + 4] for s in range(4)], lax.axis_index("y"))


def picked(values, index):
    out = values[0]
    for s in range(1, len(values)):
        out = jnp.where(index == s, values[s], out)
    return out


def pack_body(mine_ref, other_ref, share_ref, out_ref):
    share = share_ref[...]
    for d in range(PEERS):
        out_ref[CHUNK * d : CHUNK * d + 16] = mine_ref[d] + other_ref[d]
        out_ref[CHUNK * d + 16 : CHUNK * d + CHUNK] = share


def plane_body(in_ref, out_ref):
    total = in_ref[0:16]
    for s in range(1, PEERS):
        total = total + in_ref[CHUNK * s : CHUNK * s + 16]
    parts = []
    for y in range(4):
        part = None
        for x in range(4):
            at = CHUNK * (4 * y + x) + 16
            piece = in_ref[at : at + 4]
            part = piece if part is None else part + piece
        parts.append(part)
    share = picked(parts, lax.axis_index("zlo"))
    for z in range(STACK):
        out_ref[CHUNK * z : CHUNK * z + 16] = total
        out_ref[CHUNK * z + 16 : CHUNK * z + CHUNK] = share


def column_body(in_ref, out_ref, gram_ref):
    total = in_ref[0:16]
    for s in range(1, STACK):
        total = total + in_ref[CHUNK * s : CHUNK * s + 16]
    for d in range(PEERS):
        out_ref[d] = total
    for q in range(4):
        at = 2 * CHUNK * q + 16
        gram_ref[4 * q : 4 * q + 4] = in_ref[at : at + 4] + in_ref[at + CHUNK : at + CHUNK + 4]


def inverse_factors(packed):
    turned = pltpu.roll(packed, 64, 1)
    grams = [packed[0:8], packed[8:16], turned[0:8], turned[8:16]]
    shape = (8, LANES)
    lane, row = lane_of(shape), row_of(shape)
    first = (lane // RANK) % 2 == 0
    front = lane < 64
    units = [(lane % RANK) == row + 8 * r for r in range(4)]
    diagonal = jnp.zeros(shape, jnp.float32)
    for r in range(4):
        diagonal = diagonal + jnp.where(units[r] & front, grams[r], 0.0)
    mean0 = jnp.sum(jnp.where(first, diagonal, 0.0)) * (1.0 / RANK)
    mean1 = jnp.sum(jnp.where(first, 0.0, diagonal)) * (1.0 / RANK)
    ridge = jnp.where(front, 0.001 * jnp.where(first, mean0, mean1), 1.0)
    work = [jnp.where(front, grams[r], 0.0) + jnp.where(units[r], ridge, 0.0) for r in range(4)]
    for b in range(0, RANK, BLOCK):
        columns = [
            {
                r: jnp.where(first, work[r][:, k : k + 1], work[r][:, RANK + k : RANK + k + 1])
                for r in range(b // 8, 4)
            }
            for k in range(b, b + BLOCK)
        ]
        for i in range(BLOCK):
            at, s = divmod(b + i, 8)
            pivot = columns[i][at][s : s + 1]
            inverse = 1.0 / pivot
            chosen = work[at][s : s + 1]
            ahead = {j: columns[j][at][s : s + 1] for j in range(i + 1, BLOCK)}
            for r in range(at, 4):
                factor = columns[i][r] * inverse
                if r == at:
                    factor = jnp.where(row > s, factor, 0.0)
                work[r] = work[r] - factor * chosen
                for j in ahead:
                    columns[j][r] = columns[j][r] - factor * ahead[j]
            work[at] = jnp.where(row == s, work[at] * lax.rsqrt(pivot), work[at])
    return pltpu.roll(jnp.concatenate(work, axis=0), 64, 1)


def settled(layer, right_ref, inverse, left_ref, weights_ref, momentum_ref):
    place = (lax.axis_index("zlo") * 4 + lax.axis_index("y")) * 2 + core()
    block = place // 4
    shift = (4 - place % 4) * 32
    own = jnp.concatenate([right_ref[8 * t + block] for t in range(4)], axis=0)
    own = pltpu.roll(own, shift, 1)[:, :RANK]
    inverse = jnp.where(layer == 0, inverse[:, :RANK], inverse[:, RANK : 2 * RANK])
    half = jnp.dot(inverse, own, precision=EXACT, preferred_element_type=jnp.float32)
    columns = (((0,), (0,)), ((), ()))
    mixed = lax.dot_general(
        inverse, half, columns, precision=EXACT, preferred_element_type=jnp.float32
    )
    change = lax.dot_general(
        mixed,
        joined(left_ref, 4, 4),
        columns,
        precision=EXACT,
        preferred_element_type=jnp.float32,
    )
    new = 0.9 * momentum_ref[layer] + change * (1.0 / REPLICAS)
    return new, weights_ref[layer] - 0.02 * new


def scale_of(right_ref):
    squares = [jnp.zeros((8, LANES), jnp.float32)] * 4
    for i in range(32):
        tile = right_ref[i]
        squares[i % 4] = squares[i % 4] + tile * tile
    square = (squares[0] + squares[1]) + (squares[2] + squares[3])
    return lax.rsqrt(jnp.sum(square) * (1.0 / (RANK * 1024)) + 1e-12)


def put_scaled(right_ref, scale, t, basis_ref):
    for j in range(8):
        at = (slice(8 * t, 8 * t + 8), slice(LANES * j, LANES * j + LANES))
        basis_ref[at] = right_ref[8 * t + j] * scale


def early_body(
    gram_ref, right_ref, left_ref, weights_ref, momentum_ref, inverse_ref, basis_ref, w_ref, m_ref
):
    inverse = inverse_factors(gram_ref[...])
    inverse_ref[...] = inverse
    scale = scale_of(right_ref)
    for t in range(4):
        put_scaled(right_ref, scale, t, basis_ref)
    m_ref[...], w_ref[...] = settled(
        owned(), right_ref, inverse, left_ref, weights_ref, momentum_ref
    )


def late_body(
    right_ref, left_ref, weights_ref, momentum_ref, inverse_ref, b_ref, w_ref, m_ref,
    basis_hbm, w_hbm, m_hbm, basis_ref, new_w_ref, new_m_ref, sems,
):
    layer = held()
    copies = []

    def send(source, target):
        copies.append(pltpu.make_async_copy(source, target, sems.at[len(copies)]))
        copies[-1].start()

    send(b_ref, basis_hbm.at[1 - layer])
    send(w_ref, w_hbm.at[1 - layer])
    send(m_ref, m_hbm.at[1 - layer])
    new, weights = settled(
        layer, right_ref, inverse_ref[...], left_ref, weights_ref, momentum_ref
    )
    scale = scale_of(right_ref)
    for t in range(4):
        put_scaled(right_ref, scale, t, basis_ref)
        rows = slice(8 * t, 8 * t + 8)
        send(basis_ref.at[rows], basis_hbm.at[layer, rows])
    new_m_ref[...] = new
    send(new_m_ref, m_hbm.at[layer])
    new_w_ref[...] = weights
    send(new_w_ref, w_hbm.at[layer])
    for copy in copies:
        copy.wait()


def last(right, left, weights, momentum, early):
    local, far = pl.BlockSpec(memory_space=pltpu.VMEM), pl.BlockSpec(memory_space=pltpu.HBM)
    shapes = [early[1].shape, early[2].shape, early[3].shape]
    return pl.pallas_call(
        late_body,
        out_shape=[f32(2, *shape) for shape in shapes],
        in_specs=[local] * 8,
        out_specs=[far] * 3,
        scratch_shapes=[
            *(pltpu.VMEM(shape, jnp.float32) for shape in shapes),
            pltpu.SemaphoreType.DMA((9,)),
        ],
        compiler_params=pltpu.CompilerParams(vmem_limit_bytes=VMEM_LIMIT),
        cost_estimate=pl.CostEstimate(flops=1 << 20, bytes_accessed=1 << 18, transcendentals=0),
    )(right, left, weights, momentum, *early)


DOUBLING = ((1, 0), (3, 1), (4, 1), (8, 0))


def swapped(value):
    return lax.ppermute(value, "core", [(0, 1), (1, 0)])


def all_to_all(value, axes):
    groups = ([], [])
    for i, place in enumerate(itertools.product(*(range(SIZES[a]) for a in axes))):
        at = dict(zip(axes, place))
        groups[colour(at.get("y", 0), at.get("zlo", 0), at.get("zhi", 0), at["core"])].append(i)
    return lax.all_to_all(value, axes, 0, 0, axis_index_groups=groups, tiled=True)


def shards(layer_grads, last_basis, layer_weights, momentum):
    grads = layer_grads[0]
    _, rows, width = grads.shape
    basis = jnp.swapaxes(last_basis, 1, 2)
    weights, momentum = jnp.swapaxes(layer_weights, 1, 2), jnp.swapaxes(momentum, 1, 2)
    lefts, rights = f32(PEERS, 8, LANES), f32(PEERS, 16, LANES)

    anywhere = pl.BlockSpec(memory_space=pltpu.HBM)
    local = pl.BlockSpec(memory_space=pltpu.VMEM)
    away, grads, basis = pl.pallas_call(
        first_body,
        out_shape=[lefts, jax.ShapeDtypeStruct(grads.shape, grads.dtype), f32(*basis.shape)],
        in_specs=[anywhere] * 2,
        out_specs=[local] * 3,
        scratch_shapes=[pltpu.SemaphoreType.DMA((9,))],
        compiler_params=pltpu.CompilerParams(vmem_limit_bytes=VMEM_LIMIT),
        cost_estimate=pl.CostEstimate(flops=1 << 20, bytes_accessed=1 << 18, transcendentals=0),
    )(*(pltpu.with_memory_space_constraint(a, pltpu.HBM) for a in (basis, grads)))
    away = swapped(away)
    mine = kernel_call(left_body, lefts)(basis, grads) + away
    for flip, cross in DOUBLING:
        pairs = [(2 * p + c, 2 * (p ^ flip) + (c ^ cross)) for p in range(16) for c in range(2)]
        mine = mine + lax.ppermute(mine, REPLICA, pairs)
    other = swapped(mine)
    away = kernel_call(sent_body, rights)(mine, grads)
    away = swapped(away)
    kept, share = kernel_call(kept_body, [rights, f32(4, LANES)])(mine, other, grads)

    sent = kernel_call(pack_body, f32(PEERS * CHUNK, LANES))(kept, away, share)
    came = all_to_all(sent.reshape(PEERS * CHUNK // 4, 4, LANES), PLANE)
    sent = kernel_call(plane_body, f32(STACK * CHUNK, LANES))(came.reshape(-1, LANES))
    came = all_to_all(sent.reshape(STACK * CHUNK // 4, 4, LANES), COLUMN)
    sent, gram = kernel_call(column_body, [rights, f32(16, LANES)])(came.reshape(-1, LANES))
    right = all_to_all(sent, PLANE)
    right, gram = lax.optimization_barrier((right.reshape(32, 8, LANES), gram))
    late = swapped(right)
    early = kernel_call(
        early_body, [f32(RANK, LANES), f32(RANK, width), f32(RANK, rows), f32(RANK, rows)]
    )(gram, right, other, weights, momentum)
    new_basis, new_weights, new_momentum = last(late, mine, weights, momentum, early)
    return tuple(jnp.swapaxes(a, 1, 2) for a in (new_weights, new_basis, new_momentum))


def solution(mesh):
    fine = Mesh(mesh.devices.reshape(tuple(SIZES.values())), tuple(SIZES))
    sharded = P(None, MODEL, REPLICA)
    return jax.shard_map(
        shards,
        mesh=fine,
        in_specs=(P(REPLICA, None, MODEL, None), P(), sharded, sharded),
        out_specs=(sharded, P(), sharded),
        check_vma=False,
    )
```

```python
import itertools

import jax
import jax.numpy as jnp
from jax import lax
from jax.experimental import pallas as pl
from jax.experimental.pallas import tpu as pltpu
from jax.sharding import Mesh
from jax.sharding import PartitionSpec as P


RANK = 32
LANES = 128
SIZES = {"zlo": 4, "y": 4, "core": 2, "zhi": 2, "x": 4}
REPLICA = ("zlo", "y", "core")
MODEL = ("zhi", "x")
PLANE = ("y", "core", "x")
COLUMN = ("zlo", "core", "zhi")
REPLICAS, PEERS, STACK = 32, 16, 8
CHUNK = 20
BLOCK = 16
EXACT = lax.Precision.HIGHEST
VMEM_LIMIT = 24 * 1024 * 1024


def kernel_call(body, outs, flops=1 << 20, moved=1 << 18):
    many = isinstance(outs, (list, tuple))
    count = len(outs) if many else 1
    spec = pl.BlockSpec(memory_space=pltpu.VMEM)
    return lambda *args: pl.pallas_call(
        body,
        out_shape=outs,
        in_specs=[spec] * len(args),
        out_specs=[spec] * count if many else spec,
        compiler_params=pltpu.CompilerParams(vmem_limit_bytes=VMEM_LIMIT),
        cost_estimate=pl.CostEstimate(flops=flops, bytes_accessed=moved, transcendentals=0),
    )(*args)


def f32(*shape):
    return jax.ShapeDtypeStruct(shape, jnp.float32)


def joined(ref, rows, columns):
    return jnp.concatenate(
        [
            jnp.concatenate([ref[t * columns + j] for j in range(columns)], axis=1)
            for t in range(rows)
        ],
        axis=0,
    )


def lane_of(shape):
    return lax.broadcasted_iota(jnp.int32, shape, 1)


def row_of(shape):
    return lax.broadcasted_iota(jnp.int32, shape, 0)


def core():
    return lax.axis_index("core")


def colour(y, zlo, zhi, c):
    return (c + y // 2 + zlo + zhi) % 2


def held():
    return colour(lax.axis_index("y"), lax.axis_index("zlo"), lax.axis_index("zhi"), core())


def owned():
    return 1 - held()


WIDE = 256


def left_of(basis, grads):
    return lax.dot_general(
        basis.astype(jnp.bfloat16),
        grads,
        (((1,), (1,)), ((), ())),
        preferred_element_type=jnp.float32,
    )


def put_left(left, out_ref):
    for t in range(4):
        for j in range(4):
            out_ref[4 * t + j] = left[8 * t : 8 * t + 8, LANES * j : LANES * j + LANES]


def first_body(basis_hbm, grads_hbm, out_ref, grads_ref, basis_ref, sems):
    h = held()
    whole = pltpu.make_async_copy(basis_hbm, basis_ref, sems.at[8])
    whole.start()
    copies = []
    for k in range(8):
        at = (1 - h if k < 4 else h, slice(None), pl.ds(WIDE * (k % 4), WIDE))
        copies.append(pltpu.make_async_copy(grads_hbm.at[at], grads_ref.at[at], sems.at[k]))
        copies[-1].start()
    whole.wait()
    left = jnp.zeros((RANK, grads_ref.shape[1]), jnp.float32)
    for j in range(4):
        copies[j].wait()
        columns = slice(WIDE * j, WIDE * (j + 1))
        left = left + left_of(basis_ref[1 - h, :, columns], grads_ref[1 - h, :, columns])
    put_left(left, out_ref)
    for k in range(4, 8):
        copies[k].wait()


def left_body(basis_ref, grads_ref, out_ref):
    h = held()
    put_left(left_of(basis_ref[h], grads_ref[h]), out_ref)


def put_right(left, grads, out_ref):
    right = jnp.dot(left.astype(jnp.bfloat16), grads, preferred_element_type=jnp.float32)
    for t in range(4):
        for j in range(8):
            d, h = divmod(8 * t + j, 2)
            out_ref[d, 8 * h : 8 * h + 8] = right[8 * t : 8 * t + 8, LANES * j : LANES * j + LANES]


def packed_gram(left):
    gram = lax.dot_general(
        left,
        jnp.concatenate([left] * 4, axis=0),
        (((1,), (1,)), ((), ())),
        precision=EXACT,
        preferred_element_type=jnp.float32,
    )
    return jnp.where(lane_of((16, LANES)) < 64, gram[:16], gram[16:])


def sent_body(left_ref, grads_ref, out_ref):
    put_right(joined(left_ref, 4, 4), grads_ref[held()], out_ref)


def kept_body(mine_ref, other_ref, grads_ref, out_ref, share_ref):
    layer = owned()
    left = joined(other_ref, 4, 4)
    put_right(left, grads_ref[layer], out_ref)
    group = lane_of((16, LANES)) // RANK % 2
    packed = jnp.where(group == layer, packed_gram(left), packed_gram(joined(mine_ref, 4, 4)))
    share_ref[...] = picked([packed[4 * s : 4 * s + 4] for s in range(4)], lax.axis_index("y"))


def picked(values, index):
    out = values[0]
    for s in range(1, len(values)):
        out = jnp.where(index == s, values[s], out)
    return out


def pack_body(mine_ref, other_ref, share_ref, out_ref):
    share = share_ref[...]
    for d in range(PEERS):
        out_ref[CHUNK * d : CHUNK * d + 16] = mine_ref[d] + other_ref[d]
        out_ref[CHUNK * d + 16 : CHUNK * d + CHUNK] = share


def plane_body(in_ref, out_ref):
    total = in_ref[0:16]
    for s in range(1, PEERS):
        total = total + in_ref[CHUNK * s : CHUNK * s + 16]
    parts = []
    for y in range(4):
        part = None
        for x in range(4):
            at = CHUNK * (4 * y + x) + 16
            piece = in_ref[at : at + 4]
            part = piece if part is None else part + piece
        parts.append(part)
    share = picked(parts, lax.axis_index("zlo"))
    for z in range(STACK):
        out_ref[CHUNK * z : CHUNK * z + 16] = total
        out_ref[CHUNK * z + 16 : CHUNK * z + CHUNK] = share


def column_body(in_ref, out_ref, gram_ref):
    total = in_ref[0:16]
    for s in range(1, STACK):
        total = total + in_ref[CHUNK * s : CHUNK * s + 16]
    for d in range(PEERS):
        out_ref[d] = total
    for q in range(4):
        at = 2 * CHUNK * q + 16
        gram_ref[4 * q : 4 * q + 4] = in_ref[at : at + 4] + in_ref[at + CHUNK : at + CHUNK + 4]


def inverse_factors(packed):
    turned = pltpu.roll(packed, 64, 1)
    grams = [packed[0:8], packed[8:16], turned[0:8], turned[8:16]]
    shape = (8, LANES)
    lane, row = lane_of(shape), row_of(shape)
    first = (lane // RANK) % 2 == 0
    front = lane < 64
    units = [(lane % RANK) == row + 8 * r for r in range(4)]
    diagonal = jnp.zeros(shape, jnp.float32)
    for r in range(4):
        diagonal = diagonal + jnp.where(units[r] & front, grams[r], 0.0)
    mean0 = jnp.sum(jnp.where(first, diagonal, 0.0)) * (1.0 / RANK)
    mean1 = jnp.sum(jnp.where(first, 0.0, diagonal)) * (1.0 / RANK)
    ridge = jnp.where(front, 0.001 * jnp.where(first, mean0, mean1), 1.0)
    work = [jnp.where(front, grams[r], 0.0) + jnp.where(units[r], ridge, 0.0) for r in range(4)]
    for b in range(0, RANK, BLOCK):
        columns = [
            {
                r: jnp.where(first, work[r][:, k : k + 1], work[r][:, RANK + k : RANK + k + 1])
                for r in range(b // 8, 4)
            }
            for k in range(b, b + BLOCK)
        ]
        for i in range(BLOCK):
            at, s = divmod(b + i, 8)
            pivot = columns[i][at][s : s + 1]
            inverse = 1.0 / pivot
            chosen = work[at][s : s + 1]
            ahead = {j: columns[j][at][s : s + 1] for j in range(i + 1, BLOCK)}
            for r in range(at, 4):
                factor = columns[i][r] * inverse
                if r == at:
                    factor = jnp.where(row > s, factor, 0.0)
                work[r] = work[r] - factor * chosen
                for j in ahead:
                    columns[j][r] = columns[j][r] - factor * ahead[j]
            work[at] = jnp.where(row == s, work[at] * lax.rsqrt(pivot), work[at])
    return pltpu.roll(jnp.concatenate(work, axis=0), 64, 1)


def settled(layer, right_ref, inverse, left_ref, weights_ref, momentum_ref):
    place = (lax.axis_index("zlo") * 4 + lax.axis_index("y")) * 2 + core()
    block = place // 4
    shift = (4 - place % 4) * 32
    own = jnp.concatenate([right_ref[8 * t + block] for t in range(4)], axis=0)
    own = pltpu.roll(own, shift, 1)[:, :RANK]
    inverse = jnp.where(layer == 0, inverse[:, :RANK], inverse[:, RANK : 2 * RANK])
    half = jnp.dot(inverse, own, precision=EXACT, preferred_element_type=jnp.float32)
    columns = (((0,), (0,)), ((), ()))
    mixed = lax.dot_general(
        inverse, half, columns, precision=EXACT, preferred_element_type=jnp.float32
    )
    change = lax.dot_general(
        mixed,
        joined(left_ref, 4, 4),
        columns,
        precision=EXACT,
        preferred_element_type=jnp.float32,
    )
    new = 0.9 * momentum_ref[layer] + change * (1.0 / REPLICAS)
    return new, weights_ref[layer] - 0.02 * new


def scale_of(right_ref):
    squares = [jnp.zeros((8, LANES), jnp.float32)] * 4
    for i in range(32):
        tile = right_ref[i]
        squares[i % 4] = squares[i % 4] + tile * tile
    square = (squares[0] + squares[1]) + (squares[2] + squares[3])
    return lax.rsqrt(jnp.sum(square) * (1.0 / (RANK * 1024)) + 1e-12)


def put_scaled(right_ref, scale, t, basis_ref):
    for j in range(8):
        at = (slice(8 * t, 8 * t + 8), slice(LANES * j, LANES * j + LANES))
        basis_ref[at] = right_ref[8 * t + j] * scale


def early_body(
    gram_ref, right_ref, left_ref, weights_ref, momentum_ref, inverse_ref, basis_ref, w_ref, m_ref
):
    inverse = inverse_factors(gram_ref[...])
    inverse_ref[...] = inverse
    scale = scale_of(right_ref)
    for t in range(4):
        put_scaled(right_ref, scale, t, basis_ref)
    m_ref[...], w_ref[...] = settled(
        owned(), right_ref, inverse, left_ref, weights_ref, momentum_ref
    )


def late_body(
    right_ref, left_ref, weights_ref, momentum_ref, inverse_ref, b_ref, w_ref, m_ref,
    basis_hbm, w_hbm, m_hbm, basis_ref, new_w_ref, new_m_ref, sems,
):
    layer = held()
    copies = []

    def send(source, target):
        copies.append(pltpu.make_async_copy(source, target, sems.at[len(copies)]))
        copies[-1].start()

    send(b_ref, basis_hbm.at[1 - layer])
    send(w_ref, w_hbm.at[1 - layer])
    send(m_ref, m_hbm.at[1 - layer])
    new, weights = settled(
        layer, right_ref, inverse_ref[...], left_ref, weights_ref, momentum_ref
    )
    scale = scale_of(right_ref)
    for t in range(4):
        put_scaled(right_ref, scale, t, basis_ref)
        rows = slice(8 * t, 8 * t + 8)
        send(basis_ref.at[rows], basis_hbm.at[layer, rows])
    new_m_ref[...] = new
    send(new_m_ref, m_hbm.at[layer])
    new_w_ref[...] = weights
    send(new_w_ref, w_hbm.at[layer])
    for copy in copies:
        copy.wait()


def last(right, left, weights, momentum, early):
    local, far = pl.BlockSpec(memory_space=pltpu.VMEM), pl.BlockSpec(memory_space=pltpu.HBM)
    shapes = [early[1].shape, early[2].shape, early[3].shape]
    return pl.pallas_call(
        late_body,
        out_shape=[f32(2, *shape) for shape in shapes],
        in_specs=[local] * 8,
        out_specs=[far] * 3,
        scratch_shapes=[
            *(pltpu.VMEM(shape, jnp.float32) for shape in shapes),
            pltpu.SemaphoreType.DMA((9,)),
        ],
        compiler_params=pltpu.CompilerParams(vmem_limit_bytes=VMEM_LIMIT),
        cost_estimate=pl.CostEstimate(flops=1 << 20, bytes_accessed=1 << 18, transcendentals=0),
    )(right, left, weights, momentum, *early)


DOUBLING = ((1, 0), (3, 1), (4, 1), (8, 0))


def swapped(value):
    return lax.ppermute(value, "core", [(0, 1), (1, 0)])


def all_to_all(value, axes):
    groups = ([], [])
    for i, place in enumerate(itertools.product(*(range(SIZES[a]) for a in axes))):
        at = dict(zip(axes, place))
        groups[colour(at.get("y", 0), at.get("zlo", 0), at.get("zhi", 0), at["core"])].append(i)
    return lax.all_to_all(value, axes, 0, 0, axis_index_groups=groups, tiled=True)


def shards(layer_grads, last_basis, layer_weights, momentum):
    grads = layer_grads[0]
    _, rows, width = grads.shape
    basis = jnp.swapaxes(last_basis, 1, 2)
    weights, momentum = jnp.swapaxes(layer_weights, 1, 2), jnp.swapaxes(momentum, 1, 2)
    lefts, rights = f32(PEERS, 8, LANES), f32(PEERS, 16, LANES)

    anywhere = pl.BlockSpec(memory_space=pltpu.HBM)
    local = pl.BlockSpec(memory_space=pltpu.VMEM)
    away, grads, basis = pl.pallas_call(
        first_body,
        out_shape=[lefts, jax.ShapeDtypeStruct(grads.shape, grads.dtype), f32(*basis.shape)],
        in_specs=[anywhere] * 2,
        out_specs=[local] * 3,
        scratch_shapes=[pltpu.SemaphoreType.DMA((9,))],
        compiler_params=pltpu.CompilerParams(vmem_limit_bytes=VMEM_LIMIT),
        cost_estimate=pl.CostEstimate(flops=1 << 20, bytes_accessed=1 << 18, transcendentals=0),
    )(*(pltpu.with_memory_space_constraint(a, pltpu.HBM) for a in (basis, grads)))
    away = swapped(away)
    mine = kernel_call(left_body, lefts)(basis, grads)
    halves = [mine[:8] + away[:8], mine[8:] + away[8:]]
    for flip, cross in DOUBLING:
        pairs = [(2 * p + c, 2 * (p ^ flip) + (c ^ cross)) for p in range(16) for c in range(2)]
        halves = [half + lax.ppermute(half, REPLICA, pairs) for half in halves]
    mine = jnp.concatenate(halves, axis=0)
    other = swapped(mine)
    away = kernel_call(sent_body, rights)(mine, grads)
    away = swapped(away)
    kept, share = kernel_call(kept_body, [rights, f32(4, LANES)])(mine, other, grads)

    sent = kernel_call(pack_body, f32(PEERS * CHUNK, LANES))(kept, away, share)
    came = all_to_all(sent.reshape(PEERS * CHUNK // 4, 4, LANES), PLANE)
    sent = kernel_call(plane_body, f32(STACK * CHUNK, LANES))(came.reshape(-1, LANES))
    came = all_to_all(sent.reshape(STACK * CHUNK // 4, 4, LANES), COLUMN)
    sent, gram = kernel_call(column_body, [rights, f32(16, LANES)])(came.reshape(-1, LANES))
    right = all_to_all(sent, PLANE)
    right, gram = lax.optimization_barrier((right.reshape(32, 8, LANES), gram))
    late = swapped(right)
    early = kernel_call(
        early_body, [f32(RANK, LANES), f32(RANK, width), f32(RANK, rows), f32(RANK, rows)]
    )(gram, right, other, weights, momentum)
    new_basis, new_weights, new_momentum = last(late, mine, weights, momentum, early)
    return tuple(jnp.swapaxes(a, 1, 2) for a in (new_weights, new_basis, new_momentum))


def solution(mesh):
    fine = Mesh(mesh.devices.reshape(tuple(SIZES.values())), tuple(SIZES))
    sharded = P(None, MODEL, REPLICA)
    return jax.shard_map(
        shards,
        mesh=fine,
        in_specs=(P(REPLICA, None, MODEL, None), P(), sharded, sharded),
        out_specs=(sharded, P(), sharded),
        check_vma=False,
    )
```

```python
import itertools

import jax
import jax.numpy as jnp
from jax import lax
from jax.experimental import pallas as pl
from jax.experimental.pallas import tpu as pltpu
from jax.sharding import Mesh
from jax.sharding import PartitionSpec as P


RANK = 32
LANES = 128
SIZES = {"zlo": 4, "y": 4, "core": 2, "zhi": 2, "x": 4}
REPLICA = ("zlo", "y", "core")
MODEL = ("zhi", "x")
PLANE = ("y", "core", "x")
COLUMN = ("zlo", "core", "zhi")
REPLICAS, PEERS, STACK = 32, 16, 8
CHUNK = 20
BLOCK = 16
EXACT = lax.Precision.HIGHEST
VMEM_LIMIT = 24 * 1024 * 1024


def kernel_call(body, outs, flops=1 << 20, moved=1 << 18):
    many = isinstance(outs, (list, tuple))
    count = len(outs) if many else 1
    spec = pl.BlockSpec(memory_space=pltpu.VMEM)
    return lambda *args: pl.pallas_call(
        body,
        out_shape=outs,
        in_specs=[spec] * len(args),
        out_specs=[spec] * count if many else spec,
        compiler_params=pltpu.CompilerParams(vmem_limit_bytes=VMEM_LIMIT),
        cost_estimate=pl.CostEstimate(flops=flops, bytes_accessed=moved, transcendentals=0),
    )(*args)


def f32(*shape):
    return jax.ShapeDtypeStruct(shape, jnp.float32)


def joined(ref, rows, columns):
    return jnp.concatenate(
        [
            jnp.concatenate([ref[t * columns + j] for j in range(columns)], axis=1)
            for t in range(rows)
        ],
        axis=0,
    )


def lane_of(shape):
    return lax.broadcasted_iota(jnp.int32, shape, 1)


def row_of(shape):
    return lax.broadcasted_iota(jnp.int32, shape, 0)


def core():
    return lax.axis_index("core")


def colour(y, zlo, zhi, c):
    return (c + y // 2 + zlo + zhi) % 2


def held():
    return colour(lax.axis_index("y"), lax.axis_index("zlo"), lax.axis_index("zhi"), core())


def owned():
    return 1 - held()


WIDE = 256


def left_of(basis, grads):
    return lax.dot_general(
        basis.astype(jnp.bfloat16),
        grads,
        (((1,), (1,)), ((), ())),
        preferred_element_type=jnp.float32,
    )


def put_left(left, out_ref):
    for t in range(4):
        for j in range(4):
            out_ref[4 * t + j] = left[8 * t : 8 * t + 8, LANES * j : LANES * j + LANES]


def first_body(basis_hbm, grads_hbm, out_ref, grads_ref, basis_ref, sems):
    h = held()
    whole = pltpu.make_async_copy(basis_hbm, basis_ref, sems.at[8])
    whole.start()
    copies = []
    for k in range(8):
        at = (1 - h if k < 4 else h, slice(None), pl.ds(WIDE * (k % 4), WIDE))
        copies.append(pltpu.make_async_copy(grads_hbm.at[at], grads_ref.at[at], sems.at[k]))
        copies[-1].start()
    whole.wait()
    left = jnp.zeros((RANK, grads_ref.shape[1]), jnp.float32)
    for j in range(4):
        copies[j].wait()
        columns = slice(WIDE * j, WIDE * (j + 1))
        left = left + left_of(basis_ref[1 - h, :, columns], grads_ref[1 - h, :, columns])
    put_left(left, out_ref)
    for k in range(4, 8):
        copies[k].wait()


def left_body(basis_ref, grads_ref, out_ref):
    h = held()
    put_left(left_of(basis_ref[h], grads_ref[h]), out_ref)


def put_right(left, grads, out_ref):
    right = jnp.dot(left.astype(jnp.bfloat16), grads, preferred_element_type=jnp.float32)
    for t in range(4):
        for j in range(8):
            d, h = divmod(8 * t + j, 2)
            out_ref[d, 8 * h : 8 * h + 8] = right[8 * t : 8 * t + 8, LANES * j : LANES * j + LANES]


def packed_gram(left):
    gram = lax.dot_general(
        left,
        jnp.concatenate([left] * 4, axis=0),
        (((1,), (1,)), ((), ())),
        precision=EXACT,
        preferred_element_type=jnp.float32,
    )
    return jnp.where(lane_of((16, LANES)) < 64, gram[:16], gram[16:])


def sent_body(left_ref, grads_ref, out_ref):
    put_right(joined(left_ref, 4, 4), grads_ref[held()], out_ref)


def kept_body(mine_ref, other_ref, grads_ref, out_ref, share_ref):
    layer = owned()
    left = joined(other_ref, 4, 4)
    put_right(left, grads_ref[layer], out_ref)
    group = lane_of((16, LANES)) // RANK % 2
    packed = jnp.where(group == layer, packed_gram(left), packed_gram(joined(mine_ref, 4, 4)))
    share_ref[...] = picked([packed[4 * s : 4 * s + 4] for s in range(4)], lax.axis_index("y"))


def picked(values, index):
    out = values[0]
    for s in range(1, len(values)):
        out = jnp.where(index == s, values[s], out)
    return out


def pack_body(mine_ref, other_ref, share_ref, out_ref):
    share = share_ref[...]
    for d in range(PEERS):
        out_ref[CHUNK * d : CHUNK * d + 16] = mine_ref[d] + other_ref[d]
        out_ref[CHUNK * d + 16 : CHUNK * d + CHUNK] = share


def plane_body(in_ref, out_ref):
    total = in_ref[0:16]
    for s in range(1, PEERS):
        total = total + in_ref[CHUNK * s : CHUNK * s + 16]
    parts = []
    for y in range(4):
        part = None
        for x in range(4):
            at = CHUNK * (4 * y + x) + 16
            piece = in_ref[at : at + 4]
            part = piece if part is None else part + piece
        parts.append(part)
    share = picked(parts, lax.axis_index("zlo"))
    for z in range(STACK):
        out_ref[CHUNK * z : CHUNK * z + 16] = total
        out_ref[CHUNK * z + 16 : CHUNK * z + CHUNK] = share


def column_body(in_ref, out_ref, gram_ref):
    total = in_ref[0:16]
    for s in range(1, STACK):
        total = total + in_ref[CHUNK * s : CHUNK * s + 16]
    for d in range(PEERS):
        out_ref[d] = total
    for q in range(4):
        at = 2 * CHUNK * q + 16
        gram_ref[4 * q : 4 * q + 4] = in_ref[at : at + 4] + in_ref[at + CHUNK : at + CHUNK + 4]


def inverse_factors(packed):
    turned = pltpu.roll(packed, 64, 1)
    grams = [packed[0:8], packed[8:16], turned[0:8], turned[8:16]]
    shape = (8, LANES)
    lane, row = lane_of(shape), row_of(shape)
    first = (lane // RANK) % 2 == 0
    front = lane < 64
    units = [(lane % RANK) == row + 8 * r for r in range(4)]
    diagonal = jnp.zeros(shape, jnp.float32)
    for r in range(4):
        diagonal = diagonal + jnp.where(units[r] & front, grams[r], 0.0)
    mean0 = jnp.sum(jnp.where(first, diagonal, 0.0)) * (1.0 / RANK)
    mean1 = jnp.sum(jnp.where(first, 0.0, diagonal)) * (1.0 / RANK)
    ridge = jnp.where(front, 0.001 * jnp.where(first, mean0, mean1), 1.0)
    work = [jnp.where(front, grams[r], 0.0) + jnp.where(units[r], ridge, 0.0) for r in range(4)]
    for b in range(0, RANK, BLOCK):
        columns = [
            {
                r: jnp.where(first, work[r][:, k : k + 1], work[r][:, RANK + k : RANK + k + 1])
                for r in range(b // 8, 4)
            }
            for k in range(b, b + BLOCK)
        ]
        for i in range(BLOCK):
            at, s = divmod(b + i, 8)
            pivot = columns[i][at][s : s + 1]
            inverse = 1.0 / pivot
            chosen = work[at][s : s + 1]
            ahead = {j: columns[j][at][s : s + 1] for j in range(i + 1, BLOCK)}
            for r in range(at, 4):
                factor = columns[i][r] * inverse
                if r == at:
                    factor = jnp.where(row > s, factor, 0.0)
                work[r] = work[r] - factor * chosen
                for j in ahead:
                    columns[j][r] = columns[j][r] - factor * ahead[j]
            work[at] = jnp.where(row == s, work[at] * lax.rsqrt(pivot), work[at])
    return pltpu.roll(jnp.concatenate(work, axis=0), 64, 1)


def settled(layer, right_ref, inverse, left_ref, weights_ref, momentum_ref):
    place = (lax.axis_index("zlo") * 4 + lax.axis_index("y")) * 2 + core()
    block = place // 4
    shift = (4 - place % 4) % 4 * 32
    own = jnp.concatenate([right_ref[8 * t + block] for t in range(4)], axis=0)
    own = pltpu.roll(own, shift, 1)[:, :RANK]
    inverse = jnp.where(layer == 0, inverse[:, :RANK], inverse[:, RANK : 2 * RANK])
    half = jnp.dot(inverse, own, precision=EXACT, preferred_element_type=jnp.float32)
    columns = (((0,), (0,)), ((), ()))
    mixed = lax.dot_general(
        inverse, half, columns, precision=EXACT, preferred_element_type=jnp.float32
    )
    change = lax.dot_general(
        mixed,
        joined(left_ref, 4, 4),
        columns,
        precision=EXACT,
        preferred_element_type=jnp.float32,
    )
    new = 0.9 * momentum_ref[layer] + change * (1.0 / REPLICAS)
    return new, weights_ref[layer] - 0.02 * new


def scale_of(right_ref):
    squares = [jnp.zeros((8, LANES), jnp.float32)] * 4
    for i in range(32):
        tile = right_ref[i]
        squares[i % 4] = squares[i % 4] + tile * tile
    square = (squares[0] + squares[1]) + (squares[2] + squares[3])
    return lax.rsqrt(jnp.sum(square) * (1.0 / (RANK * 1024)) + 1e-12)


def put_scaled(right_ref, scale, t, basis_ref):
    for j in range(8):
        at = (slice(8 * t, 8 * t + 8), slice(LANES * j, LANES * j + LANES))
        basis_ref[at] = right_ref[8 * t + j] * scale


def early_body(gram_ref, right_ref, inverse_ref, basis_ref):
    inverse_ref[...] = inverse_factors(gram_ref[...])
    scale = scale_of(right_ref)
    for t in range(4):
        put_scaled(right_ref, scale, t, basis_ref)


def late_body(
    own_right_ref, right_ref, own_left_ref, left_ref, weights_ref, momentum_ref, inverse_ref, b_ref,
    basis_hbm, w_hbm, m_hbm, basis_ref, new_w_ref, new_m_ref, sems,
):
    layer = held()
    copies = []

    def send(source, target):
        copies.append(pltpu.make_async_copy(source, target, sems.at[len(copies)]))
        copies[-1].start()

    send(b_ref, basis_hbm.at[1 - layer])
    inverse = inverse_ref[...]
    scale = scale_of(right_ref)
    results = [
        settled(1 - layer, own_right_ref, inverse, own_left_ref, weights_ref, momentum_ref),
        settled(layer, right_ref, inverse, left_ref, weights_ref, momentum_ref),
    ]
    for t in range(4):
        put_scaled(right_ref, scale, t, basis_ref)
        rows = slice(8 * t, 8 * t + 8)
        send(basis_ref.at[rows], basis_hbm.at[layer, rows])
    for i, (new, weights) in enumerate(results):
        at = layer if i else 1 - layer
        new_m_ref[i] = new
        send(new_m_ref.at[i], m_hbm.at[at])
        new_w_ref[i] = weights
        send(new_w_ref.at[i], w_hbm.at[at])
    for copy in copies:
        copy.wait()


def last(*args):
    _, basis = args[-2:]
    weights = args[-4]
    local, far = pl.BlockSpec(memory_space=pltpu.VMEM), pl.BlockSpec(memory_space=pltpu.HBM)
    return pl.pallas_call(
        late_body,
        out_shape=[f32(2, *basis.shape), f32(*weights.shape), f32(*weights.shape)],
        in_specs=[local] * len(args),
        out_specs=[far] * 3,
        scratch_shapes=[
            pltpu.VMEM(basis.shape, jnp.float32),
            pltpu.VMEM(weights.shape, jnp.float32),
            pltpu.VMEM(weights.shape, jnp.float32),
            pltpu.SemaphoreType.DMA((9,)),
        ],
        compiler_params=pltpu.CompilerParams(vmem_limit_bytes=VMEM_LIMIT),
        cost_estimate=pl.CostEstimate(flops=1 << 20, bytes_accessed=1 << 18, transcendentals=0),
    )(*args)


DOUBLING = (((1, 0), (3, 1), (4, 1), (8, 0)), ((4, 1), (8, 0), (1, 0), (3, 1)))


def swapped(value):
    return lax.ppermute(value, "core", [(0, 1), (1, 0)])


def all_to_all(value, axes):
    groups = ([], [])
    for i, place in enumerate(itertools.product(*(range(SIZES[a]) for a in axes))):
        at = dict(zip(axes, place))
        groups[colour(at.get("y", 0), at.get("zlo", 0), at.get("zhi", 0), at["core"])].append(i)
    return lax.all_to_all(value, axes, 0, 0, axis_index_groups=groups, tiled=True)


def shards(layer_grads, last_basis, layer_weights, momentum):
    grads = layer_grads[0]
    _, _, width = grads.shape
    basis = jnp.swapaxes(last_basis, 1, 2)
    weights, momentum = jnp.swapaxes(layer_weights, 1, 2), jnp.swapaxes(momentum, 1, 2)
    lefts, rights = f32(PEERS, 8, LANES), f32(PEERS, 16, LANES)

    anywhere = pl.BlockSpec(memory_space=pltpu.HBM)
    local = pl.BlockSpec(memory_space=pltpu.VMEM)
    away, grads, basis = pl.pallas_call(
        first_body,
        out_shape=[lefts, jax.ShapeDtypeStruct(grads.shape, grads.dtype), f32(*basis.shape)],
        in_specs=[anywhere] * 2,
        out_specs=[local] * 3,
        scratch_shapes=[pltpu.SemaphoreType.DMA((9,))],
        compiler_params=pltpu.CompilerParams(vmem_limit_bytes=VMEM_LIMIT),
        cost_estimate=pl.CostEstimate(flops=1 << 20, bytes_accessed=1 << 18, transcendentals=0),
    )(*(pltpu.with_memory_space_constraint(a, pltpu.HBM) for a in (basis, grads)))
    away = swapped(away)
    mine = kernel_call(left_body, lefts)(basis, grads)
    halves = [mine[:8] + away[:8], mine[8:] + away[8:]]
    for steps in zip(*DOUBLING):
        for h, (flip, cross) in enumerate(steps):
            pairs = [
                (2 * p + c, 2 * (p ^ flip) + (c ^ cross)) for p in range(16) for c in range(2)
            ]
            halves[h] = halves[h] + lax.ppermute(halves[h], REPLICA, pairs)
    mine = jnp.concatenate(halves, axis=0)
    other = swapped(mine)
    away = kernel_call(sent_body, rights)(mine, grads)
    away = swapped(away)
    kept, share = kernel_call(kept_body, [rights, f32(4, LANES)])(mine, other, grads)

    sent = kernel_call(pack_body, f32(PEERS * CHUNK, LANES))(kept, away, share)
    came = all_to_all(sent.reshape(PEERS * CHUNK // 4, 4, LANES), PLANE)
    sent = kernel_call(plane_body, f32(STACK * CHUNK, LANES))(came.reshape(-1, LANES))
    came = all_to_all(sent.reshape(STACK * CHUNK // 4, 4, LANES), COLUMN)
    sent, gram = kernel_call(column_body, [rights, f32(16, LANES)])(came.reshape(-1, LANES))
    right = all_to_all(sent, PLANE)
    right, gram = lax.optimization_barrier((right.reshape(32, 8, LANES), gram))
    late = swapped(right)
    inverse, early = kernel_call(early_body, [f32(RANK, LANES), f32(RANK, width)])(gram, right)
    new_basis, new_weights, new_momentum = last(
        right, late, other, mine, weights, momentum, inverse, early
    )
    return tuple(jnp.swapaxes(a, 1, 2) for a in (new_weights, new_basis, new_momentum))


def solution(mesh):
    fine = Mesh(mesh.devices.reshape(tuple(SIZES.values())), tuple(SIZES))
    sharded = P(None, MODEL, REPLICA)
    return jax.shard_map(
        shards,
        mesh=fine,
        in_specs=(P(REPLICA, None, MODEL, None), P(), sharded, sharded),
        out_specs=(sharded, P(), sharded),
        check_vma=False,
    )
```

```python
import itertools

import jax
import jax.numpy as jnp
from jax import lax
from jax.experimental import pallas as pl
from jax.experimental.pallas import tpu as pltpu
from jax.sharding import Mesh
from jax.sharding import PartitionSpec as P


RANK = 32
LANES = 128
SIZES = {"zlo": 4, "y": 4, "core": 2, "zhi": 2, "x": 4}
REPLICA = ("zlo", "y", "core")
MODEL = ("zhi", "x")
PLANE = ("y", "core", "x")
COLUMN = ("zlo", "core", "zhi")
REPLICAS, PEERS, STACK = 32, 16, 8
CHUNK = 20
BLOCK = 16
EXACT = lax.Precision.HIGHEST
VMEM_LIMIT = 24 * 1024 * 1024


def kernel_call(body, outs, flops=1 << 20, moved=1 << 18):
    many = isinstance(outs, (list, tuple))
    count = len(outs) if many else 1
    spec = pl.BlockSpec(memory_space=pltpu.VMEM)
    return lambda *args: pl.pallas_call(
        body,
        out_shape=outs,
        in_specs=[spec] * len(args),
        out_specs=[spec] * count if many else spec,
        compiler_params=pltpu.CompilerParams(vmem_limit_bytes=VMEM_LIMIT),
        cost_estimate=pl.CostEstimate(flops=flops, bytes_accessed=moved, transcendentals=0),
    )(*args)


def f32(*shape):
    return jax.ShapeDtypeStruct(shape, jnp.float32)


def joined(ref, rows, columns):
    return jnp.concatenate(
        [
            jnp.concatenate([ref[t * columns + j] for j in range(columns)], axis=1)
            for t in range(rows)
        ],
        axis=0,
    )


def lane_of(shape):
    return lax.broadcasted_iota(jnp.int32, shape, 1)


def row_of(shape):
    return lax.broadcasted_iota(jnp.int32, shape, 0)


def core():
    return lax.axis_index("core")


def colour(y, zlo, zhi, c):
    return (c + y // 2 + zlo + zhi) % 2


def held():
    return colour(lax.axis_index("y"), lax.axis_index("zlo"), lax.axis_index("zhi"), core())


def owned():
    return 1 - held()


WIDE = 256


def left_of(basis, grads):
    return lax.dot_general(
        basis.astype(jnp.bfloat16),
        grads,
        (((1,), (1,)), ((), ())),
        preferred_element_type=jnp.float32,
    )


def put_left(left, out_ref):
    for t in range(4):
        for j in range(4):
            out_ref[4 * t + j] = left[8 * t : 8 * t + 8, LANES * j : LANES * j + LANES]


def first_body(basis_hbm, grads_hbm, out_ref, grads_ref, basis_ref, sems):
    h = held()
    whole = pltpu.make_async_copy(basis_hbm, basis_ref, sems.at[8])
    whole.start()
    copies = []
    for k in range(8):
        at = (1 - h if k < 4 else h, slice(None), pl.ds(WIDE * (k % 4), WIDE))
        copies.append(pltpu.make_async_copy(grads_hbm.at[at], grads_ref.at[at], sems.at[k]))
        copies[-1].start()
    whole.wait()
    left = jnp.zeros((RANK, grads_ref.shape[1]), jnp.float32)
    for j in range(4):
        copies[j].wait()
        columns = slice(WIDE * j, WIDE * (j + 1))
        left = left + left_of(basis_ref[1 - h, :, columns], grads_ref[1 - h, :, columns])
    put_left(left, out_ref)
    for k in range(4, 8):
        copies[k].wait()


def left_body(basis_ref, grads_ref, out_ref):
    h = held()
    put_left(left_of(basis_ref[h], grads_ref[h]), out_ref)


def put_right(left, grads, out_ref):
    right = jnp.dot(left.astype(jnp.bfloat16), grads, preferred_element_type=jnp.float32)
    for t in range(4):
        for j in range(8):
            d, h = divmod(8 * t + j, 2)
            out_ref[d, 8 * h : 8 * h + 8] = right[8 * t : 8 * t + 8, LANES * j : LANES * j + LANES]


def packed_gram(left):
    gram = lax.dot_general(
        left,
        jnp.concatenate([left] * 4, axis=0),
        (((1,), (1,)), ((), ())),
        precision=EXACT,
        preferred_element_type=jnp.float32,
    )
    return jnp.where(lane_of((16, LANES)) < 64, gram[:16], gram[16:])


def sent_body(left_ref, grads_ref, out_ref):
    put_right(joined(left_ref, 4, 4), grads_ref[held()], out_ref)


def kept_body(mine_ref, other_ref, grads_ref, out_ref, share_ref):
    layer = owned()
    left = joined(other_ref, 4, 4)
    put_right(left, grads_ref[layer], out_ref)
    group = lane_of((16, LANES)) // RANK % 2
    packed = jnp.where(group == layer, packed_gram(left), packed_gram(joined(mine_ref, 4, 4)))
    share_ref[...] = picked([packed[4 * s : 4 * s + 4] for s in range(4)], lax.axis_index("y"))


def picked(values, index):
    out = values[0]
    for s in range(1, len(values)):
        out = jnp.where(index == s, values[s], out)
    return out


def pack_body(mine_ref, other_ref, share_ref, out_ref):
    share = share_ref[...]
    for d in range(PEERS):
        out_ref[CHUNK * d : CHUNK * d + 16] = mine_ref[d] + other_ref[d]
        out_ref[CHUNK * d + 16 : CHUNK * d + CHUNK] = share


def plane_body(in_ref, out_ref):
    total = in_ref[0:16]
    for s in range(1, PEERS):
        total = total + in_ref[CHUNK * s : CHUNK * s + 16]
    parts = []
    for y in range(4):
        part = None
        for x in range(4):
            at = CHUNK * (4 * y + x) + 16
            piece = in_ref[at : at + 4]
            part = piece if part is None else part + piece
        parts.append(part)
    share = picked(parts, lax.axis_index("zlo"))
    for z in range(STACK):
        out_ref[CHUNK * z : CHUNK * z + 16] = total
        out_ref[CHUNK * z + 16 : CHUNK * z + CHUNK] = share


def column_body(in_ref, out_ref, gram_ref):
    total = in_ref[0:16]
    for s in range(1, STACK):
        total = total + in_ref[CHUNK * s : CHUNK * s + 16]
    for d in range(PEERS):
        out_ref[d] = total
    for q in range(4):
        at = 2 * CHUNK * q + 16
        gram_ref[4 * q : 4 * q + 4] = in_ref[at : at + 4] + in_ref[at + CHUNK : at + CHUNK + 4]


def inverse_factors(packed):
    turned = pltpu.roll(packed, 64, 1)
    grams = [packed[0:8], packed[8:16], turned[0:8], turned[8:16]]
    shape = (8, LANES)
    lane, row = lane_of(shape), row_of(shape)
    first = (lane // RANK) % 2 == 0
    front = lane < 64
    units = [(lane % RANK) == row + 8 * r for r in range(4)]
    diagonal = jnp.zeros(shape, jnp.float32)
    for r in range(4):
        diagonal = diagonal + jnp.where(units[r] & front, grams[r], 0.0)
    mean0 = jnp.sum(jnp.where(first, diagonal, 0.0)) * (1.0 / RANK)
    mean1 = jnp.sum(jnp.where(first, 0.0, diagonal)) * (1.0 / RANK)
    ridge = jnp.where(front, 0.001 * jnp.where(first, mean0, mean1), 1.0)
    work = [jnp.where(front, grams[r], 0.0) + jnp.where(units[r], ridge, 0.0) for r in range(4)]
    for b in range(0, RANK, BLOCK):
        columns = [
            {
                r: jnp.where(first, work[r][:, k : k + 1], work[r][:, RANK + k : RANK + k + 1])
                for r in range(b // 8, 4)
            }
            for k in range(b, b + BLOCK)
        ]
        for i in range(BLOCK):
            at, s = divmod(b + i, 8)
            pivot = columns[i][at][s : s + 1]
            inverse = 1.0 / pivot
            chosen = work[at][s : s + 1]
            ahead = {j: columns[j][at][s : s + 1] for j in range(i + 1, BLOCK)}
            for r in range(at, 4):
                factor = columns[i][r] * inverse
                if r == at:
                    factor = jnp.where(row > s, factor, 0.0)
                work[r] = work[r] - factor * chosen
                for j in ahead:
                    columns[j][r] = columns[j][r] - factor * ahead[j]
            work[at] = jnp.where(row == s, work[at] * lax.rsqrt(pivot), work[at])
    return pltpu.roll(jnp.concatenate(work, axis=0), 64, 1)


def settled(layer, right_ref, inverse, left_ref, weights_ref, momentum_ref):
    place = (lax.axis_index("zlo") * 4 + lax.axis_index("y")) * 2 + core()
    block = place // 4
    shift = (4 - place % 4) % 4 * 32
    own = jnp.concatenate([right_ref[8 * t + block] for t in range(4)], axis=0)
    own = pltpu.roll(own, shift, 1)[:, :RANK]
    inverse = jnp.where(layer == 0, inverse[:, :RANK], inverse[:, RANK : 2 * RANK])
    half = jnp.dot(inverse, own, precision=EXACT, preferred_element_type=jnp.float32)
    columns = (((0,), (0,)), ((), ()))
    mixed = lax.dot_general(
        inverse, half, columns, precision=EXACT, preferred_element_type=jnp.float32
    )
    change = lax.dot_general(
        mixed,
        joined(left_ref, 4, 4),
        columns,
        precision=EXACT,
        preferred_element_type=jnp.float32,
    )
    new = 0.9 * momentum_ref[layer] + change * (1.0 / REPLICAS)
    return new, weights_ref[layer] - 0.02 * new


def scale_of(right_ref):
    squares = [jnp.zeros((8, LANES), jnp.float32)] * 4
    for i in range(32):
        tile = right_ref[i]
        squares[i % 4] = squares[i % 4] + tile * tile
    square = (squares[0] + squares[1]) + (squares[2] + squares[3])
    return lax.rsqrt(jnp.sum(square) * (1.0 / (RANK * 1024)) + 1e-12)


def put_scaled(right_ref, scale, t, basis_ref):
    for j in range(8):
        at = (slice(8 * t, 8 * t + 8), slice(LANES * j, LANES * j + LANES))
        basis_ref[at] = right_ref[8 * t + j] * scale


def early_body(
    gram_ref, right_ref, left_ref, weights_ref, momentum_ref, inverse_ref, basis_ref, w_ref, m_ref
):
    inverse = inverse_factors(gram_ref[...])
    inverse_ref[...] = inverse
    scale = scale_of(right_ref)
    for t in range(4):
        put_scaled(right_ref, scale, t, basis_ref)
    m_ref[...], w_ref[...] = settled(
        owned(), right_ref, inverse, left_ref, weights_ref, momentum_ref
    )


def late_body(
    right_ref, left_ref, weights_ref, momentum_ref, inverse_ref, b_ref, w_ref, m_ref,
    basis_hbm, w_hbm, m_hbm, basis_ref, new_w_ref, new_m_ref, sems,
):
    layer = held()
    copies = []

    def send(source, target):
        copies.append(pltpu.make_async_copy(source, target, sems.at[len(copies)]))
        copies[-1].start()

    send(b_ref, basis_hbm.at[1 - layer])
    send(w_ref, w_hbm.at[1 - layer])
    send(m_ref, m_hbm.at[1 - layer])
    new, weights = settled(
        layer, right_ref, inverse_ref[...], left_ref, weights_ref, momentum_ref
    )
    scale = scale_of(right_ref)
    for t in range(4):
        put_scaled(right_ref, scale, t, basis_ref)
        rows = slice(8 * t, 8 * t + 8)
        send(basis_ref.at[rows], basis_hbm.at[layer, rows])
    new_m_ref[...] = new
    send(new_m_ref, m_hbm.at[layer])
    new_w_ref[...] = weights
    send(new_w_ref, w_hbm.at[layer])
    for copy in copies:
        copy.wait()


def last(right, left, weights, momentum, early):
    local, far = pl.BlockSpec(memory_space=pltpu.VMEM), pl.BlockSpec(memory_space=pltpu.HBM)
    shapes = [early[1].shape, early[2].shape, early[3].shape]
    return pl.pallas_call(
        late_body,
        out_shape=[f32(2, *shape) for shape in shapes],
        in_specs=[local] * 8,
        out_specs=[far] * 3,
        scratch_shapes=[
            *(pltpu.VMEM(shape, jnp.float32) for shape in shapes),
            pltpu.SemaphoreType.DMA((9,)),
        ],
        compiler_params=pltpu.CompilerParams(vmem_limit_bytes=VMEM_LIMIT),
        cost_estimate=pl.CostEstimate(flops=1 << 20, bytes_accessed=1 << 18, transcendentals=0),
    )(right, left, weights, momentum, *early)


DOUBLING = (((1, 0), (3, 1), (4, 1), (8, 0)), ((4, 1), (8, 0), (1, 0), (3, 1)))


def swapped(value):
    return lax.ppermute(value, "core", [(0, 1), (1, 0)])


def all_to_all(value, axes):
    groups = ([], [])
    for i, place in enumerate(itertools.product(*(range(SIZES[a]) for a in axes))):
        at = dict(zip(axes, place))
        groups[colour(at.get("y", 0), at.get("zlo", 0), at.get("zhi", 0), at["core"])].append(i)
    return lax.all_to_all(value, axes, 0, 0, axis_index_groups=groups, tiled=True)


def shards(layer_grads, last_basis, layer_weights, momentum):
    grads = layer_grads[0]
    _, rows, width = grads.shape
    basis = jnp.swapaxes(last_basis, 1, 2)
    weights, momentum = jnp.swapaxes(layer_weights, 1, 2), jnp.swapaxes(momentum, 1, 2)
    lefts, rights = f32(PEERS, 8, LANES), f32(PEERS, 16, LANES)

    anywhere = pl.BlockSpec(memory_space=pltpu.HBM)
    local = pl.BlockSpec(memory_space=pltpu.VMEM)
    away, grads, basis = pl.pallas_call(
        first_body,
        out_shape=[lefts, jax.ShapeDtypeStruct(grads.shape, grads.dtype), f32(*basis.shape)],
        in_specs=[anywhere] * 2,
        out_specs=[local] * 3,
        scratch_shapes=[pltpu.SemaphoreType.DMA((9,))],
        compiler_params=pltpu.CompilerParams(vmem_limit_bytes=VMEM_LIMIT),
        cost_estimate=pl.CostEstimate(flops=1 << 20, bytes_accessed=1 << 18, transcendentals=0),
    )(*(pltpu.with_memory_space_constraint(a, pltpu.HBM) for a in (basis, grads)))
    away = swapped(away)
    mine = kernel_call(left_body, lefts)(basis, grads)
    halves = [mine[:10] + away[:10], mine[10:] + away[10:]]
    for steps in zip(*DOUBLING):
        for h, (flip, cross) in enumerate(steps):
            pairs = [
                (2 * p + c, 2 * (p ^ flip) + (c ^ cross)) for p in range(16) for c in range(2)
            ]
            halves[h] = halves[h] + lax.ppermute(halves[h], REPLICA, pairs)
    mine = jnp.concatenate(halves, axis=0)
    other = swapped(mine)
    away = kernel_call(sent_body, rights)(mine, grads)
    away = swapped(away)
    kept, share = kernel_call(kept_body, [rights, f32(4, LANES)])(mine, other, grads)

    sent = kernel_call(pack_body, f32(PEERS * CHUNK, LANES))(kept, away, share)
    came = all_to_all(sent.reshape(PEERS * CHUNK // 4, 4, LANES), PLANE)
    sent = kernel_call(plane_body, f32(STACK * CHUNK, LANES))(came.reshape(-1, LANES))
    came = all_to_all(sent.reshape(STACK * CHUNK // 4, 4, LANES), COLUMN)
    sent, gram = kernel_call(column_body, [rights, f32(16, LANES)])(came.reshape(-1, LANES))
    right = all_to_all(sent, PLANE)
    right, gram = lax.optimization_barrier((right.reshape(32, 8, LANES), gram))
    late = swapped(right)
    early = kernel_call(
        early_body, [f32(RANK, LANES), f32(RANK, width), f32(RANK, rows), f32(RANK, rows)]
    )(gram, right, other, weights, momentum)
    new_basis, new_weights, new_momentum = last(late, mine, weights, momentum, early)
    return tuple(jnp.swapaxes(a, 1, 2) for a in (new_weights, new_basis, new_momentum))


def solution(mesh):
    fine = Mesh(mesh.devices.reshape(tuple(SIZES.values())), tuple(SIZES))
    sharded = P(None, MODEL, REPLICA)
    return jax.shard_map(
        shards,
        mesh=fine,
        in_specs=(P(REPLICA, None, MODEL, None), P(), sharded, sharded),
        out_specs=(sharded, P(), sharded),
        check_vma=False,
    )
```
